32 devices in a mesh: mem: 4 (over y, x), tile: 8 (over z, core).
Axes of the slice: x: 2, y: 2, z: 4, core: 2. Of those that a mesh axis runs over, the one named last changes fastest.
Arguments:
- ensemble: bfloat16 [8, 256, 64, 256], P('mem', None, 'tile'), may hold values from -4 to 4
- control: float32 [8, 64, 256], P('mem', 'tile'), may hold values from -6 to 6
- weights: float32 [8], P('mem'), may hold values from 0.1 to 0.6
- member_band: int32 [8], P('mem'), may hold values from 0 to 3
- spread: float32 [4], replicated, may hold values from 0.05 to 0.24
- advect: float32 [2, 256], replicated, may hold values from -0.9 to 0.9
- damping: float32 [256], replicated, may hold values from 0.02 to 0.2
- innovation: float32 [256, 64, 256], P(None, 'tile'), may hold values from -4 to 4
- obs_weight: float32 [64, 256], P('tile'), may hold values from 0.3 to 27
Outputs:
- grad_control: float32 [8, 64, 256], P('mem', 'tile')
- grad_weight: float32 [8], P('mem')
The draws below stay inside these ranges and needn't reach their ends.
All inputs are finite; a program needn't handle non-finite values.
Results may differ from the reference program's by a relative error of at most 0.0003.
Values sent between devices are 32-bit elements; how exact they have to be, the bound alone decides.
A program may use at most 64 MiB of HBM per device.

```python
import math
import jax
import jax.numpy as jnp
from jax import lax

VL = 256
NY = 256
SWEEPS = 8
BANDS = 4
M = 8
NX = 64


def draw_obs_weight(key, part):
    position = jnp.arange(NX, dtype=jnp.float32) / max(NX - 1, 1)
    ramp = jnp.exp(jnp.log(3.0) * position)
    noise = jax.random.uniform(key, (NX, NY), jnp.float32, 0.5, 2.0)
    return ramp[:, None] * noise


def touch_ends(drawn, stream_key, low, high):
    index_at = [jax.random.randint(jax.random.fold_in(stream_key, axis), (), 0, length) for axis, length in enumerate(drawn.shape)]
    longest = drawn.shape.index(max(drawn.shape))
    beside = index_at[:longest] + [(index_at[longest] + 1) % drawn.shape[longest]] + index_at[longest + 1:]
    return drawn.at[tuple(index_at)].set(low).at[tuple(beside)].set(high)


def levels(rng, dims, shards, smallest, largest):
    level, own = 1.0, jax.random.fold_in(rng, 6)
    for dim, shards_of in shards:
        steps = jnp.exp(jax.random.uniform(jax.random.fold_in(own, dim), (shards_of,), jnp.float32, smallest / len(shards), largest / len(shards)))
        level = level * jnp.repeat(steps, dims[dim] // shards_of).reshape([-1 if axis == dim else 1 for axis in range(len(dims))])
    return level


def bell_draw(own_key, shape, deviation, limit, shards=(), kind=jnp.bfloat16):
    drawn = jax.random.normal(own_key, shape, jnp.float32) * deviation
    if len(shards) > 0:
        drawn = levels(own_key, shape, shards, -0.22, 0.18) * drawn
    return jnp.clip(drawn, min=-limit, max=limit).astype(kind)


def setup_inputs(seed: int = 0) -> dict:
    seeds = jax.random.split(jax.random.key(seed), 10)
    return {
        "ensemble": bell_draw(seeds[0], (M, VL, NX, NY), 0.5, 4.0, ((0, 4), (2, 8))),
        "control": bell_draw(seeds[1], (M, NX, NY), 1.0, 6.0, ((0, 4), (1, 8)), jnp.float32),
        "weights": jnp.clip(0.1 + 0.5 * jax.random.uniform(seeds[2], (M,), jnp.float32) ** levels(seeds[2], (M,), ((0, 4),), -0.2, 0.2), 0.1, 0.6),
        "member_band": touch_ends(jax.random.randint(seeds[3], (M,), 0, BANDS), jax.random.fold_in(seeds[3], 1), 0, BANDS - 1).astype(jnp.int32),
        "spread": jnp.clip(jax.random.uniform(seeds[4], (BANDS,), jnp.float32, 0.05, 0.24), 0.05, 0.24),
        "advect": jnp.clip(jax.random.uniform(seeds[5], (2, VL), jnp.float32, -0.9, 0.9), -0.9, 0.9),
        "damping": jnp.clip(jax.random.uniform(seeds[6], (VL,), jnp.float32, 0.02, 0.2), 0.02, 0.2),
        "innovation": bell_draw(seeds[7], (VL, NX, NY), 0.5, 4.0, ((1, 8),), jnp.float32),
        "obs_weight": draw_obs_weight(jax.random.fold_in(seeds[9], 71), 0),
    }


def y_pairs(field):
    zero_col = jnp.zeros(field.shape[:-1] + (1,), field.dtype)
    north = jnp.concatenate([field[..., 1:], zero_col], axis=-1)
    south = jnp.concatenate([zero_col, field[..., :-1]], axis=-1)
    return (north, south)

def laplace(field):
    north, south = y_pairs(field)
    return jnp.roll(field, -1, -2) + jnp.roll(field, 1, -2) + north + south - 4.0 * field

def localize(field, rates):
    for sweep in range(SWEEPS):
        field = field + rates * laplace(field)
    return field

def dynamics(field, along_x, along_y, smooth):
    east = jnp.roll(field, -1, -2)
    west = jnp.roll(field, 1, -2)
    north, south = y_pairs(field)
    return field - along_x * ((east - west) * 0.5) - along_y * ((north - south) * 0.5) + smooth * (east + west + north + south - 4.0 * field)

def reference(ensemble, control, weights, member_band, spread, advect, damping, innovation, obs_weight):
    one_hot = (member_band[:, None] == jnp.arange(spread.shape[0], dtype=jnp.int32)[None, :]).astype(spread.dtype)
    rates = jnp.dot(one_hot, spread, precision=lax.Precision.HIGHEST)[:, None, None]
    localized = localize(control, rates)

    def accumulate(total, pair):
        member, field = pair
        return (total + member.astype(control.dtype) * field[None], None)
    scaled = weights[:, None, None] * localized
    increment, unused = lax.scan(accumulate, jnp.zeros(ensemble.shape[1:], control.dtype), (ensemble, scaled))
    along_x = advect[0][:, None, None]
    along_y = advect[1][:, None, None]
    smooth = damping[:, None, None]
    forward = dynamics(increment, along_x, along_y, smooth)
    weighted = obs_weight[None] * (forward - innovation)
    gradient = dynamics(weighted, -along_x, -along_y, smooth)

    def project(member):
        return lax.optimization_barrier(jnp.sum(member.astype(control.dtype) * gradient, axis=0))
    projected = lax.map(project, ensemble)
    grad_control = control + localize(weights[:, None, None] * projected, rates)
    grad_weight = lax.optimization_barrier(jnp.sum(localized * projected, axis=(1, 2))) / math.sqrt(NX * NY * VL)
    return (grad_control, grad_weight)
```

```python
import functools
import math

import jax
import jax.numpy as jnp
from jax import lax
from jax.experimental import pallas as pl
from jax.experimental.pallas import tpu as pltpu
from jax.sharding import PartitionSpec as P

SWEEPS = 8
CHUNKS = 4
SHIPPED = 1
LANES = 128
MESH = pl.DeviceIdType.MESH


def factors(n):
    a = max(d for d in range(1, n + 1) if n % d == 0 and d * d <= n)
    return a, n // a


def y_pair(f):
    ny = f.shape[-1]
    col = lax.broadcasted_iota(jnp.int32, f.shape, 1)
    north = jnp.where(col == ny - 1, 0.0, pltpu.roll(f, ny - 1, 1))
    south = jnp.where(col == 0, 0.0, pltpu.roll(f, 1, 1))
    return north, south


def sweeps(f, rates):
    rows = f.shape[0]
    for _ in range(SWEEPS):
        north, south = y_pair(f)
        east = pltpu.roll(f, rows - 1, 0)
        west = pltpu.roll(f, 1, 0)
        f = f + rates * (east + west + north + south - 4.0 * f)
    return f


def kernel(
    n, tiles, steps, ship,
    ens, control_h, weights_h, band_h, spread_h, advect_h, damping_h, innov, obs_h,
    out_h, gw_h,
    args, outs, local_sems,
    e_v, fields, per_q,
    sems,
):
    a, b = factors(n)
    control, weights, band, spread, advect, damping, obs = args
    out, gw_out = outs
    arg_sem, out_sem, e_sem, i_sem = local_sems
    loc, scl, proj, ch, wh, wb, ph, gwr = fields
    ml, rows, ny = control.shape
    vl = ens.shape[1]
    nc = ny // LANES
    me = lax.axis_index("mem")
    t = lax.axis_index("tile")
    nxt = (t + 1) % tiles
    prv = (t + tiles - 1) % tiles
    ia = me // b
    ib = me % b
    first = (b, a)
    second = (a, b)
    fi = (ib, ia)
    gi = (ia, ib)
    size = [vl // (2 * f) for f in first]
    chunk = [k // steps for k in size]
    lone = tuple(range(ship, steps))
    sent = tuple(range(ship))

    def device(q, f, g):
        return g * b + f if q == 0 else f * b + g

    def start_of(q, owner, s):
        return pl.multiple_of(q * (vl // 2) + (owner * steps + s) * chunk[q], chunk[q])

    def ahead(q, d):
        return (fi[q] + d) % first[q]

    def behind(q, d):
        return (fi[q] + first[q] - d) % first[q]

    def to_first(q, d):
        return device(q, ahead(q, d), gi[q])

    def back_first(q, d):
        return device(q, behind(q, d), gi[q])

    def to_second(q, d):
        return device(q, fi[q], (gi[q] + d) % second[q])

    def remote(kind, index, src, dst, axis, dev):
        s_sem, r_sem = sems[kind]
        return pltpu.make_async_remote_copy(
            src_ref=src, dst_ref=dst, send_sem=s_sem.at[index], recv_sem=r_sem.at[index],
            device_id={axis: dev}, device_id_type=MESH,
        )

    def lanes(c):
        return slice(c * LANES, (c + 1) * LANES)

    barrier = pltpu.get_barrier_semaphore()
    for d in range(1, tiles):
        pl.semaphore_signal(
            barrier, inc=1, device_id={"tile": (t + d) % tiles}, device_id_type=MESH
        )
    for q in range(2):
        for d in range(1, first[q]):
            pl.semaphore_signal(
                barrier, inc=1, device_id={"mem": to_first(q, d)}, device_id_type=MESH
            )

    def ens_copy(q, d, late):
        if d == 0:
            where = pl.ds(start_of(q, fi[q], 0), size[q])
        elif late:
            where = pl.ds(start_of(q, ahead(q, d), ship), (steps - ship) * chunk[q])
        else:
            where = pl.ds(start_of(q, ahead(q, d), 0), ship * chunk[q])
        return pltpu.make_async_copy(
            ens.at[:, where], e_v.at[:, where], e_sem.at[q, d, int(late)]
        )

    arg_copy = [
        pltpu.make_async_copy(src, dst, arg_sem.at[i])
        for i, (src, dst) in enumerate((
            (control_h, control), (obs_h, obs), (weights_h, weights), (band_h, band),
            (spread_h, spread), (advect_h, advect), (damping_h, damping),
        ))
    ]
    innov_copy = [
        pltpu.make_async_copy(
            innov.at[pl.ds(start_of(q, fi[q], 0), size[q]), :, lanes(c)],
            per_q["iv"][q].at[:, c],
            i_sem.at[q, c],
        )
        for q in range(2)
        for c in range(nc)
    ]
    early = [ens_copy(q, d, False) for q in range(2) for d in range(1, first[q])]
    late = [ens_copy(q, 0, False) for q in range(2)]
    late += [ens_copy(q, d, True) for q in range(2) for d in range(1, first[q])]
    for c in early + arg_copy + late + innov_copy:
        c.start()

    def ship_copy(q, i, d):
        return remote(
            "ship", (q, i, d - 1), per_q["es"][q].at[i, d - 1], per_q["er"][q].at[i, d - 1],
            "mem", to_first(q, d),
        )

    def scl_copy(q, d):
        return remote(
            "scl", (q, d - 1), scl, per_q["sr"][q].at[d - 1], "mem", to_first(q, d)
        )

    def part_copy(q, s, d):
        i = s - ship
        return remote(
            "part", (q, i, d - 1), per_q["to"][q].at[i, d - 1], per_q["r1"][q].at[i, d - 1],
            "mem", to_first(q, d),
        )

    def swap_copy(q, s, d):
        return remote(
            "swap", (q, s, d - 1),
            per_q["part"][q].at[pl.ds(s * chunk[q], chunk[q])], per_q["r2"][q].at[s, d - 1],
            "mem", to_second(q, d),
        )

    def grad_copy(q, s, d):
        i = s - ship
        return remote(
            "grad", (q, i, d - 1),
            per_q["grad"][q].at[pl.ds(s * chunk[q], chunk[q])], per_q["gr"][q].at[i, d - 1],
            "mem", to_first(q, d),
        )

    def proj_copy(q, d):
        return remote(
            "proj", (q, d - 1), per_q["pp"][q].at[d - 1], per_q["pr"][q].at[d - 1],
            "mem", back_first(q, d),
        )

    def both(kind, k, src, dst):
        return (
            remote(kind, k, src, dst.at[0], "tile", nxt),
            remote(kind, k + 1, src, dst.at[1], "tile", prv),
        )

    def innov_halo(q):
        ov = per_q["ov"][q]
        return (
            remote("edge", 4 + 2 * q, ov.at[rows], ov.at[0], "tile", nxt),
            remote("edge", 5 + 2 * q, ov.at[1], ov.at[rows + 1], "tile", prv),
        )

    def halo(q, s):
        ip = per_q["ip"][q]
        where = pl.ds(s * chunk[q], chunk[q])
        return (
            remote("halo", (0, q, s), ip.at[pl.ds(rows, 2), where], ip.at[pl.ds(0, 2), where], "tile", nxt),
            remote("halo", (1, q, s), ip.at[pl.ds(2, 2), where], ip.at[pl.ds(rows + 2, 2), where], "tile", prv),
        )

    c_copy = both("edge", 0, control, ch)
    w_copy = both("edge", 2, obs, wh)
    p_copy = both("edge", 8, scl, ph)
    o_copy = innov_halo(0) + innov_halo(1)

    for c in early:
        c.wait()
    for q in range(2):
        for i in sent:
            for d in range(1, first[q]):
                where = pl.ds(start_of(q, ahead(q, d), i), chunk[q])
                for m in range(ml):
                    e = e_v[m, where].astype(jnp.float32)
                    for c in range(nc):
                        per_q["es"][q][i, d - 1, m, :, c] = e[:, :, lanes(c)]
    for c in arg_copy[:2]:
        c.wait()
    pl.semaphore_wait(barrier, tiles - 1 + a - 1 + b - 1)
    for c in c_copy + w_copy:
        c.start()
    for i in sent:
        for q in range(2):
            for d in range(1, first[q]):
                ship_copy(q, i, d).start()

    for c in innov_copy:
        c.wait()
    for q in range(2):
        flat = per_q["iv"][q].reshape(size[q] * nc * rows, LANES)
        ov = per_q["ov"][q]

        @pl.loop(0, size[q] // 8)
        def _(j):
            for c in range(nc):
                for r in range(rows):
                    ov[1 + r, pl.ds(pl.multiple_of(j * 8, 8), 8), lanes(c)] = flat[
                        pl.ds(j * (8 * nc * rows) + c * rows + r, 8, stride=nc * rows), :
                    ]

    for c in o_copy:
        c.start()
    for c in arg_copy[2:]:
        c.wait()
    for q in range(2):
        coef = per_q["coef"][q]
        base = start_of(q, fi[q], 0)
        sub = lax.broadcasted_iota(jnp.int32, (8, LANES), 0)

        @pl.loop(0, size[q] // 8)
        def _(j):
            for kind, value in enumerate((
                lambda k: advect[0, k], lambda k: advect[1, k], lambda k: damping[k]
            )):
                v = jnp.full((8, LANES), value(base + j * 8), jnp.float32)
                for i in range(1, 8):
                    v = jnp.where(sub == i, value(base + j * 8 + i), v)
                coef[kind, pl.ds(pl.multiple_of(j * 8, 8), 8)] = v

    rates = jnp.concatenate(
        [jnp.full((3 * rows, ny), spread[band[m]], jnp.float32) for m in range(ml)], axis=0
    )
    for c in c_copy:
        c.wait_recv()
    field = []
    for m in range(ml):
        field += [ch[0, m], control[m], ch[1, m]]
    field = sweeps(jnp.concatenate(field, axis=0), rates)
    for m in range(ml):
        center = field[(3 * m + 1) * rows : (3 * m + 2) * rows]
        loc[m] = center
        scl[m] = weights[m] * center
        proj[m] = jnp.zeros_like(center)
        for q in range(2):
            for d in range(1, first[q]):
                per_q["pp"][q][d - 1, m] = jnp.zeros_like(center)
    for q in range(2):
        for d in range(1, first[q]):
            if ship:
                scl_copy(q, d).start()
    for c in late:
        c.wait()

    def own_sum(q, owner, s, c):
        where = pl.ds(start_of(q, owner, s), chunk[q])
        total = None
        for m in range(ml):
            term = e_v[m, where, :, lanes(c)].astype(jnp.float32) * scl[m, :, lanes(c)][None]
            total = term if total is None else total + term
        return total

    for s in lone:
        for q in range(2):
            for d in range(1, first[q]):
                for c in range(nc):
                    per_q["to"][q][s - ship, d - 1, :, c] = own_sum(q, ahead(q, d), s, c)
                part_copy(q, s, d).start()
    for s in range(steps):
        for q in range(2):
            for c in range(nc):
                per_q["part"][q][s * chunk[q] : (s + 1) * chunk[q], c] = own_sum(q, fi[q], s, c)
    for c in w_copy:
        c.wait_recv()
    weight = (wh[0, rows - 1 :], obs[...], wh[1, :1])
    wb[0] = jnp.broadcast_to(weight[0], (8, ny))
    wb[rows + 1] = jnp.broadcast_to(weight[2], (8, ny))
    for r in range(rows):
        wb[1 + r] = jnp.broadcast_to(weight[1][r : r + 1], (8, ny))

    def add_first(s):
        for q in range(2):
            where = slice(s * chunk[q], (s + 1) * chunk[q])
            for c in range(nc):
                total = per_q["part"][q][where, c]
                for d in range(1, first[q]):
                    if s >= ship:
                        if c == 0:
                            part_copy(q, s, d).wait_recv()
                        total = total + per_q["r1"][q][s - ship, d - 1, :, c]
                    else:
                        if c == 0:
                            ship_copy(q, s, d).wait_recv()
                            if s == 0:
                                scl_copy(q, d).wait_recv()
                        for m in range(ml):
                            total = total + (
                                per_q["er"][q][s, d - 1, m, :, c]
                                * per_q["sr"][q][d - 1, m, :, lanes(c)][None]
                            )
                per_q["part"][q][where, c] = total
            for d in range(1, second[q]):
                swap_copy(q, s, d).start()

    def add_second(s):
        for q in range(2):
            for d in range(1, second[q]):
                swap_copy(q, s, d).wait_recv()
            flat = per_q["part"][q].reshape(size[q] * nc * rows, LANES)
            peers = [
                per_q["r2"][q].at[s, d - 1].reshape(chunk[q] * nc * rows, LANES)
                for d in range(1, second[q])
            ]
            ip = per_q["ip"][q]

            @pl.loop(0, chunk[q] // 8)
            def _(j):
                for c in range(nc):
                    for r in range(rows):
                        at = j * (8 * nc * rows) + c * rows + r
                        total = flat[
                            pl.ds(s * (chunk[q] * nc * rows) + at, 8, stride=nc * rows), :
                        ]
                        for p in peers:
                            total = total + p[pl.ds(at, 8, stride=nc * rows), :]
                        ip[2 + r, pl.ds(pl.multiple_of(s * chunk[q] + j * 8, 8), 8), lanes(c)] = total

            for c in halo(q, s):
                c.start()

    def adjoint(s):
        col = lax.broadcasted_iota(jnp.int32, (8, ny), 1)
        for q in range(2):
            for c in halo(q, s):
                c.wait_recv()
            flat = per_q["grad"][q].reshape(size[q] * nc * rows, LANES)
            ip = per_q["ip"][q]
            ov = per_q["ov"][q]
            coef = per_q["coef"][q]

            @pl.loop(0, chunk[q] // 8)
            def _(j):
                where = pl.ds(pl.multiple_of(s * chunk[q] + j * 8, 8), 8)
                ax, ay, e = (
                    jnp.concatenate([coef[k, where]] * nc, axis=1) for k in range(3)
                )
                mid = 1.0 - 4.0 * e
                up = e - 0.5 * ax
                down = e + 0.5 * ax
                left = e - 0.5 * ay
                right = e + 0.5 * ay
                north1 = jnp.where(col == ny - 1, 0.0, left)
                south1 = jnp.where(col == 0, 0.0, right)
                north2 = jnp.where(col == ny - 1, 0.0, right)
                south2 = jnp.where(col == 0, 0.0, left)

                def turn(f):
                    return pltpu.roll(f, ny - 1, 1), pltpu.roll(f, 1, 1)

                f = [ip[r, where, :] for r in range(rows + 4)]
                w = []
                for r in range(1, rows + 3):
                    north, south = turn(f[r])
                    d = (
                        mid * f[r] + up * f[r + 1] + down * f[r - 1]
                        + north1 * north + south1 * south
                    )
                    w.append(wb[r - 1] * (d - ov[r - 1, where, :]))
                for r in range(1, rows + 1):
                    north, south = turn(w[r])
                    g = (
                        mid * w[r] + down * w[r + 1] + up * w[r - 1]
                        + north2 * north + south2 * south
                    )
                    for c in range(nc):
                        at = (s * chunk[q] + j * 8) * (nc * rows) + c * rows + r - 1
                        flat[pl.ds(at, 8, stride=nc * rows), :] = g[:, lanes(c)]

            if s >= ship:
                for d in range(1, first[q]):
                    grad_copy(q, s, d).start()

    def project_own(s):
        for q in range(2):
            where = pl.ds(start_of(q, fi[q], s), chunk[q])
            for c in range(nc):
                g = per_q["grad"][q][s * chunk[q] : (s + 1) * chunk[q], c]
                for m in range(ml):
                    e = e_v[m, where, :, lanes(c)].astype(jnp.float32)
                    proj[m, :, lanes(c)] += jnp.sum(e * g, axis=0)
                if s < ship:
                    for d in range(1, first[q]):
                        for m in range(ml):
                            e = per_q["er"][q][s, d - 1, m, :, c]
                            per_q["pp"][q][d - 1, m, :, lanes(c)] += jnp.sum(e * g, axis=0)

    def project_in(s):
        for q in range(2):
            for d in range(1, first[q]):
                grad_copy(q, s, d).wait_recv()
                where = pl.ds(start_of(q, behind(q, d), s), chunk[q])
                for c in range(nc):
                    g = per_q["gr"][q][s - ship, d - 1, :, c]
                    for m in range(ml):
                        e = e_v[m, where, :, lanes(c)].astype(jnp.float32)
                        proj[m, :, lanes(c)] += jnp.sum(e * g, axis=0)

    order = lone + sent
    scope = jax.named_scope
    for s in order:
        with scope(f"add_first{s}"):
            add_first(s)
    lag = 1
    for tick in range(len(order) + lag):
        if tick < len(order):
            with scope(f"add_second{order[tick]}"):
                add_second(order[tick])
        if tick == lag:
            for c in o_copy:
                c.wait_recv()
        if tick >= lag:
            s = order[tick - lag]
            with scope(f"adjoint{s}"):
                adjoint(s)
            with scope(f"project_own{s}"):
                project_own(s)
    if ship:
        for q in range(2):
            for d in range(1, first[q]):
                proj_copy(q, d).start()
    for s in lone:
        with scope(f"project_in{s}"):
            project_in(s)
    with scope("tail"):
        if ship:
            for q in range(2):
                for d in range(1, first[q]):
                    proj_copy(q, d).wait_recv()
        for m in range(ml):
            total = proj[m]
            if ship:
                for q in range(2):
                    for d in range(1, first[q]):
                        total = total + per_q["pr"][q][d - 1, m]
                        scl_copy(q, d).wait_send() if m == 0 else None
            proj[m] = total
            scl[m] = weights[m] * total
    with scope("halo_out"):
        for c in p_copy:
            c.start()
        row = lax.broadcasted_iota(jnp.int32, (8, LANES), 0)
        sums = jnp.zeros((8, LANES), jnp.float32)
        for m in range(ml):
            v = jnp.sum(loc[m] * proj[m], axis=0, keepdims=True)
            v = sum(v[:, lanes(c)] for c in range(nc))
            sums = jnp.where(row == m, jnp.broadcast_to(v, (8, LANES)), sums)
        gwr[t] = sums

        def gw_copy(d, incoming=False):
            slot = (t + tiles - d) % tiles if incoming else t
            return remote("gw", d - 1, gwr.at[slot], gwr.at[slot], "tile", (t + d) % tiles)

        for d in range(1, tiles):
            gw_copy(d).start()
        for c in p_copy:
            c.wait_recv()
    with scope("sweeps"):
        field = []
        for m in range(ml):
            field += [ph[0, m], scl[m], ph[1, m]]
        field = sweeps(jnp.concatenate(field, axis=0), rates)
        for m in range(ml):
            out[m] = control[m] + field[(3 * m + 1) * rows : (3 * m + 2) * rows]
    with scope("finish"):
        done = (
            pltpu.make_async_copy(out, out_h, out_sem.at[0]),
            pltpu.make_async_copy(gw_out, gw_h, out_sem.at[1]),
        )
        done[0].start()
        for d in range(1, tiles):
            gw_copy(d, True).wait_recv()
        total = gwr[0]
        for d in range(1, tiles):
            total = total + gwr[d]
        gw_out[...] = jnp.broadcast_to(jnp.sum(total, axis=1, keepdims=True), (8, LANES))
        done[1].start()

        for c in c_copy + w_copy + o_copy + p_copy:
            c.wait_send()
        for d in range(1, tiles):
            gw_copy(d).wait_send()
        for q in range(2):
            for s in range(steps):
                for c in halo(q, s):
                    c.wait_send()
                for d in range(1, second[q]):
                    swap_copy(q, s, d).wait_send()
                for d in range(1, first[q]):
                    if s >= ship:
                        part_copy(q, s, d).wait_send()
                        grad_copy(q, s, d).wait_send()
                    else:
                        ship_copy(q, s, d).wait_send()
            if ship:
                for d in range(1, first[q]):
                    proj_copy(q, d).wait_send()
        for c in done:
            c.wait()


def per_device(
    n, tiles,
    ensemble, control, weights, member_band, spread, advect, damping, innovation, obs_weight
):
    ml, vl, rows, ny = ensemble.shape
    a, b = factors(n)
    first, second = (b, a), (a, b)
    assert rows == SWEEPS and ny % LANES == 0 and ml <= 8 and vl % (16 * b) == 0
    nc = ny // LANES
    size = [vl // (2 * f) for f in first]
    steps = max(d for d in range(1, CHUNKS + 1) if all(k % (8 * d) == 0 for k in size))
    ship = min(SHIPPED, steps - 1)
    chunk = [k // steps for k in size]
    f32 = jnp.float32
    peers = max(a, b, 2) - 1
    dma = pltpu.SemaphoreType.DMA
    hbm = pl.BlockSpec(memory_space=pl.ANY)
    field = (rows, ny)
    tile = (nc, rows, LANES)
    vmem = lambda *shape: pltpu.VMEM(shape, f32)
    fp = [max(f - 1, 1) for f in first]
    gp = [max(g - 1, 1) for g in second]
    ns, nl = max(ship, 1), max(steps - ship, 1)

    def per(shape):
        return tuple(vmem(*shape(q)) for q in range(2))

    per_q = {
        "es": per(lambda q: (ns, fp[q], ml, chunk[q]) + tile),
        "er": per(lambda q: (ns, fp[q], ml, chunk[q]) + tile),
        "to": per(lambda q: (nl, fp[q], chunk[q]) + tile),
        "r1": per(lambda q: (nl, fp[q], chunk[q]) + tile),
        "part": per(lambda q: (size[q],) + tile),
        "r2": per(lambda q: (steps, gp[q], chunk[q]) + tile),
        "grad": per(lambda q: (size[q],) + tile),
        "gr": per(lambda q: (nl, fp[q], chunk[q]) + tile),
        "iv": per(lambda q: (size[q],) + tile),
        "ip": per(lambda q: (rows + 4, size[q], ny)),
        "ov": per(lambda q: (rows + 2, size[q], ny)),
        "coef": per(lambda q: (3, size[q], LANES)),
        "pp": per(lambda q: (fp[q], ml) + field),
        "pr": per(lambda q: (fp[q], ml) + field),
        "sr": per(lambda q: (fp[q], ml) + field),
    }
    pair = lambda *shape: (dma(shape), dma(shape))
    sems = {
        "ship": pair(2, ns, peers),
        "scl": pair(2, peers),
        "part": pair(2, nl, peers),
        "swap": pair(2, steps, peers),
        "grad": pair(2, nl, peers),
        "proj": pair(2, peers),
        "edge": pair(10),
        "halo": pair(2, 2, steps),
        "gw": pair(max(tiles - 1, 1)),
    }
    args = (
        vmem(*control.shape),
        pltpu.SMEM(weights.shape, f32),
        pltpu.SMEM(member_band.shape, member_band.dtype),
        pltpu.SMEM(spread.shape, f32),
        pltpu.SMEM(advect.shape, f32),
        pltpu.SMEM(damping.shape, f32),
        vmem(*obs_weight.shape),
    )
    fields = (
        vmem(ml, *field), vmem(ml, *field), vmem(ml, *field),
        vmem(2, ml, *field), vmem(2, *field), vmem(rows + 2, 8, ny),
        vmem(2, ml, *field), vmem(tiles, 8, LANES),
    )
    out, gw = pl.pallas_call(
        functools.partial(kernel, n, tiles, steps, ship),
        out_shape=(
            jax.ShapeDtypeStruct((ml, rows, ny), f32),
            jax.ShapeDtypeStruct((8, LANES), f32),
        ),
        in_specs=[hbm] * 9,
        out_specs=(hbm, hbm),
        scratch_shapes=[
            args,
            (vmem(*control.shape), vmem(8, LANES)),
            (dma((7,)), dma((2,)), dma((2, peers + 1, 2)), dma((2, nc))),
            pltpu.VMEM((ml, vl) + field, ensemble.dtype),
            fields,
            per_q,
            sems,
        ],
        compiler_params=pltpu.CompilerParams(
            collective_id=0, has_side_effects=True, vmem_limit_bytes=60 * 1024 * 1024
        ),
    )(ensemble, control, weights, member_band, spread, advect, damping, innovation, obs_weight)
    total_cells = tiles * rows * ny * vl
    return out, gw[:ml, 0] / math.sqrt(total_cells)


def solution(mesh):
    in_specs = (
        P("mem", None, "tile", None),
        P("mem", "tile", None),
        P("mem"),
        P("mem"),
        P(),
        P(),
        P(),
        P(None, "tile", None),
        P("tile", None),
    )
    out_specs = (P("mem", "tile", None), P("mem"))
    return jax.shard_map(
        functools.partial(per_device, mesh.shape["mem"], mesh.shape["tile"]),
        mesh=mesh, in_specs=in_specs, out_specs=out_specs, check_vma=False,
    )
```

```python
import functools
import math

import jax
import jax.numpy as jnp
from jax import lax
from jax.experimental import pallas as pl
from jax.experimental.pallas import tpu as pltpu
from jax.sharding import PartitionSpec as P

SWEEPS = 8
CHUNKS = 4
SHIPPED = 1
AFTER = 9
LAG = 1
LANES = 128
MESH = pl.DeviceIdType.MESH


def factors(n):
    a = max(d for d in range(1, n + 1) if n % d == 0 and d * d <= n)
    return a, n // a


def y_pair(f):
    ny = f.shape[-1]
    col = lax.broadcasted_iota(jnp.int32, f.shape, 1)
    north = jnp.where(col == ny - 1, 0.0, pltpu.roll(f, ny - 1, 1))
    south = jnp.where(col == 0, 0.0, pltpu.roll(f, 1, 1))
    return north, south


def sweeps(f, rates):
    rows = f.shape[0]
    for _ in range(SWEEPS):
        north, south = y_pair(f)
        east = pltpu.roll(f, rows - 1, 0)
        west = pltpu.roll(f, 1, 0)
        f = f + rates * (east + west + north + south - 4.0 * f)
    return f


def kernel(
    n, tiles, steps, ship,
    ens, control_h, weights_h, band_h, spread_h, advect_h, damping_h, innov, obs_h,
    out, gw_out,
    args, arg_sem, e_v, buf, sems,
):
    a, b = factors(n)
    control, obs, weights, band, spread, advect, damping = args
    loc, scl, proj = buf["loc"], buf["scl"], buf["proj"]
    ml, rows, ny = control.shape
    vl = ens.shape[1]
    nc = ny // LANES
    me = lax.axis_index("mem")
    t = lax.axis_index("tile")
    nxt = (t + 1) % tiles
    prv = (t + tiles - 1) % tiles
    ia = me // b
    ib = me % b
    first = (b, a)
    second = (a, b)
    fi = (ib, ia)
    gi = (ia, ib)
    size = [vl // (2 * f) for f in first]
    chunk = [k // steps for k in size]
    both_q = sum(chunk)
    lead = (0, chunk[0])
    lead1 = (0, (first[0] - 1) * chunk[0])
    lead2 = (0, (second[0] - 1) * chunk[0])
    some_first = sum(f - 1 for f in first) > 0
    some_second = sum(g - 1 for g in second) > 0
    lone = tuple(range(ship, steps))
    sent = tuple(range(ship)) if some_first else ()
    order = lone[:AFTER] + tuple(range(ship)) + lone[AFTER:]
    near = tiles // 2 <= 2 + steps
    greet = sorted({1, tiles - 1}) if near else list(range(1, tiles))
    greet = [d for d in greet if d % tiles]

    def device(q, f, g):
        return g * b + f if q == 0 else f * b + g

    def start_of(q, owner, s):
        return pl.multiple_of(q * (vl // 2) + (owner * steps + s) * chunk[q], chunk[q])

    def ahead(q, d):
        return (fi[q] + d) % first[q]

    def behind(q, d):
        return (fi[q] + first[q] - d) % first[q]

    def to_first(q, d):
        return device(q, ahead(q, d), gi[q])

    def back_first(q, d):
        return device(q, behind(q, d), gi[q])

    def to_second(q, d):
        return device(q, fi[q], (gi[q] + d) % second[q])

    def first_peers():
        return [(q, d) for q in range(2) for d in range(1, first[q])]

    def second_peers():
        return [(q, d) for q in range(2) for d in range(1, second[q])]

    def remote(kind, index, src, dst, axis, dev):
        s_sem, r_sem = sems[kind]
        return pltpu.make_async_remote_copy(
            src_ref=src, dst_ref=dst, send_sem=s_sem.at[0], recv_sem=r_sem.at[index],
            device_id={axis: dev}, device_id_type=MESH,
        )

    def arrived(kind, index, ref):
        remote(kind, index, ref, ref, "tile", nxt).wait_recv()

    def left(kind, ref):
        remote(kind, 0, ref, ref, "tile", nxt).wait_send()

    def lanes(c):
        return slice(c * LANES, (c + 1) * LANES)

    barrier = pltpu.get_barrier_semaphore()
    for q, d in first_peers():
        pl.semaphore_signal(
            barrier, inc=1, device_id={"mem": to_first(q, d)}, device_id_type=MESH
        )
    for d in greet:
        pl.semaphore_signal(
            barrier, inc=1, device_id={"tile": (t + d) % tiles}, device_id_type=MESH
        )

    def load(k, src, dst):
        return pltpu.make_async_copy(src, dst, arg_sem.at[k])

    def ens_load(k, q, owner, s, count):
        where = pl.ds(start_of(q, owner, s), count * chunk[q])
        return load(k, ens.at[:, where], e_v.at[:, where])

    early = [ens_load(0, q, ahead(q, d), 0, ship) for q, d in first_peers() if ship]
    late = [ens_load(1, q, fi[q], 0, steps) for q in range(2)]
    late += [ens_load(1, q, ahead(q, d), ship, steps - ship) for q, d in first_peers()]
    innov_load = [
        load(
            2,
            innov.at[pl.ds(start_of(q, fi[q], s), chunk[q]), :, lanes(c)],
            buf["iv"].at[pl.ds(s * both_q + lead[q], chunk[q]), c],
        )
        for s in range(steps)
        for q in range(2)
        for c in range(nc)
    ]
    arg_load = [
        load(3 + i, src, dst)
        for i, (src, dst) in enumerate((
            (control_h, control), (obs_h, obs), (weights_h, weights), (band_h, band),
            (spread_h, spread), (advect_h, advect), (damping_h, damping),
        ))
    ]
    for c in early + arg_load + innov_load + late:
        c.start()
    early_planes = ship * sum((first[q] - 1) * chunk[q] for q in range(2))

    def block1(q, d, per=1):
        return pl.ds((lead1[q] + (d - 1) * chunk[q]) * per, chunk[q] * per)

    def block2(q, d):
        return pl.ds(lead2[q] + (d - 1) * chunk[q], chunk[q])

    def own(q, s):
        return pl.ds(s * both_q + lead[q], chunk[q])

    def slot(q, d):
        return (first[0] - 1) * q + d - 1

    def ship_copy(q, s, d):
        where = block1(q, d, ml)
        return remote(
            "ship", s, buf["es"].at[s, where], buf["er"].at[s, where], "mem", to_first(q, d)
        )

    def scl_copy(q, d):
        return remote("scl", 0, scl, buf["sr"].at[slot(q, d)], "mem", to_first(q, d))

    def part_copy(q, s, d):
        where = block1(q, d)
        return remote(
            "part", s - ship, buf["to"].at[s - ship, where], buf["r1"].at[s - ship, where],
            "mem", to_first(q, d),
        )

    def swap_copy(q, s, d):
        return remote(
            "swap", s, buf["part"].at[own(q, s)], buf["r2"].at[s, block2(q, d)],
            "mem", to_second(q, d),
        )

    def grad_copy(q, s, d):
        return remote(
            "grad", s - ship, buf["grad"].at[own(q, s)], buf["gr"].at[s - ship, block1(q, d)],
            "mem", to_first(q, d),
        )

    def proj_copy(q, d):
        return remote(
            "proj", 0, buf["pp"].at[slot(q, d)], buf["pr"].at[slot(q, d)],
            "mem", back_first(q, d),
        )

    def to_both(kind, src, dst):
        return (
            remote(kind, 0, src, dst.at[0], "tile", nxt),
            remote(kind, 0, src, dst.at[1], "tile", prv),
        )

    ip, ov = buf["ip"], buf["ov"]

    def halo(s):
        where = pl.ds(s * both_q, both_q)
        return (
            remote("halo", s, ip.at[pl.ds(rows, 2), where], ip.at[pl.ds(0, 2), where], "tile", nxt),
            remote("halo", s, ip.at[pl.ds(2, 2), where], ip.at[pl.ds(rows + 2, 2), where], "tile", prv),
        )

    c_copy = to_both("control", control, buf["ch"])
    w_copy = to_both("weight", obs, buf["wh"])
    p_copy = to_both("field", scl, buf["ph"])
    o_copy = (
        remote("innov", 0, ov.at[rows], ov.at[0], "tile", nxt),
        remote("innov", 0, ov.at[1], ov.at[rows + 1], "tile", prv),
    )

    if sent:
        where = e_v.at[:, pl.ds(0, early_planes)]
        load(0, where, where).wait()
    for s in sent:
        for q, d in first_peers():
            where = pl.ds(start_of(q, ahead(q, d), s), chunk[q])
            for m in range(ml):
                e = e_v[m, where].astype(jnp.float32)
                at = (lead1[q] + (d - 1) * chunk[q]) * ml + m * chunk[q]
                for c in range(nc):
                    buf["es"][s, at : at + chunk[q], c] = e[:, :, lanes(c)]
    pl.semaphore_wait(barrier, len(greet) + a - 1 + b - 1)
    for s in sent:
        for q, d in first_peers():
            ship_copy(q, s, d).start()
    for c in arg_load[:2]:
        c.wait()
    for c in c_copy + w_copy:
        c.start()

    load(2, buf["iv"], buf["iv"]).wait()
    flat_iv = buf["iv"].reshape(steps * both_q * nc * rows, LANES)

    @pl.loop(0, steps * both_q // 8)
    def _(j):
        for c in range(nc):
            for r in range(rows):
                ov[1 + r, pl.ds(pl.multiple_of(j * 8, 8), 8), lanes(c)] = flat_iv[
                    pl.ds(j * (8 * nc * rows) + c * rows + r, 8, stride=nc * rows), :
                ]

    for c in o_copy:
        c.start()
    for c in arg_load[2:]:
        c.wait()
    coef = buf["coef"]
    sub = lax.broadcasted_iota(jnp.int32, (8, LANES), 0)
    for q in range(2):

        @pl.loop(0, size[q] // 8)
        def _(j):
            s = j // (chunk[q] // 8)
            at = pl.multiple_of(s * both_q + lead[q] + (j % (chunk[q] // 8)) * 8, 8)
            k = start_of(q, fi[q], 0) + j * 8
            for kind, value in enumerate((
                lambda i: advect[0, i], lambda i: advect[1, i], lambda i: damping[i]
            )):
                v = jnp.full((8, LANES), value(k), jnp.float32)
                for i in range(1, 8):
                    v = jnp.where(sub == i, value(k + i), v)
                coef[kind, pl.ds(at, 8)] = v

    rates = jnp.concatenate(
        [jnp.full((3 * rows, ny), spread[band[m]], jnp.float32) for m in range(ml)], axis=0
    )
    arrived("control", 0, buf["ch"])
    field = []
    for m in range(ml):
        field += [buf["ch"][0, m], control[m], buf["ch"][1, m]]
    field = sweeps(jnp.concatenate(field, axis=0), rates)
    for m in range(ml):
        center = field[(3 * m + 1) * rows : (3 * m + 2) * rows]
        loc[m] = center
        scl[m] = weights[m] * center
        proj[m] = jnp.zeros_like(center)
        for q, d in first_peers():
            buf["pp"][slot(q, d), m] = jnp.zeros_like(center)
    if sent:
        for q, d in first_peers():
            scl_copy(q, d).start()
    where = e_v.at[:, pl.ds(0, vl - early_planes)]
    load(1, where, where).wait()

    def own_sum(q, owner, s, c):
        where = pl.ds(start_of(q, owner, s), chunk[q])
        total = None
        for m in range(ml):
            term = e_v[m, where, :, lanes(c)].astype(jnp.float32) * scl[m, :, lanes(c)][None]
            total = term if total is None else total + term
        return total

    for s in lone:
        for q, d in first_peers():
            for c in range(nc):
                buf["to"][s - ship, block1(q, d), c] = own_sum(q, ahead(q, d), s, c)
            part_copy(q, s, d).start()
    for s in range(steps):
        for q in range(2):
            for c in range(nc):
                buf["part"][own(q, s), c] = own_sum(q, fi[q], s, c)
    arrived("weight", 0, buf["wh"])
    wb = buf["wb"]
    wb[0] = jnp.broadcast_to(buf["wh"][0, rows - 1 :], (8, ny))
    wb[rows + 1] = jnp.broadcast_to(buf["wh"][1, :1], (8, ny))
    for r in range(rows):
        wb[1 + r] = jnp.broadcast_to(obs[r : r + 1], (8, ny))

    def add_first(s):
        if some_first:
            if s >= ship:
                arrived("part", s - ship, buf["r1"].at[s - ship])
            else:
                arrived("ship", s, buf["er"].at[s])
        for q in range(2):
            for c in range(nc):
                total = buf["part"][own(q, s), c]
                for d in range(1, first[q]):
                    if s >= ship:
                        total = total + buf["r1"][s - ship, block1(q, d), c]
                    else:
                        for m in range(ml):
                            at = (lead1[q] + (d - 1) * chunk[q]) * ml + m * chunk[q]
                            total = total + (
                                buf["er"][s, at : at + chunk[q], c]
                                * buf["sr"][slot(q, d), m, :, lanes(c)][None]
                            )
                buf["part"][own(q, s), c] = total
            for d in range(1, second[q]):
                swap_copy(q, s, d).start()

    def add_second(s):
        if some_second:
            arrived("swap", s, buf["r2"].at[s])
        rows_of = lambda planes: planes * nc * rows
        flat = buf["part"].reshape(rows_of(steps * both_q), LANES)
        for q in range(2):
            peers = [
                buf["r2"].at[s, block2(q, d)].reshape(rows_of(chunk[q]), LANES)
                for d in range(1, second[q])
            ]
            base = s * both_q + lead[q]

            @pl.loop(0, chunk[q] // 8)
            def _(j):
                for c in range(nc):
                    for r in range(rows):
                        at = j * rows_of(8) + c * rows + r
                        total = flat[pl.ds(rows_of(base) + at, 8, stride=nc * rows), :]
                        for p in peers:
                            total = total + p[pl.ds(at, 8, stride=nc * rows), :]
                        ip[2 + r, pl.ds(pl.multiple_of(base + j * 8, 8), 8), lanes(c)] = total

        for c in halo(s):
            c.start()

    def adjoint(s):
        arrived("halo", s, ip.at[pl.ds(0, 4), pl.ds(s * both_q, both_q)])
        col = lax.broadcasted_iota(jnp.int32, (8, ny), 1)
        flat = buf["grad"].reshape(steps * both_q * nc * rows, LANES)

        @pl.loop(0, both_q // 8)
        def _(j):
            where = pl.ds(pl.multiple_of(s * both_q + j * 8, 8), 8)
            ax, ay, e = (jnp.concatenate([coef[k, where]] * nc, axis=1) for k in range(3))
            mid = 1.0 - 4.0 * e
            up = e - 0.5 * ax
            down = e + 0.5 * ax
            left_c = e - 0.5 * ay
            right_c = e + 0.5 * ay
            north1 = jnp.where(col == ny - 1, 0.0, left_c)
            south1 = jnp.where(col == 0, 0.0, right_c)
            north2 = jnp.where(col == ny - 1, 0.0, right_c)
            south2 = jnp.where(col == 0, 0.0, left_c)

            def turn(f):
                return pltpu.roll(f, ny - 1, 1), pltpu.roll(f, 1, 1)

            f = [ip[r, where, :] for r in range(rows + 4)]
            w = []
            for r in range(1, rows + 3):
                north, south = turn(f[r])
                d = (
                    mid * f[r] + up * f[r + 1] + down * f[r - 1]
                    + north1 * north + south1 * south
                )
                w.append(wb[r - 1] * (d - ov[r - 1, where, :]))
            for r in range(1, rows + 1):
                north, south = turn(w[r])
                g = (
                    mid * w[r] + down * w[r + 1] + up * w[r - 1]
                    + north2 * north + south2 * south
                )
                for c in range(nc):
                    at = (s * both_q + j * 8) * (nc * rows) + c * rows + r - 1
                    flat[pl.ds(at, 8, stride=nc * rows), :] = g[:, lanes(c)]

        if s >= ship:
            for q, d in first_peers():
                grad_copy(q, s, d).start()

    def project_own(s):
        for q in range(2):
            where = pl.ds(start_of(q, fi[q], s), chunk[q])
            for c in range(nc):
                g = buf["grad"][own(q, s), c]
                for m in range(ml):
                    e = e_v[m, where, :, lanes(c)].astype(jnp.float32)
                    proj[m, :, lanes(c)] += jnp.sum(e * g, axis=0)
                if s < ship:
                    for d in range(1, first[q]):
                        for m in range(ml):
                            at = (lead1[q] + (d - 1) * chunk[q]) * ml + m * chunk[q]
                            e = buf["er"][s, at : at + chunk[q], c]
                            buf["pp"][slot(q, d), m, :, lanes(c)] += jnp.sum(e * g, axis=0)

    def project_in(s):
        arrived("grad", s - ship, buf["gr"].at[s - ship])
        for q, d in first_peers():
            where = pl.ds(start_of(q, behind(q, d), s), chunk[q])
            for c in range(nc):
                g = buf["gr"][s - ship, block1(q, d), c]
                for m in range(ml):
                    e = e_v[m, where, :, lanes(c)].astype(jnp.float32)
                    proj[m, :, lanes(c)] += jnp.sum(e * g, axis=0)

    scope = jax.named_scope
    if sent:
        arrived("scl", 0, buf["sr"])
    for s in order:
        with scope(f"add_first{s}"):
            add_first(s)
    for tick in range(steps + LAG):
        if tick < steps:
            with scope(f"add_second{order[tick]}"):
                add_second(order[tick])
        if tick == LAG:
            arrived("innov", 0, ov.at[pl.ds(0, 2)])
        if tick >= LAG:
            s = order[tick - LAG]
            with scope(f"adjoint{s}"):
                adjoint(s)
            with scope(f"project_own{s}"):
                project_own(s)
            if sent and s == ship - 1:
                for q, d in first_peers():
                    proj_copy(q, d).start()
    if some_first:
        for s in lone:
            with scope(f"project_in{s}"):
                project_in(s)
    with scope("tail"):
        if sent:
            left("scl", buf["sr"])
            arrived("proj", 0, buf["pr"])
        for m in range(ml):
            total = proj[m]
            if sent:
                for q, d in first_peers():
                    total = total + buf["pr"][slot(q, d), m]
            proj[m] = total
            scl[m] = weights[m] * total
    with scope("halo_out"):
        for c in p_copy:
            c.start()
        gwr = buf["gwr"]
        row = lax.broadcasted_iota(jnp.int32, (8, LANES), 0)
        sums = jnp.zeros((8, LANES), jnp.float32)
        for m in range(ml):
            v = jnp.sum(loc[m] * proj[m], axis=0, keepdims=True)
            v = sum(v[:, lanes(c)] for c in range(nc))
            sums = jnp.where(row == m, jnp.broadcast_to(v, (8, LANES)), sums)
        gwr[t] = sums
        for d in range(1, tiles):
            remote("gw", 0, gwr.at[t], gwr.at[t], "tile", (t + d) % tiles).start()
        left("control", buf["ch"])
        left("weight", buf["wh"])
        left("innov", ov.at[pl.ds(0, 2)])
        left("halo", ip.at[pl.ds(0, 4)])
        if some_second:
            left("swap", buf["r2"])
        if some_first:
            left("part", buf["r1"])
            left("grad", buf["gr"])
        if sent:
            left("ship", buf["er"])
            left("proj", buf["pr"])
        arrived("field", 0, buf["ph"])
    with scope("sweeps"):
        field = []
        for m in range(ml):
            field += [buf["ph"][0, m], scl[m], buf["ph"][1, m]]
        field = sweeps(jnp.concatenate(field, axis=0), rates)
        for m in range(ml):
            out[m] = control[m] + field[(3 * m + 1) * rows : (3 * m + 2) * rows]
    with scope("finish"):
        if tiles > 1:
            arrived("gw", 0, gwr.at[pl.ds(0, tiles - 1)])
        total = gwr[0]
        for d in range(1, tiles):
            total = total + gwr[d]
        gw_out[...] = jnp.broadcast_to(jnp.sum(total, axis=1, keepdims=True), (8, LANES))
        left("field", buf["ph"])
        if tiles > 1:
            left("gw", gwr.at[pl.ds(0, tiles - 1)])


def per_device(
    n, tiles,
    ensemble, control, weights, member_band, spread, advect, damping, innovation, obs_weight
):
    ml, vl, rows, ny = ensemble.shape
    a, b = factors(n)
    first, second = (b, a), (a, b)
    assert rows == SWEEPS and ny % LANES == 0 and ml <= 8 and vl % (16 * b) == 0
    assert tiles > 2
    nc = ny // LANES
    size = [vl // (2 * f) for f in first]
    steps = max(d for d in range(1, CHUNKS + 1) if all(k % (8 * d) == 0 for k in size))
    ship = steps * SHIPPED // CHUNKS
    chunk = [k // steps for k in size]
    f32 = jnp.float32
    dma = pltpu.SemaphoreType.DMA
    hbm = pl.BlockSpec(memory_space=pl.ANY)
    whole = pl.BlockSpec(memory_space=pltpu.VMEM)
    field = (rows, ny)
    tile = (nc, rows, LANES)
    vmem = lambda *shape: pltpu.VMEM(shape, f32)
    links = max(sum(f - 1 for f in first), 1)
    block1 = max(sum((f - 1) * k for f, k in zip(first, chunk)), 8)
    block2 = max(sum((g - 1) * k for g, k in zip(second, chunk)), 8)
    ns, nl = max(ship, 1), max(steps - ship, 1)
    total = sum(size)
    buf = {
        "es": vmem(ns, ml * block1, *tile),
        "er": vmem(ns, ml * block1, *tile),
        "to": vmem(nl, block1, *tile),
        "r1": vmem(nl, block1, *tile),
        "part": vmem(total, *tile),
        "r2": vmem(steps, block2, *tile),
        "grad": vmem(total, *tile),
        "gr": vmem(nl, block1, *tile),
        "iv": vmem(total, *tile),
        "ip": vmem(rows + 4, total, ny),
        "ov": vmem(rows + 2, total, ny),
        "coef": vmem(3, total, LANES),
        "pp": vmem(links, ml, *field),
        "pr": vmem(links, ml, *field),
        "sr": vmem(links, ml, *field),
        "loc": vmem(ml, *field),
        "scl": vmem(ml, *field),
        "proj": vmem(ml, *field),
        "ch": vmem(2, ml, *field),
        "wh": vmem(2, *field),
        "wb": vmem(rows + 2, 8, ny),
        "ph": vmem(2, ml, *field),
        "gwr": vmem(tiles, 8, LANES),
    }
    pair = lambda k: (dma((1,)), dma((k,)))
    sems = {
        "ship": pair(ns), "scl": pair(1), "part": pair(nl), "swap": pair(steps),
        "grad": pair(nl), "proj": pair(1), "control": pair(1), "weight": pair(1),
        "innov": pair(1), "field": pair(1), "halo": pair(steps), "gw": pair(1),
    }
    args = (
        vmem(*control.shape),
        vmem(*obs_weight.shape),
        pltpu.SMEM(weights.shape, f32),
        pltpu.SMEM(member_band.shape, member_band.dtype),
        pltpu.SMEM(spread.shape, f32),
        pltpu.SMEM(advect.shape, f32),
        pltpu.SMEM(damping.shape, f32),
    )
    out, gw = pl.pallas_call(
        functools.partial(kernel, n, tiles, steps, ship),
        out_shape=(pltpu.VMEM((ml, rows, ny), f32), pltpu.VMEM((8, LANES), f32)),
        in_specs=[hbm] * 9,
        out_specs=(whole, whole),
        scratch_shapes=[args, dma((10,)), pltpu.VMEM((ml, vl) + field, ensemble.dtype), buf, sems],
        compiler_params=pltpu.CompilerParams(
            collective_id=0, has_side_effects=True, vmem_limit_bytes=63 * 1024 * 1024
        ),
    )(ensemble, control, weights, member_band, spread, advect, damping, innovation, obs_weight)
    total_cells = tiles * rows * ny * vl
    return out, gw[:ml, 0] / math.sqrt(total_cells)


def solution(mesh):
    in_specs = (
        P("mem", None, "tile", None),
        P("mem", "tile", None),
        P("mem"),
        P("mem"),
        P(),
        P(),
        P(),
        P(None, "tile", None),
        P("tile", None),
    )
    out_specs = (P("mem", "tile", None), P("mem"))
    return jax.shard_map(
        functools.partial(per_device, mesh.shape["mem"], mesh.shape["tile"]),
        mesh=mesh, in_specs=in_specs, out_specs=out_specs, check_vma=False,
    )
```

```python
import functools
import math

import jax
import jax.numpy as jnp
from jax import lax
from jax.experimental import pallas as pl
from jax.experimental.pallas import tpu as pltpu
from jax.sharding import PartitionSpec as P

SWEEPS = 8
CHUNKS = 4
SHIPPED = 1
AFTER = 9
LAG = 1
LANES = 128
MESH = pl.DeviceIdType.MESH


def factors(n):
    a = max(d for d in range(1, n + 1) if n % d == 0 and d * d <= n)
    return a, n // a


def y_pair(f):
    ny = f.shape[-1]
    col = lax.broadcasted_iota(jnp.int32, f.shape, 1)
    north = jnp.where(col == ny - 1, 0.0, pltpu.roll(f, ny - 1, 1))
    south = jnp.where(col == 0, 0.0, pltpu.roll(f, 1, 1))
    return north, south


def sweeps(f, rates):
    rows = f.shape[0]
    for _ in range(SWEEPS):
        north, south = y_pair(f)
        east = pltpu.roll(f, rows - 1, 0)
        west = pltpu.roll(f, 1, 0)
        f = f + rates * (east + west + north + south - 4.0 * f)
    return f


def kernel(
    n, tiles, steps, ship,
    ens, control_h, weights_h, band_h, spread_h, advect_h, damping_h, innov, obs_h,
    out, gw_out,
    args, arg_sem, e_v, buf, sems,
):
    a, b = factors(n)
    control, obs, weights, band, spread, advect, damping = args
    loc, scl, proj = buf["loc"], buf["scl"], buf["proj"]
    ml, rows, ny = control.shape
    vl = ens.shape[1]
    nc = ny // LANES
    me = lax.axis_index("mem")
    t = lax.axis_index("tile")
    nxt = (t + 1) % tiles
    prv = (t + tiles - 1) % tiles
    ia = me // b
    ib = me % b
    first = (b, a)
    second = (a, b)
    fi = (ib, ia)
    gi = (ia, ib)
    size = [vl // (2 * f) for f in first]
    chunk = [k // steps for k in size]
    both_q = sum(chunk)
    lead = (0, chunk[0])
    lead1 = (0, (first[0] - 1) * chunk[0])
    lead2 = (0, (second[0] - 1) * chunk[0])
    some_first = sum(f - 1 for f in first) > 0
    some_second = sum(g - 1 for g in second) > 0
    lone = tuple(range(ship, steps))
    sent = tuple(range(ship)) if some_first else ()
    order = lone[:AFTER] + tuple(range(ship)) + lone[AFTER:]
    near = tiles // 2 <= 2 + steps
    greet = sorted({1, tiles - 1}) if near else list(range(1, tiles))
    greet = [d for d in greet if d % tiles]

    def device(q, f, g):
        return g * b + f if q == 0 else f * b + g

    def start_of(q, owner, s):
        return pl.multiple_of(q * (vl // 2) + (owner * steps + s) * chunk[q], chunk[q])

    def ahead(q, d):
        return (fi[q] + d) % first[q]

    def behind(q, d):
        return (fi[q] + first[q] - d) % first[q]

    def to_first(q, d):
        return device(q, ahead(q, d), gi[q])

    def back_first(q, d):
        return device(q, behind(q, d), gi[q])

    def to_second(q, d):
        return device(q, fi[q], (gi[q] + d) % second[q])

    def first_peers():
        return [(q, d) for q in range(2) for d in range(1, first[q])]

    def second_peers():
        return [(q, d) for q in range(2) for d in range(1, second[q])]

    def remote(kind, index, src, dst, axis, dev):
        s_sem, r_sem = sems[kind]
        return pltpu.make_async_remote_copy(
            src_ref=src, dst_ref=dst, send_sem=s_sem.at[0], recv_sem=r_sem.at[index],
            device_id={axis: dev}, device_id_type=MESH,
        )

    def arrived(kind, index, ref):
        remote(kind, index, ref, ref, "tile", nxt).wait_recv()

    def left(kind, ref):
        remote(kind, 0, ref, ref, "tile", nxt).wait_send()

    def lanes(c):
        return slice(c * LANES, (c + 1) * LANES)

    barrier = pltpu.get_barrier_semaphore()
    for q, d in first_peers():
        pl.semaphore_signal(
            barrier, inc=1, device_id={"mem": to_first(q, d)}, device_id_type=MESH
        )
    for d in greet:
        pl.semaphore_signal(
            barrier, inc=1, device_id={"tile": (t + d) % tiles}, device_id_type=MESH
        )

    def load(k, src, dst):
        return pltpu.make_async_copy(src, dst, arg_sem.at[k])

    def ens_load(k, q, owner, s, count):
        where = pl.ds(start_of(q, owner, s), count * chunk[q])
        return load(k, ens.at[:, where], e_v.at[:, where])

    early = [ens_load(0, q, ahead(q, d), 0, ship) for q, d in first_peers() if ship]
    late = [ens_load(1, q, fi[q], 0, steps) for q in range(2)]
    late += [ens_load(1, q, ahead(q, d), ship, steps - ship) for q, d in first_peers()]
    innov_load = [
        load(
            2,
            innov.at[pl.ds(start_of(q, fi[q], s), chunk[q]), :, lanes(c)],
            buf["iv"].at[pl.ds(s * both_q + lead[q], chunk[q]), c],
        )
        for s in range(steps)
        for q in range(2)
        for c in range(nc)
    ]
    arg_load = [
        load(3 + i, src, dst)
        for i, (src, dst) in enumerate((
            (control_h, control), (obs_h, obs), (weights_h, weights), (band_h, band),
            (spread_h, spread), (advect_h, advect), (damping_h, damping),
        ))
    ]
    for c in early + arg_load + innov_load + late:
        c.start()
    early_planes = ship * sum((first[q] - 1) * chunk[q] for q in range(2))

    def block1(q, d, per=1):
        return pl.ds((lead1[q] + (d - 1) * chunk[q]) * per, chunk[q] * per)

    def block2(q, d):
        return pl.ds(lead2[q] + (d - 1) * chunk[q], chunk[q])

    def own(q, s):
        return pl.ds(s * both_q + lead[q], chunk[q])

    def slot(q, d):
        return (first[0] - 1) * q + d - 1

    def ship_copy(q, s, d):
        where = block1(q, d, ml)
        return remote(
            "ship", s, buf["es"].at[s, where], buf["er"].at[s, where], "mem", to_first(q, d)
        )

    def scl_copy(q, d):
        return remote("scl", 0, scl, buf["sr"].at[slot(q, d)], "mem", to_first(q, d))

    def part_copy(q, s, d):
        where = block1(q, d)
        return remote(
            "part", s - ship, buf["to"].at[s - ship, where], buf["r1"].at[s - ship, where],
            "mem", to_first(q, d),
        )

    def swap_copy(q, s, d):
        return remote(
            "swap", s, buf["part"].at[own(q, s)], buf["r2"].at[s, block2(q, d)],
            "mem", to_second(q, d),
        )

    def grad_copy(q, s, d):
        return remote(
            "grad", s - ship, buf["grad"].at[own(q, s)], buf["gr"].at[s - ship, block1(q, d)],
            "mem", to_first(q, d),
        )

    def proj_copy(q, d):
        return remote(
            "proj", 0, buf["pp"].at[slot(q, d)], buf["pr"].at[slot(q, d)],
            "mem", back_first(q, d),
        )

    def to_both(kind, src, dst):
        return (
            remote(kind, 0, src, dst.at[0], "tile", nxt),
            remote(kind, 0, src, dst.at[1], "tile", prv),
        )

    ip, ov = buf["ip"], buf["ov"]

    def halo(s):
        where = pl.ds(s * both_q, both_q)
        return (
            remote("halo", s, ip.at[pl.ds(rows, 2), where], ip.at[pl.ds(0, 2), where], "tile", nxt),
            remote("halo", s, ip.at[pl.ds(2, 2), where], ip.at[pl.ds(rows + 2, 2), where], "tile", prv),
        )

    c_copy = to_both("control", control, buf["ch"])
    w_copy = to_both("weight", obs, buf["wh"])
    p_copy = to_both("field", scl, buf["ph"])
    o_copy = (
        remote("innov", 0, ov.at[rows], ov.at[0], "tile", nxt),
        remote("innov", 0, ov.at[1], ov.at[rows + 1], "tile", prv),
    )

    if sent:
        where = e_v.at[:, pl.ds(0, early_planes)]
        load(0, where, where).wait()
    for s in sent:
        for q, d in first_peers():
            where = pl.ds(start_of(q, ahead(q, d), s), chunk[q])
            for m in range(ml):
                e = e_v[m, where].astype(jnp.float32)
                at = (lead1[q] + (d - 1) * chunk[q]) * ml + m * chunk[q]
                for c in range(nc):
                    buf["es"][s, at : at + chunk[q], c] = e[:, :, lanes(c)]
    pl.semaphore_wait(barrier, len(greet) + a - 1 + b - 1)
    for s in sent:
        for q, d in first_peers():
            ship_copy(q, s, d).start()
    for c in arg_load[:2]:
        c.wait()
    for c in c_copy + w_copy:
        c.start()

    load(2, buf["iv"], buf["iv"]).wait()
    flat_iv = buf["iv"].reshape(steps * both_q * nc * rows, LANES)

    @pl.loop(0, steps * both_q // 8)
    def _(j):
        for c in range(nc):
            for r in range(rows):
                ov[1 + r, pl.ds(pl.multiple_of(j * 8, 8), 8), lanes(c)] = flat_iv[
                    pl.ds(j * (8 * nc * rows) + c * rows + r, 8, stride=nc * rows), :
                ]

    for c in o_copy:
        c.start()
    for c in arg_load[2:]:
        c.wait()
    coef = buf["coef"]
    sub = lax.broadcasted_iota(jnp.int32, (8, LANES), 0)
    for q in range(2):

        @pl.loop(0, size[q] // 8)
        def _(j):
            s = j // (chunk[q] // 8)
            at = pl.multiple_of(s * both_q + lead[q] + (j % (chunk[q] // 8)) * 8, 8)
            k = start_of(q, fi[q], 0) + j * 8
            for kind, value in enumerate((
                lambda i: advect[0, i], lambda i: advect[1, i], lambda i: damping[i]
            )):
                v = jnp.full((8, LANES), value(k), jnp.float32)
                for i in range(1, 8):
                    v = jnp.where(sub == i, value(k + i), v)
                coef[kind, pl.ds(at, 8)] = v

    rates = jnp.concatenate(
        [jnp.full((3 * rows, ny), spread[band[m]], jnp.float32) for m in range(ml)], axis=0
    )
    arrived("control", 0, buf["ch"])
    field = []
    for m in range(ml):
        field += [buf["ch"][0, m], control[m], buf["ch"][1, m]]
    field = sweeps(jnp.concatenate(field, axis=0), rates)
    for m in range(ml):
        center = field[(3 * m + 1) * rows : (3 * m + 2) * rows]
        loc[m] = center
        scl[m] = weights[m] * center
        proj[m] = jnp.zeros_like(center)
        for q, d in first_peers():
            buf["pp"][slot(q, d), m] = jnp.zeros_like(center)
    if sent:
        for q, d in first_peers():
            scl_copy(q, d).start()
    where = e_v.at[:, pl.ds(0, vl - early_planes)]
    load(1, where, where).wait()

    def own_sum(q, owner, s, c):
        where = pl.ds(start_of(q, owner, s), chunk[q])
        total = None
        for m in range(ml):
            term = e_v[m, where, :, lanes(c)].astype(jnp.float32) * scl[m, :, lanes(c)][None]
            total = term if total is None else total + term
        return total

    for s in lone:
        for q, d in first_peers():
            for c in range(nc):
                buf["to"][s - ship, block1(q, d), c] = own_sum(q, ahead(q, d), s, c)
            part_copy(q, s, d).start()
    for s in range(steps):
        for q in range(2):
            for c in range(nc):
                buf["part"][own(q, s), c] = own_sum(q, fi[q], s, c)
    arrived("weight", 0, buf["wh"])
    wb = buf["wb"]
    wb[0] = jnp.broadcast_to(buf["wh"][0, rows - 1 :], (8, ny))
    wb[rows + 1] = jnp.broadcast_to(buf["wh"][1, :1], (8, ny))
    for r in range(rows):
        wb[1 + r] = jnp.broadcast_to(obs[r : r + 1], (8, ny))

    def add_first(s):
        if some_first:
            if s >= ship:
                arrived("part", s - ship, buf["r1"].at[s - ship])
            else:
                arrived("ship", s, buf["er"].at[s])
        for q in range(2):
            for c in range(nc):
                total = buf["part"][own(q, s), c]
                for d in range(1, first[q]):
                    if s >= ship:
                        total = total + buf["r1"][s - ship, block1(q, d), c]
                    else:
                        for m in range(ml):
                            at = (lead1[q] + (d - 1) * chunk[q]) * ml + m * chunk[q]
                            total = total + (
                                buf["er"][s, at : at + chunk[q], c]
                                * buf["sr"][slot(q, d), m, :, lanes(c)][None]
                            )
                buf["part"][own(q, s), c] = total
            for d in range(1, second[q]):
                swap_copy(q, s, d).start()

    def add_second(s):
        if some_second:
            arrived("swap", s, buf["r2"].at[s])
        rows_of = lambda planes: planes * nc * rows
        flat = buf["part"].reshape(rows_of(steps * both_q), LANES)
        for q in range(2):
            peers = [
                buf["r2"].at[s, block2(q, d)].reshape(rows_of(chunk[q]), LANES)
                for d in range(1, second[q])
            ]
            base = s * both_q + lead[q]

            @pl.loop(0, chunk[q] // 8)
            def _(j):
                for c in range(nc):
                    for r in range(rows):
                        at = j * rows_of(8) + c * rows + r
                        total = flat[pl.ds(rows_of(base) + at, 8, stride=nc * rows), :]
                        for p in peers:
                            total = total + p[pl.ds(at, 8, stride=nc * rows), :]
                        ip[2 + r, pl.ds(pl.multiple_of(base + j * 8, 8), 8), lanes(c)] = total

        for c in halo(s):
            c.start()

    def adjoint(s):
        arrived("halo", s, ip.at[pl.ds(0, 4), pl.ds(s * both_q, both_q)])
        col = lax.broadcasted_iota(jnp.int32, (8, ny), 1)
        flat = buf["grad"].reshape(steps * both_q * nc * rows, LANES)

        @pl.loop(0, both_q // 8)
        def _(j):
            where = pl.ds(pl.multiple_of(s * both_q + j * 8, 8), 8)
            ax, ay, e = (jnp.concatenate([coef[k, where]] * nc, axis=1) for k in range(3))
            mid = 1.0 - 4.0 * e
            up = e - 0.5 * ax
            down = e + 0.5 * ax
            left_c = e - 0.5 * ay
            right_c = e + 0.5 * ay
            north1 = jnp.where(col == ny - 1, 0.0, left_c)
            south1 = jnp.where(col == 0, 0.0, right_c)
            north2 = jnp.where(col == ny - 1, 0.0, right_c)
            south2 = jnp.where(col == 0, 0.0, left_c)

            def turn(f):
                return pltpu.roll(f, ny - 1, 1), pltpu.roll(f, 1, 1)

            f = [ip[r, where, :] for r in range(rows + 4)]
            w = []
            for r in range(1, rows + 3):
                north, south = turn(f[r])
                d = (
                    mid * f[r] + up * f[r + 1] + down * f[r - 1]
                    + north1 * north + south1 * south
                )
                w.append(wb[r - 1] * (d - ov[r - 1, where, :]))
            for r in range(1, rows + 1):
                north, south = turn(w[r])
                g = (
                    mid * w[r] + down * w[r + 1] + up * w[r - 1]
                    + north2 * north + south2 * south
                )
                for c in range(nc):
                    at = (s * both_q + j * 8) * (nc * rows) + c * rows + r - 1
                    flat[pl.ds(at, 8, stride=nc * rows), :] = g[:, lanes(c)]

        if s >= ship:
            for q, d in first_peers():
                grad_copy(q, s, d).start()

    def project_own(s):
        for q in range(2):
            where = pl.ds(start_of(q, fi[q], s), chunk[q])
            for c in range(nc):
                g = buf["grad"][own(q, s), c]
                for m in range(ml):
                    e = e_v[m, where, :, lanes(c)].astype(jnp.float32)
                    proj[m, :, lanes(c)] += jnp.sum(e * g, axis=0)
                if s < ship:
                    for d in range(1, first[q]):
                        for m in range(ml):
                            at = (lead1[q] + (d - 1) * chunk[q]) * ml + m * chunk[q]
                            e = buf["er"][s, at : at + chunk[q], c]
                            buf["pp"][slot(q, d), m, :, lanes(c)] += jnp.sum(e * g, axis=0)

    def project_in(s):
        arrived("grad", s - ship, buf["gr"].at[s - ship])
        for q, d in first_peers():
            where = pl.ds(start_of(q, behind(q, d), s), chunk[q])
            for c in range(nc):
                g = buf["gr"][s - ship, block1(q, d), c]
                for m in range(ml):
                    e = e_v[m, where, :, lanes(c)].astype(jnp.float32)
                    proj[m, :, lanes(c)] += jnp.sum(e * g, axis=0)

    scope = jax.named_scope
    if sent:
        arrived("scl", 0, buf["sr"])
    for s in order:
        with scope(f"add_first{s}"):
            add_first(s)
    for tick in range(steps + LAG):
        if tick < steps:
            with scope(f"add_second{order[tick]}"):
                add_second(order[tick])
        if tick == LAG:
            arrived("innov", 0, ov.at[pl.ds(0, 2)])
        if tick >= LAG:
            s = order[tick - LAG]
            with scope(f"adjoint{s}"):
                adjoint(s)
            with scope(f"project_own{s}"):
                project_own(s)
            if sent and s == ship - 1:
                for q, d in first_peers():
                    proj_copy(q, d).start()
    if some_first:
        for s in lone:
            with scope(f"project_in{s}"):
                project_in(s)
    with scope("tail"):
        if sent:
            left("scl", buf["sr"])
            arrived("proj", 0, buf["pr"])
        for m in range(ml):
            total = proj[m]
            if sent:
                for q, d in first_peers():
                    total = total + buf["pr"][slot(q, d), m]
            proj[m] = total
            scl[m] = weights[m] * total
    with scope("halo_out"):
        for c in p_copy:
            c.start()
        gwr = buf["gwr"]
        row = lax.broadcasted_iota(jnp.int32, (8, LANES), 0)
        sums = jnp.zeros((8, LANES), jnp.float32)
        for m in range(ml):
            v = jnp.sum(loc[m] * proj[m], axis=0, keepdims=True)
            v = sum(v[:, lanes(c)] for c in range(nc))
            sums = jnp.where(row == m, jnp.broadcast_to(v, (8, LANES)), sums)
        gwr[t] = sums
        for d in range(1, tiles):
            remote("gw", 0, gwr.at[t], gwr.at[t], "tile", (t + d) % tiles).start()
        left("control", buf["ch"])
        left("weight", buf["wh"])
        left("innov", ov.at[pl.ds(0, 2)])
        left("halo", ip.at[pl.ds(0, 4)])
        if some_second:
            left("swap", buf["r2"])
        if some_first:
            left("part", buf["r1"])
            left("grad", buf["gr"])
        if sent:
            left("ship", buf["er"])
            left("proj", buf["pr"])
        arrived("field", 0, buf["ph"])
    with scope("sweeps"):
        field = []
        for m in range(ml):
            field += [buf["ph"][0, m], scl[m], buf["ph"][1, m]]
        field = sweeps(jnp.concatenate(field, axis=0), rates)
        for m in range(ml):
            out[m] = control[m] + field[(3 * m + 1) * rows : (3 * m + 2) * rows]
    with scope("finish"):
        if tiles > 1:
            arrived("gw", 0, gwr.at[pl.ds(0, tiles - 1)])
        total = gwr[0]
        for d in range(1, tiles):
            total = total + gwr[d]
        sums = jnp.broadcast_to(jnp.sum(total, axis=1, keepdims=True), (8, LANES))
        row = lax.broadcasted_iota(jnp.int32, (8, LANES), 0)
        lane = lax.broadcasted_iota(jnp.int32, (8, LANES), 1)
        sums = jnp.sum(jnp.where(row == lane, sums, 0.0), axis=0)
        gw_out[...] = sums[:ml] / math.sqrt(tiles * rows * ny * vl)
        left("field", buf["ph"])
        if tiles > 1:
            left("gw", gwr.at[pl.ds(0, tiles - 1)])


def store(field, sums, out, gw, sem):
    copies = [
        pltpu.make_async_copy(src, dst, sem.at[i])
        for i, (src, dst) in enumerate(((field, out), (sums, gw)))
    ]
    for c in copies:
        c.start()
    for c in copies:
        c.wait()


def per_device(
    n, tiles,
    ensemble, control, weights, member_band, spread, advect, damping, innovation, obs_weight
):
    ml, vl, rows, ny = ensemble.shape
    a, b = factors(n)
    first, second = (b, a), (a, b)
    assert rows == SWEEPS and ny % LANES == 0 and ml <= 8 and vl % (16 * b) == 0
    assert tiles > 2
    nc = ny // LANES
    size = [vl // (2 * f) for f in first]
    steps = max(d for d in range(1, CHUNKS + 1) if all(k % (8 * d) == 0 for k in size))
    ship = steps * SHIPPED // CHUNKS
    chunk = [k // steps for k in size]
    f32 = jnp.float32
    dma = pltpu.SemaphoreType.DMA
    hbm = pl.BlockSpec(memory_space=pl.ANY)
    whole = pl.BlockSpec(memory_space=pltpu.VMEM)
    field = (rows, ny)
    tile = (nc, rows, LANES)
    vmem = lambda *shape: pltpu.VMEM(shape, f32)
    links = max(sum(f - 1 for f in first), 1)
    block1 = max(sum((f - 1) * k for f, k in zip(first, chunk)), 8)
    block2 = max(sum((g - 1) * k for g, k in zip(second, chunk)), 8)
    ns, nl = max(ship, 1), max(steps - ship, 1)
    total = sum(size)
    buf = {
        "es": vmem(ns, ml * block1, *tile),
        "er": vmem(ns, ml * block1, *tile),
        "to": vmem(nl, block1, *tile),
        "r1": vmem(nl, block1, *tile),
        "part": vmem(total, *tile),
        "r2": vmem(steps, block2, *tile),
        "grad": vmem(total, *tile),
        "gr": vmem(nl, block1, *tile),
        "iv": vmem(total, *tile),
        "ip": vmem(rows + 4, total, ny),
        "ov": vmem(rows + 2, total, ny),
        "coef": vmem(3, total, LANES),
        "pp": vmem(links, ml, *field),
        "pr": vmem(links, ml, *field),
        "sr": vmem(links, ml, *field),
        "loc": vmem(ml, *field),
        "scl": vmem(ml, *field),
        "proj": vmem(ml, *field),
        "ch": vmem(2, ml, *field),
        "wh": vmem(2, *field),
        "wb": vmem(rows + 2, 8, ny),
        "ph": vmem(2, ml, *field),
        "gwr": vmem(tiles, 8, LANES),
    }
    pair = lambda k: (dma((1,)), dma((k,)))
    sems = {
        "ship": pair(ns), "scl": pair(1), "part": pair(nl), "swap": pair(steps),
        "grad": pair(nl), "proj": pair(1), "control": pair(1), "weight": pair(1),
        "innov": pair(1), "field": pair(1), "halo": pair(steps), "gw": pair(1),
    }
    args = (
        vmem(*control.shape),
        vmem(*obs_weight.shape),
        pltpu.SMEM(weights.shape, f32),
        pltpu.SMEM(member_band.shape, member_band.dtype),
        pltpu.SMEM(spread.shape, f32),
        pltpu.SMEM(advect.shape, f32),
        pltpu.SMEM(damping.shape, f32),
    )
    out, gw = pl.pallas_call(
        functools.partial(kernel, n, tiles, steps, ship),
        out_shape=(pltpu.VMEM((ml, rows, ny), f32), pltpu.VMEM((ml,), f32)),
        in_specs=[hbm] * 9,
        out_specs=(whole, whole),
        scratch_shapes=[args, dma((10,)), pltpu.VMEM((ml, vl) + field, ensemble.dtype), buf, sems],
        compiler_params=pltpu.CompilerParams(
            collective_id=0, has_side_effects=True, vmem_limit_bytes=63 * 1024 * 1024
        ),
    )(ensemble, control, weights, member_band, spread, advect, damping, innovation, obs_weight)
    return pl.pallas_call(
        store,
        out_shape=(
            jax.ShapeDtypeStruct((ml, rows, ny), f32),
            jax.ShapeDtypeStruct((ml,), f32),
        ),
        in_specs=[whole, whole],
        out_specs=(hbm, hbm),
        scratch_shapes=[dma((2,))],
    )(*(pltpu.with_memory_space_constraint(x, pltpu.VMEM) for x in (out, gw)))


def solution(mesh):
    in_specs = (
        P("mem", None, "tile", None),
        P("mem", "tile", None),
        P("mem"),
        P("mem"),
        P(),
        P(),
        P(),
        P(None, "tile", None),
        P("tile", None),
    )
    out_specs = (P("mem", "tile", None), P("mem"))
    return jax.shard_map(
        functools.partial(per_device, mesh.shape["mem"], mesh.shape["tile"]),
        mesh=mesh, in_specs=in_specs, out_specs=out_specs, check_vma=False,
    )
```

```python
import functools
import math

import jax
import jax.numpy as jnp
from jax import lax
from jax.experimental import pallas as pl
from jax.experimental.pallas import tpu as pltpu
from jax.sharding import PartitionSpec as P

SWEEPS = 8
CHUNKS = 4
SHIPPED = 1
AFTER = 9
LAG = 1
LANES = 128
MESH = pl.DeviceIdType.MESH


def factors(n):
    a = max(d for d in range(1, n + 1) if n % d == 0 and d * d <= n)
    return a, n // a


def y_pair(f):
    ny = f.shape[-1]
    col = lax.broadcasted_iota(jnp.int32, f.shape, 1)
    north = jnp.where(col == ny - 1, 0.0, pltpu.roll(f, ny - 1, 1))
    south = jnp.where(col == 0, 0.0, pltpu.roll(f, 1, 1))
    return north, south


def sweeps(f, rates):
    rows = f.shape[0]
    for _ in range(SWEEPS):
        north, south = y_pair(f)
        east = pltpu.roll(f, rows - 1, 0)
        west = pltpu.roll(f, 1, 0)
        f = f + rates * (east + west + north + south - 4.0 * f)
    return f


def kernel(
    n, tiles, steps, ship,
    ens, control_h, weights_h, band_h, spread_h, advect_h, damping_h, innov, obs_h,
    out, gw_out,
    args, arg_sem, e_v, buf, sems,
):
    a, b = factors(n)
    control, obs, weights, band, spread, advect, damping = args
    loc, scl, proj = buf["loc"], buf["scl"], buf["proj"]
    ml, rows, ny = control.shape
    vl = ens.shape[1]
    nc = ny // LANES
    me = lax.axis_index("mem")
    t = lax.axis_index("tile")
    nxt = (t + 1) % tiles
    prv = (t + tiles - 1) % tiles
    ia = me // b
    ib = me % b
    first = (b, a)
    second = (a, b)
    fi = (ib, ia)
    gi = (ia, ib)
    size = [vl // (2 * f) for f in first]
    chunk = [k // steps for k in size]
    both_q = sum(chunk)
    lead = (0, chunk[0])
    lead1 = (0, (first[0] - 1) * chunk[0])
    lead2 = (0, (second[0] - 1) * chunk[0])
    some_first = sum(f - 1 for f in first) > 0
    some_second = sum(g - 1 for g in second) > 0
    lone = tuple(range(ship, steps))
    sent = tuple(range(ship)) if some_first else ()
    order = lone[:AFTER] + tuple(range(ship)) + lone[AFTER:]
    near = tiles // 2 <= 2 + steps
    greet = sorted({1, tiles - 1}) if near else list(range(1, tiles))
    greet = [d for d in greet if d % tiles]

    def device(q, f, g):
        return g * b + f if q == 0 else f * b + g

    def start_of(q, owner, s):
        return pl.multiple_of(q * (vl // 2) + (owner * steps + s) * chunk[q], chunk[q])

    def ahead(q, d):
        return (fi[q] + d) % first[q]

    def behind(q, d):
        return (fi[q] + first[q] - d) % first[q]

    def to_first(q, d):
        return device(q, ahead(q, d), gi[q])

    def back_first(q, d):
        return device(q, behind(q, d), gi[q])

    def to_second(q, d):
        return device(q, fi[q], (gi[q] + d) % second[q])

    def first_peers():
        return [(q, d) for q in range(2) for d in range(1, first[q])]

    def second_peers():
        return [(q, d) for q in range(2) for d in range(1, second[q])]

    def remote(kind, index, src, dst, axis, dev):
        return pltpu.make_async_remote_copy(
            src_ref=src, dst_ref=dst, send_sem=sems["sent"].at[0], recv_sem=sems[kind].at[index],
            device_id={axis: dev}, device_id_type=MESH,
        )

    def arrived(kind, index, ref):
        remote(kind, index, ref, ref, "tile", nxt).wait_recv()

    def lanes(c):
        return slice(c * LANES, (c + 1) * LANES)

    def load(k, src, dst):
        return pltpu.make_async_copy(src, dst, arg_sem.at[k])

    def ens_load(k, q, owner, s, count):
        where = pl.ds(start_of(q, owner, s), count * chunk[q])
        return load(k, ens.at[:, where], e_v.at[:, where])

    early = [ens_load(0, q, ahead(q, d), 0, ship) for q, d in first_peers() if ship]
    late = [ens_load(1, q, fi[q], 0, steps) for q in range(2)]
    late += [ens_load(1, q, ahead(q, d), ship, steps - ship) for q, d in first_peers()]
    innov_load = [
        load(
            2,
            innov.at[pl.ds(start_of(q, fi[q], s), chunk[q]), :, lanes(c)],
            buf["iv"].at[pl.ds(s * both_q + lead[q], chunk[q]), c],
        )
        for s in range(steps)
        for q in range(2)
        for c in range(nc)
    ]
    arg_load = [
        load(3 + i, src, dst)
        for i, (src, dst) in enumerate((
            (control_h, control), (obs_h, obs), (weights_h, weights), (band_h, band),
            (spread_h, spread), (advect_h, advect), (damping_h, damping),
        ))
    ]
    for c in early:
        c.start()
    barrier = pltpu.get_barrier_semaphore()
    for q, d in first_peers():
        pl.semaphore_signal(
            barrier, inc=1, device_id={"mem": to_first(q, d)}, device_id_type=MESH
        )
    for d in greet:
        pl.semaphore_signal(
            barrier, inc=1, device_id={"tile": (t + d) % tiles}, device_id_type=MESH
        )
    for c in arg_load + innov_load + late:
        c.start()
    early_planes = ship * sum((first[q] - 1) * chunk[q] for q in range(2))

    def block1(q, d, per=1):
        return pl.ds((lead1[q] + (d - 1) * chunk[q]) * per, chunk[q] * per)

    def block2(q, d):
        return pl.ds(lead2[q] + (d - 1) * chunk[q], chunk[q])

    def own(q, s):
        return pl.ds(s * both_q + lead[q], chunk[q])

    def slot(q, d):
        return (first[0] - 1) * q + d - 1

    def ship_copy(q, s, d):
        where = block1(q, d, ml)
        return remote(
            "ship", s, buf["es"].at[s, where], buf["er"].at[s, where], "mem", to_first(q, d)
        )

    def scl_copy(q, d):
        return remote("scl", 0, scl, buf["sr"].at[slot(q, d)], "mem", to_first(q, d))

    def part_copy(q, s, d):
        where = block1(q, d)
        return remote(
            "part", s - ship, buf["to"].at[s - ship, where], buf["r1"].at[s - ship, where],
            "mem", to_first(q, d),
        )

    def swap_copy(q, s, d):
        return remote(
            "swap", s, buf["part"].at[own(q, s)], buf["r2"].at[s, block2(q, d)],
            "mem", to_second(q, d),
        )

    def grad_copy(q, s, d):
        return remote(
            "grad", s - ship, buf["grad"].at[own(q, s)], buf["gr"].at[s - ship, block1(q, d)],
            "mem", to_first(q, d),
        )

    def proj_copy(q, d):
        return remote(
            "proj", 0, buf["pp"].at[slot(q, d)], buf["pr"].at[slot(q, d)],
            "mem", back_first(q, d),
        )

    def to_both(kind, src, dst):
        return (
            remote(kind, 0, src, dst.at[0], "tile", nxt),
            remote(kind, 0, src, dst.at[1], "tile", prv),
        )

    ip, ov = buf["ip"], buf["ov"]

    def halo(s):
        where = pl.ds(s * both_q, both_q)
        return (
            remote("halo", s, ip.at[pl.ds(rows, 2), where], ip.at[pl.ds(0, 2), where], "tile", nxt),
            remote("halo", s, ip.at[pl.ds(2, 2), where], ip.at[pl.ds(rows + 2, 2), where], "tile", prv),
        )

    c_copy = to_both("control", control, buf["ch"])
    w_copy = to_both("weight", obs, buf["wh"])
    last = buf["last"]
    p_copy = to_both("field", last, buf["ph"])
    o_copy = (
        remote("innov", 0, ov.at[rows], ov.at[0], "tile", nxt),
        remote("innov", 0, ov.at[1], ov.at[rows + 1], "tile", prv),
    )

    if sent:
        where = e_v.at[:, pl.ds(0, early_planes)]
        load(0, where, where).wait()
    for s in sent:
        for q, d in first_peers():
            where = pl.ds(start_of(q, ahead(q, d), s), chunk[q])
            for m in range(ml):
                e = e_v[m, where].astype(jnp.float32)
                at = (lead1[q] + (d - 1) * chunk[q]) * ml + m * chunk[q]
                for c in range(nc):
                    buf["es"][s, at : at + chunk[q], c] = e[:, :, lanes(c)]
    pl.semaphore_wait(barrier, len(greet) + a - 1 + b - 1)
    for s in sent:
        for q, d in first_peers():
            ship_copy(q, s, d).start()
    for c in arg_load[:2]:
        c.wait()
    for c in c_copy + w_copy:
        c.start()

    load(2, buf["iv"], buf["iv"]).wait()
    flat_iv = buf["iv"].reshape(steps * both_q * nc * rows, LANES)

    @pl.loop(0, steps * both_q // 8)
    def _(j):
        for c in range(nc):
            for r in range(rows):
                ov[1 + r, pl.ds(pl.multiple_of(j * 8, 8), 8), lanes(c)] = flat_iv[
                    pl.ds(j * (8 * nc * rows) + c * rows + r, 8, stride=nc * rows), :
                ]

    for c in o_copy:
        c.start()
    for c in arg_load[2:]:
        c.wait()
    coef = buf["coef"]
    sub = lax.broadcasted_iota(jnp.int32, (8, LANES), 0)
    for q in range(2):

        @pl.loop(0, size[q] // 8)
        def _(j):
            s = j // (chunk[q] // 8)
            at = pl.multiple_of(s * both_q + lead[q] + (j % (chunk[q] // 8)) * 8, 8)
            k = start_of(q, fi[q], 0) + j * 8
            for kind, value in enumerate((
                lambda i: advect[0, i], lambda i: advect[1, i], lambda i: damping[i]
            )):
                v = jnp.full((8, LANES), value(k), jnp.float32)
                for i in range(1, 8):
                    v = jnp.where(sub == i, value(k + i), v)
                coef[kind, pl.ds(at, 8)] = v

    rates = jnp.concatenate(
        [jnp.full((3 * rows, ny), spread[band[m]], jnp.float32) for m in range(ml)], axis=0
    )
    arrived("control", 0, buf["ch"])
    field = []
    for m in range(ml):
        field += [buf["ch"][0, m], control[m], buf["ch"][1, m]]
    field = sweeps(jnp.concatenate(field, axis=0), rates)
    for m in range(ml):
        center = field[(3 * m + 1) * rows : (3 * m + 2) * rows]
        loc[m] = center
        scl[m] = weights[m] * center
        proj[m] = jnp.zeros_like(center)
        for q, d in first_peers():
            buf["pp"][slot(q, d), m] = jnp.zeros_like(center)
    if sent:
        for q, d in first_peers():
            scl_copy(q, d).start()
    where = e_v.at[:, pl.ds(0, vl - early_planes)]
    load(1, where, where).wait()

    def own_sum(q, owner, s, c):
        where = pl.ds(start_of(q, owner, s), chunk[q])
        total = None
        for m in range(ml):
            term = e_v[m, where, :, lanes(c)].astype(jnp.float32) * scl[m, :, lanes(c)][None]
            total = term if total is None else total + term
        return total

    for s in lone:
        for q, d in first_peers():
            for c in range(nc):
                buf["to"][s - ship, block1(q, d), c] = own_sum(q, ahead(q, d), s, c)
            part_copy(q, s, d).start()
    for s in range(steps):
        for q in range(2):
            for c in range(nc):
                buf["part"][own(q, s), c] = own_sum(q, fi[q], s, c)
    arrived("weight", 0, buf["wh"])
    wb = buf["wb"]
    wb[0] = jnp.broadcast_to(buf["wh"][0, rows - 1 :], (8, ny))
    wb[rows + 1] = jnp.broadcast_to(buf["wh"][1, :1], (8, ny))
    for r in range(rows):
        wb[1 + r] = jnp.broadcast_to(obs[r : r + 1], (8, ny))

    def add_first(s):
        if some_first:
            if s >= ship:
                arrived("part", s - ship, buf["r1"].at[s - ship])
            else:
                arrived("ship", s, buf["er"].at[s])
        for q in range(2):
            for c in range(nc):
                total = buf["part"][own(q, s), c]
                for d in range(1, first[q]):
                    if s >= ship:
                        total = total + buf["r1"][s - ship, block1(q, d), c]
                    else:
                        for m in range(ml):
                            at = (lead1[q] + (d - 1) * chunk[q]) * ml + m * chunk[q]
                            total = total + (
                                buf["er"][s, at : at + chunk[q], c]
                                * buf["sr"][slot(q, d), m, :, lanes(c)][None]
                            )
                buf["part"][own(q, s), c] = total
            for d in range(1, second[q]):
                swap_copy(q, s, d).start()

    def add_second(s):
        if some_second:
            arrived("swap", s, buf["r2"].at[s])
        rows_of = lambda planes: planes * nc * rows
        flat = buf["part"].reshape(rows_of(steps * both_q), LANES)
        for q in range(2):
            peers = [
                buf["r2"].at[s, block2(q, d)].reshape(rows_of(chunk[q]), LANES)
                for d in range(1, second[q])
            ]
            base = s * both_q + lead[q]

            @pl.loop(0, chunk[q] // 8)
            def _(j):
                for c in range(nc):
                    for r in range(rows):
                        at = j * rows_of(8) + c * rows + r
                        total = flat[pl.ds(rows_of(base) + at, 8, stride=nc * rows), :]
                        for p in peers:
                            total = total + p[pl.ds(at, 8, stride=nc * rows), :]
                        ip[2 + r, pl.ds(pl.multiple_of(base + j * 8, 8), 8), lanes(c)] = total

        for c in halo(s):
            c.start()

    def adjoint(s):
        arrived("halo", s, ip.at[pl.ds(0, 4), pl.ds(s * both_q, both_q)])
        col = lax.broadcasted_iota(jnp.int32, (8, ny), 1)
        flat = buf["grad"].reshape(steps * both_q * nc * rows, LANES)

        @pl.loop(0, both_q // 8)
        def _(j):
            where = pl.ds(pl.multiple_of(s * both_q + j * 8, 8), 8)
            ax, ay, e = (jnp.concatenate([coef[k, where]] * nc, axis=1) for k in range(3))
            mid = 1.0 - 4.0 * e
            up = e - 0.5 * ax
            down = e + 0.5 * ax
            left_c = e - 0.5 * ay
            right_c = e + 0.5 * ay
            north1 = jnp.where(col == ny - 1, 0.0, left_c)
            south1 = jnp.where(col == 0, 0.0, right_c)
            north2 = jnp.where(col == ny - 1, 0.0, right_c)
            south2 = jnp.where(col == 0, 0.0, left_c)

            def turn(f):
                return pltpu.roll(f, ny - 1, 1), pltpu.roll(f, 1, 1)

            f = [ip[r, where, :] for r in range(rows + 4)]
            w = []
            for r in range(1, rows + 3):
                north, south = turn(f[r])
                d = (
                    mid * f[r] + up * f[r + 1] + down * f[r - 1]
                    + north1 * north + south1 * south
                )
                w.append(wb[r - 1] * (d - ov[r - 1, where, :]))
            for r in range(1, rows + 1):
                north, south = turn(w[r])
                g = (
                    mid * w[r] + down * w[r + 1] + up * w[r - 1]
                    + north2 * north + south2 * south
                )
                for c in range(nc):
                    at = (s * both_q + j * 8) * (nc * rows) + c * rows + r - 1
                    flat[pl.ds(at, 8, stride=nc * rows), :] = g[:, lanes(c)]

        if s >= ship:
            for q, d in first_peers():
                grad_copy(q, s, d).start()

    def project_own(s):
        for q in range(2):
            where = pl.ds(start_of(q, fi[q], s), chunk[q])
            for c in range(nc):
                g = buf["grad"][own(q, s), c]
                for m in range(ml):
                    e = e_v[m, where, :, lanes(c)].astype(jnp.float32)
                    proj[m, :, lanes(c)] += jnp.sum(e * g, axis=0)
                if s < ship:
                    for d in range(1, first[q]):
                        for m in range(ml):
                            at = (lead1[q] + (d - 1) * chunk[q]) * ml + m * chunk[q]
                            e = buf["er"][s, at : at + chunk[q], c]
                            buf["pp"][slot(q, d), m, :, lanes(c)] += jnp.sum(e * g, axis=0)

    def project_in(s):
        arrived("grad", s - ship, buf["gr"].at[s - ship])
        for q, d in first_peers():
            where = pl.ds(start_of(q, behind(q, d), s), chunk[q])
            for c in range(nc):
                g = buf["gr"][s - ship, block1(q, d), c]
                for m in range(ml):
                    e = e_v[m, where, :, lanes(c)].astype(jnp.float32)
                    proj[m, :, lanes(c)] += jnp.sum(e * g, axis=0)

    scope = jax.named_scope
    if sent:
        arrived("scl", 0, buf["sr"])
    for s in order:
        with scope(f"add_first{s}"):
            add_first(s)
    for tick in range(steps + LAG):
        if tick < steps:
            with scope(f"add_second{order[tick]}"):
                add_second(order[tick])
        if tick == LAG:
            arrived("innov", 0, ov.at[pl.ds(0, 2)])
        if tick >= LAG:
            s = order[tick - LAG]
            with scope(f"adjoint{s}"):
                adjoint(s)
            with scope(f"project_own{s}"):
                project_own(s)
            if sent and s == ship - 1:
                for q, d in first_peers():
                    proj_copy(q, d).start()
    if some_first:
        for s in lone:
            with scope(f"project_in{s}"):
                project_in(s)
    with scope("tail"):
        if sent:
            arrived("proj", 0, buf["pr"])
        for m in range(ml):
            total = proj[m]
            if sent:
                for q, d in first_peers():
                    total = total + buf["pr"][slot(q, d), m]
            proj[m] = total
            last[m] = weights[m] * total
    with scope("halo_out"):
        for c in p_copy:
            c.start()
        gwr = buf["gwr"]
        for m in range(ml):
            v = jnp.sum(loc[m] * proj[m], axis=0, keepdims=True)
            gwr[t, m : m + 1] = sum(v[:, lanes(c)] for c in range(nc))
        for d in range(1, tiles):
            remote("gw", 0, gwr.at[t], gwr.at[t], "tile", (t + d) % tiles).start()
        arrived("field", 0, buf["ph"])
    with scope("sweeps"):
        field = []
        for m in range(ml):
            field += [buf["ph"][0, m], last[m], buf["ph"][1, m]]
        field = sweeps(jnp.concatenate(field, axis=0), rates)
        for m in range(ml):
            out[m] = control[m] + field[(3 * m + 1) * rows : (3 * m + 2) * rows]
    with scope("finish"):
        if tiles > 1:
            arrived("gw", 0, gwr.at[pl.ds(0, tiles - 1)])
        total = gwr[0]
        for d in range(1, tiles):
            total = total + gwr[d]
        total = jnp.broadcast_to(jnp.sum(total, axis=1, keepdims=True), (ml, LANES))
        row = lax.broadcasted_iota(jnp.int32, (ml, LANES), 0)
        lane = lax.broadcasted_iota(jnp.int32, (ml, LANES), 1)
        sums = jnp.sum(jnp.where(row == lane, total, 0.0), axis=0)
        gw_out[...] = sums[:ml] / math.sqrt(tiles * rows * ny * vl)
        remote("gw", 0, buf["all"], buf["all"], "tile", nxt).wait_send()


def store(field, sums, out, gw, sem):
    copies = [
        pltpu.make_async_copy(src, dst, sem.at[i])
        for i, (src, dst) in enumerate(((field, out), (sums, gw)))
    ]
    for c in copies:
        c.start()
    for c in copies:
        c.wait()


def per_device(
    n, tiles,
    ensemble, control, weights, member_band, spread, advect, damping, innovation, obs_weight
):
    ml, vl, rows, ny = ensemble.shape
    a, b = factors(n)
    first, second = (b, a), (a, b)
    assert rows == SWEEPS and ny % LANES == 0 and ml <= 8 and vl % (16 * b) == 0
    assert tiles > 2
    nc = ny // LANES
    size = [vl // (2 * f) for f in first]
    steps = max(d for d in range(1, CHUNKS + 1) if all(k % (8 * d) == 0 for k in size))
    ship = steps * SHIPPED // CHUNKS
    chunk = [k // steps for k in size]
    f32 = jnp.float32
    dma = pltpu.SemaphoreType.DMA
    hbm = pl.BlockSpec(memory_space=pl.ANY)
    whole = pl.BlockSpec(memory_space=pltpu.VMEM)
    field = (rows, ny)
    tile = (nc, rows, LANES)
    vmem = lambda *shape: pltpu.VMEM(shape, f32)
    links = max(sum(f - 1 for f in first), 1)
    block1 = max(sum((f - 1) * k for f, k in zip(first, chunk)), 8)
    block2 = max(sum((g - 1) * k for g, k in zip(second, chunk)), 8)
    ns, nl = max(ship, 1), max(steps - ship, 1)
    total = sum(size)
    out1 = sum((f - 1) * k for f, k in zip(first, chunk))
    out2 = sum((g - 1) * k for g, k in zip(second, chunk))
    fields = 2 * (steps - ship) * out1 + steps * out2 + 4 * ml + 2
    if ship:
        fields += ship * ml * out1 + 2 * ml * sum(f - 1 for f in first)
    sent_rows = fields * nc * rows + 6 * total * nc + (tiles - 1) * ml
    buf = {
        "es": vmem(ns, ml * block1, *tile),
        "er": vmem(ns, ml * block1, *tile),
        "to": vmem(nl, block1, *tile),
        "r1": vmem(nl, block1, *tile),
        "part": vmem(total, *tile),
        "r2": vmem(steps, block2, *tile),
        "grad": vmem(total, *tile),
        "gr": vmem(nl, block1, *tile),
        "iv": vmem(total, *tile),
        "ip": vmem(rows + 4, total, ny),
        "ov": vmem(rows + 2, total, ny),
        "coef": vmem(3, total, LANES),
        "pp": vmem(links, ml, *field),
        "pr": vmem(links, ml, *field),
        "sr": vmem(links, ml, *field),
        "loc": vmem(ml, *field),
        "scl": vmem(ml, *field),
        "proj": vmem(ml, *field),
        "ch": vmem(2, ml, *field),
        "wh": vmem(2, *field),
        "wb": vmem(rows + 2, 8, ny),
        "ph": vmem(2, ml, *field),
        "gwr": vmem(tiles, ml, LANES),
        "last": vmem(ml, *field),
        "all": vmem(sent_rows, LANES),
    }
    sems = {
        "sent": dma((1,)), "ship": dma((ns,)), "scl": dma((1,)), "part": dma((nl,)),
        "swap": dma((steps,)), "grad": dma((nl,)), "proj": dma((1,)), "control": dma((1,)),
        "weight": dma((1,)), "innov": dma((1,)), "field": dma((1,)), "halo": dma((steps,)),
        "gw": dma((1,)),
    }
    args = (
        vmem(*control.shape),
        vmem(*obs_weight.shape),
        pltpu.SMEM(weights.shape, f32),
        pltpu.SMEM(member_band.shape, member_band.dtype),
        pltpu.SMEM(spread.shape, f32),
        pltpu.SMEM(advect.shape, f32),
        pltpu.SMEM(damping.shape, f32),
    )
    out, gw = pl.pallas_call(
        functools.partial(kernel, n, tiles, steps, ship),
        out_shape=(pltpu.VMEM((ml, rows, ny), f32), pltpu.VMEM((ml,), f32)),
        in_specs=[hbm] * 9,
        out_specs=(whole, whole),
        scratch_shapes=[args, dma((10,)), pltpu.VMEM((ml, vl) + field, ensemble.dtype), buf, sems],
        compiler_params=pltpu.CompilerParams(
            collective_id=0, has_side_effects=True, vmem_limit_bytes=63 * 1024 * 1024
        ),
    )(ensemble, control, weights, member_band, spread, advect, damping, innovation, obs_weight)
    return pl.pallas_call(
        store,
        out_shape=(
            jax.ShapeDtypeStruct((ml, rows, ny), f32),
            jax.ShapeDtypeStruct((ml,), f32),
        ),
        in_specs=[whole, whole],
        out_specs=(hbm, hbm),
        scratch_shapes=[dma((2,))],
    )(*(pltpu.with_memory_space_constraint(x, pltpu.VMEM) for x in (out, gw)))


def solution(mesh):
    in_specs = (
        P("mem", None, "tile", None),
        P("mem", "tile", None),
        P("mem"),
        P("mem"),
        P(),
        P(),
        P(),
        P(None, "tile", None),
        P("tile", None),
    )
    out_specs = (P("mem", "tile", None), P("mem"))
    return jax.shard_map(
        functools.partial(per_device, mesh.shape["mem"], mesh.shape["tile"]),
        mesh=mesh, in_specs=in_specs, out_specs=out_specs, check_vma=False,
    )
```

```python
import functools
import math

import jax
import jax.numpy as jnp
from jax import lax
from jax.experimental import pallas as pl
from jax.experimental.pallas import tpu as pltpu
from jax.sharding import PartitionSpec as P

SWEEPS = 8
CHUNKS = 4
SHIPPED = 1
AFTER = 9
LAG = 1
EXTRA = 4
LANES = 128
MESH = pl.DeviceIdType.MESH


def factors(n):
    a = max(d for d in range(1, n + 1) if n % d == 0 and d * d <= n)
    return a, n // a


def y_pair(f):
    ny = f.shape[-1]
    col = lax.broadcasted_iota(jnp.int32, f.shape, 1)
    north = jnp.where(col == ny - 1, 0.0, pltpu.roll(f, ny - 1, 1))
    south = jnp.where(col == 0, 0.0, pltpu.roll(f, 1, 1))
    return north, south


def sweeps(f, rates):
    rows = f.shape[0]
    for _ in range(SWEEPS):
        north, south = y_pair(f)
        east = pltpu.roll(f, rows - 1, 0)
        west = pltpu.roll(f, 1, 0)
        f = f + rates * (east + west + north + south - 4.0 * f)
    return f


def kernel(
    n, tiles, steps, ship, sent_rows,
    ens, control_h, weights_h, band_h, spread_h, advect_h, damping_h, innov, obs_h,
    out, gw_out,
    args, arg_sem, e_v, buf, sems,
):
    a, b = factors(n)
    control, obs, weights, band, spread, advect, damping = args
    loc, scl, proj = buf["loc"], buf["scl"], buf["proj"]
    ml, rows, ny = control.shape
    vl = ens.shape[1]
    nc = ny // LANES
    me = lax.axis_index("mem")
    t = lax.axis_index("tile")
    nxt = (t + 1) % tiles
    prv = (t + tiles - 1) % tiles
    ia = me // b
    ib = me % b
    first = (b, a)
    second = (a, b)
    fi = (ib, ia)
    gi = (ia, ib)
    size = [vl // (2 * f) for f in first]
    chunk = [k // steps for k in size]
    both_q = sum(chunk)
    lead = (0, chunk[0])
    lead1 = (0, (first[0] - 1) * chunk[0])
    lead2 = (0, (second[0] - 1) * chunk[0])
    some_first = sum(f - 1 for f in first) > 0
    some_second = sum(g - 1 for g in second) > 0
    lone = tuple(range(ship, steps))
    sent = tuple(range(ship)) if some_first else ()
    extra = EXTRA if sent and min(chunk) > EXTRA else 0
    order = lone[:AFTER] + tuple(range(ship)) + lone[AFTER:]
    near = tiles // 2 <= 2 + steps
    greet = sorted({1, tiles - 1}) if near else list(range(1, tiles))
    greet = [d for d in greet if d % tiles]

    def device(q, f, g):
        return g * b + f if q == 0 else f * b + g

    def start_of(q, owner, s):
        return pl.multiple_of(q * (vl // 2) + (owner * steps + s) * chunk[q], chunk[q])

    def ahead(q, d):
        return (fi[q] + d) % first[q]

    def behind(q, d):
        return (fi[q] + first[q] - d) % first[q]

    def to_first(q, d):
        return device(q, ahead(q, d), gi[q])

    def back_first(q, d):
        return device(q, behind(q, d), gi[q])

    def to_second(q, d):
        return device(q, fi[q], (gi[q] + d) % second[q])

    def first_peers():
        return [(q, d) for q in range(2) for d in range(1, first[q])]

    def second_peers():
        return [(q, d) for q in range(2) for d in range(1, second[q])]

    def remote(kind, index, src, dst, axis, dev):
        return pltpu.make_async_remote_copy(
            src_ref=src, dst_ref=dst, send_sem=sems["sent"].at[0], recv_sem=sems[kind].at[index],
            device_id={axis: dev}, device_id_type=MESH,
        )

    def arrived(kind, index, ref):
        remote(kind, index, ref, ref, "tile", nxt).wait_recv()

    def lanes(c):
        return slice(c * LANES, (c + 1) * LANES)

    def load(k, src, dst):
        return pltpu.make_async_copy(src, dst, arg_sem.at[k])

    def ens_load(k, q, owner, start, count):
        where = pl.ds(start_of(q, owner, 0) + start, count)
        return load(k, ens.at[:, where], e_v.at[:, where])

    soon = [ship * k + extra for k in chunk]
    early = [ens_load(0, q, ahead(q, d), 0, soon[q]) for q, d in first_peers() if ship]
    late = [ens_load(1, q, fi[q], 0, size[q]) for q in range(2)]
    late += [ens_load(1, q, ahead(q, d), soon[q], size[q] - soon[q]) for q, d in first_peers()]
    innov_load = [
        load(
            2,
            innov.at[pl.ds(start_of(q, fi[q], s), chunk[q]), :, lanes(c)],
            buf["iv"].at[pl.ds(s * both_q + lead[q], chunk[q]), c],
        )
        for s in range(steps)
        for q in range(2)
        for c in range(nc)
    ]
    arg_load = [
        load(3 + i, src, dst)
        for i, (src, dst) in enumerate((
            (control_h, control), (obs_h, obs), (weights_h, weights), (band_h, band),
            (spread_h, spread), (advect_h, advect), (damping_h, damping),
        ))
    ]
    for c in early:
        c.start()
    barrier = pltpu.get_barrier_semaphore()
    for q, d in first_peers():
        pl.semaphore_signal(
            barrier, inc=1, device_id={"mem": to_first(q, d)}, device_id_type=MESH
        )
    for d in greet:
        pl.semaphore_signal(
            barrier, inc=1, device_id={"tile": (t + d) % tiles}, device_id_type=MESH
        )
    for c in arg_load + innov_load + late:
        c.start()
    early_planes = sum((first[q] - 1) * soon[q] for q in range(2))

    def block1(q, d, per=1):
        return pl.ds((lead1[q] + (d - 1) * chunk[q]) * per, chunk[q] * per)

    def block2(q, d):
        return pl.ds(lead2[q] + (d - 1) * chunk[q], chunk[q])

    def own(q, s):
        return pl.ds(s * both_q + lead[q], chunk[q])

    def slot(q, d):
        return (first[0] - 1) * q + d - 1

    def ship_copy(q, s, d):
        where = block1(q, d, ml)
        return remote(
            "ship", s, buf["es"].at[s, where], buf["er"].at[s, where], "mem", to_first(q, d)
        )

    def scl_copy(q, d):
        return remote("scl", 0, scl, buf["sr"].at[slot(q, d)], "mem", to_first(q, d))

    def part_copy(q, s, d, skip):
        where = pl.ds(lead1[q] + (d - 1) * chunk[q] + skip, chunk[q] - skip)
        return remote(
            "part", part_sem(q, s), buf["to"].at[s - ship, where], buf["r1"].at[s - ship, where],
            "mem", to_first(q, d),
        )

    def takes(coordinate):
        return coordinate != 0

    def extra_copy(q, d):
        where = pl.ds(((first[0] - 1) * q + d - 1) * ml * extra, ml * extra)
        return remote(
            "extra", q, buf["xs"].at[where], buf["xr"].at[where], "mem", to_first(q, d)
        )

    def split(copy, q, s, d, coordinate):
        if s == ship and extra:
            pl.when(takes(coordinate))(lambda: copy(q, s, d, extra).start())
            pl.when(jnp.logical_not(takes(coordinate)))(lambda: copy(q, s, d, 0).start())
        else:
            copy(q, s, d, 0).start()

    def part_sem(q, s):
        return s - ship if s > ship or q == 0 else steps - ship

    def swap_copy(q, s, d):
        return remote(
            "swap", s, buf["part"].at[own(q, s)], buf["r2"].at[s, block2(q, d)],
            "mem", to_second(q, d),
        )

    def grad_copy(q, s, d, skip):
        count = chunk[q] - skip
        return remote(
            "grad", part_sem(q, s),
            buf["grad"].at[pl.ds(s * both_q + lead[q] + skip, count)],
            buf["gr"].at[s - ship, pl.ds(lead1[q] + (d - 1) * chunk[q] + skip, count)],
            "mem", to_first(q, d),
        )

    def arrived_split(kind, ref, some, short, full):
        for q in range(2):
            if first[q] > 1:
                index = part_sem(q, ship)
                if extra:
                    pl.when(some(q))(
                        lambda q=q, index=index: arrived(kind, index, ref.at[pl.ds(0, short(q))])
                    )
                    pl.when(jnp.logical_not(some(q)))(
                        lambda q=q, index=index: arrived(kind, index, ref.at[pl.ds(0, full(q))])
                    )
                else:
                    arrived(kind, index, ref.at[pl.ds(0, (first[q] - 1) * chunk[q])])

    def proj_copy(q, d):
        return remote(
            "proj", 0, buf["pp"].at[slot(q, d)], buf["pr"].at[slot(q, d)],
            "mem", back_first(q, d),
        )

    def to_both(kind, src, dst):
        return (
            remote(kind, 0, src, dst.at[0], "tile", nxt),
            remote(kind, 0, src, dst.at[1], "tile", prv),
        )

    ip, ov = buf["ip"], buf["ov"]

    def halo(s):
        where = pl.ds(s * both_q, both_q)
        return (
            remote("halo", s, ip.at[pl.ds(rows, 2), where], ip.at[pl.ds(0, 2), where], "tile", nxt),
            remote("halo", s, ip.at[pl.ds(2, 2), where], ip.at[pl.ds(rows + 2, 2), where], "tile", prv),
        )

    c_copy = to_both("control", control, buf["ch"])
    w_copy = to_both("weight", obs, buf["wh"])
    last = buf["last"]
    p_copy = to_both("field", last, buf["ph"])
    o_copy = (
        remote("innov", 0, ov.at[rows], ov.at[0], "tile", nxt),
        remote("innov", 0, ov.at[1], ov.at[rows + 1], "tile", prv),
    )

    if sent:
        where = e_v.at[:, pl.ds(0, early_planes)]
        load(0, where, where).wait()
    for s in sent:
        for q, d in first_peers():
            where = pl.ds(start_of(q, ahead(q, d), s), chunk[q])
            for m in range(ml):
                e = e_v[m, where].astype(jnp.float32)
                at = (lead1[q] + (d - 1) * chunk[q]) * ml + m * chunk[q]
                for c in range(nc):
                    buf["es"][s, at : at + chunk[q], c] = e[:, :, lanes(c)]
    if extra:
        for q, d in first_peers():
            where = pl.ds(start_of(q, ahead(q, d), ship), extra)
            for m in range(ml):
                e = e_v[m, where].astype(jnp.float32)
                at = (slot(q, d) * ml + m) * extra
                for c in range(nc):
                    buf["xs"][at : at + extra, c] = e[:, :, lanes(c)]
    pl.semaphore_wait(barrier, len(greet) + a - 1 + b - 1)
    for s in sent:
        for q, d in first_peers():
            ship_copy(q, s, d).start()
    if extra:
        for q, d in first_peers():
            pl.when(takes(ahead(q, d)))(lambda q=q, d=d: extra_copy(q, d).start())
    for c in arg_load[:2]:
        c.wait()
    for c in c_copy + w_copy:
        c.start()

    load(2, buf["iv"], buf["iv"]).wait()
    flat_iv = buf["iv"].reshape(steps * both_q * nc * rows, LANES)

    @pl.loop(0, steps * both_q // 8)
    def _(j):
        for c in range(nc):
            for r in range(rows):
                ov[1 + r, pl.ds(pl.multiple_of(j * 8, 8), 8), lanes(c)] = flat_iv[
                    pl.ds(j * (8 * nc * rows) + c * rows + r, 8, stride=nc * rows), :
                ]

    for c in o_copy:
        c.start()
    for c in arg_load[2:]:
        c.wait()
    coef = buf["coef"]
    sub = lax.broadcasted_iota(jnp.int32, (8, LANES), 0)
    for q in range(2):

        @pl.loop(0, size[q] // 8)
        def _(j):
            s = j // (chunk[q] // 8)
            at = pl.multiple_of(s * both_q + lead[q] + (j % (chunk[q] // 8)) * 8, 8)
            k = start_of(q, fi[q], 0) + j * 8
            for kind, value in enumerate((
                lambda i: advect[0, i], lambda i: advect[1, i], lambda i: damping[i]
            )):
                v = jnp.full((8, LANES), value(k), jnp.float32)
                for i in range(1, 8):
                    v = jnp.where(sub == i, value(k + i), v)
                coef[kind, pl.ds(at, 8)] = v

    rates = jnp.concatenate(
        [jnp.full((3 * rows, ny), spread[band[m]], jnp.float32) for m in range(ml)], axis=0
    )
    arrived("control", 0, buf["ch"])
    field = []
    for m in range(ml):
        field += [buf["ch"][0, m], control[m], buf["ch"][1, m]]
    field = sweeps(jnp.concatenate(field, axis=0), rates)
    for m in range(ml):
        center = field[(3 * m + 1) * rows : (3 * m + 2) * rows]
        loc[m] = center
        scl[m] = weights[m] * center
        proj[m] = jnp.zeros_like(center)
        for q, d in first_peers():
            buf["pp"][slot(q, d), m] = jnp.zeros_like(center)
    if sent:
        for q, d in first_peers():
            scl_copy(q, d).start()
    where = e_v.at[:, pl.ds(0, vl - early_planes)]
    load(1, where, where).wait()

    def own_sum(q, owner, s, c):
        where = pl.ds(start_of(q, owner, s), chunk[q])
        total = None
        for m in range(ml):
            term = e_v[m, where, :, lanes(c)].astype(jnp.float32) * scl[m, :, lanes(c)][None]
            total = term if total is None else total + term
        return total

    for s in lone:
        for q, d in first_peers():
            for c in range(nc):
                buf["to"][s - ship, block1(q, d), c] = own_sum(q, ahead(q, d), s, c)
            split(part_copy, q, s, d, ahead(q, d))
    for s in range(steps):
        for q in range(2):
            for c in range(nc):
                buf["part"][own(q, s), c] = own_sum(q, fi[q], s, c)
    arrived("weight", 0, buf["wh"])
    wb = buf["wb"]
    wb[0] = jnp.broadcast_to(buf["wh"][0, rows - 1 :], (8, ny))
    wb[rows + 1] = jnp.broadcast_to(buf["wh"][1, :1], (8, ny))
    for r in range(rows):
        wb[1 + r] = jnp.broadcast_to(obs[r : r + 1], (8, ny))

    def add_first(s):
        if some_first:
            if s > ship:
                arrived("part", s - ship, buf["r1"].at[s - ship])
            elif s == ship:
                arrived_split(
                    "part", buf["r1"].at[0], lambda q: takes(fi[q]),
                    lambda q: (first[q] - 1) * (chunk[q] - extra),
                    lambda q: (first[q] - 1) * chunk[q],
                )
                for q in range(2):
                    if extra and first[q] > 1:
                        where = pl.ds(0, (first[q] - 1) * ml * extra)
                        pl.when(takes(fi[q]))(
                            lambda q=q, where=where: arrived("extra", q, buf["xr"].at[where])
                        )
            else:
                arrived("ship", s, buf["er"].at[s])
        skip = extra if s == ship else 0
        for q in range(2):
            rest = pl.ds(s * both_q + lead[q] + skip, chunk[q] - skip)
            for c in range(nc):
                total = buf["part"][rest, c]
                for d in range(1, first[q]):
                    if s >= ship:
                        at = lead1[q] + (d - 1) * chunk[q]
                        total = total + buf["r1"][s - ship, at + skip : at + chunk[q], c]
                    else:
                        for m in range(ml):
                            at = (lead1[q] + (d - 1) * chunk[q]) * ml + m * chunk[q]
                            total = total + (
                                buf["er"][s, at : at + chunk[q], c]
                                * buf["sr"][slot(q, d), m, :, lanes(c)][None]
                            )
                buf["part"][rest, c] = total
            if s == ship and extra and first[q] > 1:
                head = pl.ds(s * both_q + lead[q], extra)

                @pl.when(takes(fi[q]))
                def _(q=q, head=head):
                    for c in range(nc):
                        total = buf["part"][head, c]
                        for d in range(1, first[q]):
                            for m in range(ml):
                                at = (slot(q, d) * ml + m) * extra
                                total = total + (
                                    buf["xr"][at : at + extra, c]
                                    * buf["sr"][slot(q, d), m, :, lanes(c)][None]
                                )
                        buf["part"][head, c] = total

                @pl.when(jnp.logical_not(takes(fi[q])))
                def _(q=q, head=head):
                    for c in range(nc):
                        total = buf["part"][head, c]
                        for d in range(1, first[q]):
                            at = lead1[q] + (d - 1) * chunk[q]
                            total = total + buf["r1"][0, at : at + extra, c]
                        buf["part"][head, c] = total

            for d in range(1, second[q]):
                swap_copy(q, s, d).start()

    def add_second(s):
        if some_second:
            arrived("swap", s, buf["r2"].at[s])
        rows_of = lambda planes: planes * nc * rows
        flat = buf["part"].reshape(rows_of(steps * both_q), LANES)
        for q in range(2):
            peers = [
                buf["r2"].at[s, block2(q, d)].reshape(rows_of(chunk[q]), LANES)
                for d in range(1, second[q])
            ]
            base = s * both_q + lead[q]

            @pl.loop(0, chunk[q] // 8)
            def _(j):
                for c in range(nc):
                    for r in range(rows):
                        at = j * rows_of(8) + c * rows + r
                        total = flat[pl.ds(rows_of(base) + at, 8, stride=nc * rows), :]
                        for p in peers:
                            total = total + p[pl.ds(at, 8, stride=nc * rows), :]
                        ip[2 + r, pl.ds(pl.multiple_of(base + j * 8, 8), 8), lanes(c)] = total

        for c in halo(s):
            c.start()

    def adjoint(s):
        arrived("halo", s, ip.at[pl.ds(0, 4), pl.ds(s * both_q, both_q)])
        col = lax.broadcasted_iota(jnp.int32, (8, ny), 1)
        flat = buf["grad"].reshape(steps * both_q * nc * rows, LANES)

        @pl.loop(0, both_q // 8)
        def _(j):
            where = pl.ds(pl.multiple_of(s * both_q + j * 8, 8), 8)
            ax, ay, e = (jnp.concatenate([coef[k, where]] * nc, axis=1) for k in range(3))
            mid = 1.0 - 4.0 * e
            up = e - 0.5 * ax
            down = e + 0.5 * ax
            left_c = e - 0.5 * ay
            right_c = e + 0.5 * ay
            north1 = jnp.where(col == ny - 1, 0.0, left_c)
            south1 = jnp.where(col == 0, 0.0, right_c)
            north2 = jnp.where(col == ny - 1, 0.0, right_c)
            south2 = jnp.where(col == 0, 0.0, left_c)

            def turn(f):
                return pltpu.roll(f, ny - 1, 1), pltpu.roll(f, 1, 1)

            f = [ip[r, where, :] for r in range(rows + 4)]
            w = []
            for r in range(1, rows + 3):
                north, south = turn(f[r])
                d = (
                    mid * f[r] + up * f[r + 1] + down * f[r - 1]
                    + north1 * north + south1 * south
                )
                w.append(wb[r - 1] * (d - ov[r - 1, where, :]))
            for r in range(1, rows + 1):
                north, south = turn(w[r])
                g = (
                    mid * w[r] + down * w[r + 1] + up * w[r - 1]
                    + north2 * north + south2 * south
                )
                for c in range(nc):
                    at = (s * both_q + j * 8) * (nc * rows) + c * rows + r - 1
                    flat[pl.ds(at, 8, stride=nc * rows), :] = g[:, lanes(c)]

        if s >= ship:
            for q, d in first_peers():
                split(grad_copy, q, s, d, fi[q])

    def project_own(s):
        for q in range(2):
            where = pl.ds(start_of(q, fi[q], s), chunk[q])
            for c in range(nc):
                g = buf["grad"][own(q, s), c]
                for m in range(ml):
                    e = e_v[m, where, :, lanes(c)].astype(jnp.float32)
                    proj[m, :, lanes(c)] += jnp.sum(e * g, axis=0)
                if s < ship:
                    for d in range(1, first[q]):
                        for m in range(ml):
                            at = (lead1[q] + (d - 1) * chunk[q]) * ml + m * chunk[q]
                            e = buf["er"][s, at : at + chunk[q], c]
                            buf["pp"][slot(q, d), m, :, lanes(c)] += jnp.sum(e * g, axis=0)

            if s == ship and extra and first[q] > 1:

                @pl.when(takes(fi[q]))
                def _(q=q):
                    for c in range(nc):
                        g = buf["grad"][pl.ds(s * both_q + lead[q], extra), c]
                        for d in range(1, first[q]):
                            for m in range(ml):
                                at = (slot(q, d) * ml + m) * extra
                                e = buf["xr"][at : at + extra, c]
                                buf["pp"][slot(q, d), m, :, lanes(c)] += jnp.sum(e * g, axis=0)

    def project_in(s):
        if s == ship:
            arrived_split(
                "grad", buf["gr"].at[0], lambda q: jnp.logical_not(takes(fi[q])),
                lambda q: (first[q] - 1) * (chunk[q] - extra),
                lambda q: (first[q] - 1) * chunk[q] - (first[q] - 2) * extra,
            )
        else:
            arrived("grad", s - ship, buf["gr"].at[s - ship])

        def add(q, d, start, count):
            where = pl.ds(start_of(q, behind(q, d), s) + start, count)
            at = lead1[q] + (d - 1) * chunk[q] + start
            for c in range(nc):
                g = buf["gr"][s - ship, at : at + count, c]
                for m in range(ml):
                    e = e_v[m, where, :, lanes(c)].astype(jnp.float32)
                    proj[m, :, lanes(c)] += jnp.sum(e * g, axis=0)

        for q, d in first_peers():
            if s == ship and extra:
                add(q, d, extra, chunk[q] - extra)
                pl.when(jnp.logical_not(takes(behind(q, d))))(
                    lambda q=q, d=d: add(q, d, 0, extra)
                )
            else:
                add(q, d, 0, chunk[q])

    scope = jax.named_scope
    if sent:
        arrived("scl", 0, buf["sr"])
    for s in order:
        with scope(f"add_first{s}"):
            add_first(s)
    for tick in range(steps + LAG):
        if tick < steps:
            with scope(f"add_second{order[tick]}"):
                add_second(order[tick])
        if tick == LAG:
            arrived("innov", 0, ov.at[pl.ds(0, 2)])
        if tick >= LAG:
            s = order[tick - LAG]
            with scope(f"adjoint{s}"):
                adjoint(s)
            with scope(f"project_own{s}"):
                project_own(s)
            if sent and s == ship - 1:
                for q, d in first_peers():
                    proj_copy(q, d).start()
    if some_first:
        for s in lone:
            with scope(f"project_in{s}"):
                project_in(s)
    with scope("tail"):
        if sent:
            arrived("proj", 0, buf["pr"])
        for m in range(ml):
            total = proj[m]
            if sent:
                for q, d in first_peers():
                    total = total + buf["pr"][slot(q, d), m]
            proj[m] = total
            last[m] = weights[m] * total
    with scope("halo_out"):
        for c in p_copy:
            c.start()
        gwr = buf["gwr"]
        for m in range(ml):
            v = jnp.sum(loc[m] * proj[m], axis=0, keepdims=True)
            gwr[t, m : m + 1] = sum(v[:, lanes(c)] for c in range(nc))
        for d in range(1, tiles):
            remote("gw", 0, gwr.at[t], gwr.at[t], "tile", (t + d) % tiles).start()
        arrived("field", 0, buf["ph"])
    with scope("sweeps"):
        field = []
        for m in range(ml):
            field += [buf["ph"][0, m], last[m], buf["ph"][1, m]]
        field = sweeps(jnp.concatenate(field, axis=0), rates)
        for m in range(ml):
            out[m] = control[m] + field[(3 * m + 1) * rows : (3 * m + 2) * rows]
    with scope("finish"):
        if tiles > 1:
            arrived("gw", 0, gwr.at[pl.ds(0, tiles - 1)])
        total = gwr[0]
        for d in range(1, tiles):
            total = total + gwr[d]
        total = jnp.broadcast_to(jnp.sum(total, axis=1, keepdims=True), (ml, LANES))
        row = lax.broadcasted_iota(jnp.int32, (ml, LANES), 0)
        lane = lax.broadcasted_iota(jnp.int32, (ml, LANES), 1)
        sums = jnp.sum(jnp.where(row == lane, total, 0.0), axis=0)
        gw_out[...] = sums[:ml] / math.sqrt(tiles * rows * ny * vl)
        def all_left(count):
            ref = buf["all"].at[pl.ds(0, count)]
            remote("gw", 0, ref, ref, "tile", nxt).wait_send()

        if extra:
            for case in range(4):
                is_first = (case % 2 == 0, case // 2 == 0)
                change = 0
                for q in range(2):
                    if first[q] > 1:
                        out = first[q] - 1 if is_first[q] else first[q] - 2
                        change += out * (ml - 1) * extra
                        change -= 0 if is_first[q] else (first[q] - 1) * extra
                here = jnp.logical_and(
                    (fi[0] == 0) == is_first[0], (fi[1] == 0) == is_first[1]
                )
                pl.when(here)(functools.partial(all_left, sent_rows + change * nc * rows))
        else:
            all_left(sent_rows)


def store(field, sums, out, gw, sem):
    copies = [
        pltpu.make_async_copy(src, dst, sem.at[i])
        for i, (src, dst) in enumerate(((field, out), (sums, gw)))
    ]
    for c in copies:
        c.start()
    for c in copies:
        c.wait()


def per_device(
    n, tiles,
    ensemble, control, weights, member_band, spread, advect, damping, innovation, obs_weight
):
    ml, vl, rows, ny = ensemble.shape
    a, b = factors(n)
    first, second = (b, a), (a, b)
    assert rows == SWEEPS and ny % LANES == 0 and ml <= 8 and vl % (16 * b) == 0
    assert tiles > 2
    nc = ny // LANES
    size = [vl // (2 * f) for f in first]
    steps = max(d for d in range(1, CHUNKS + 1) if all(k % (8 * d) == 0 for k in size))
    ship = steps * SHIPPED // CHUNKS
    chunk = [k // steps for k in size]
    f32 = jnp.float32
    dma = pltpu.SemaphoreType.DMA
    hbm = pl.BlockSpec(memory_space=pl.ANY)
    whole = pl.BlockSpec(memory_space=pltpu.VMEM)
    field = (rows, ny)
    tile = (nc, rows, LANES)
    vmem = lambda *shape: pltpu.VMEM(shape, f32)
    links = max(sum(f - 1 for f in first), 1)
    block1 = max(sum((f - 1) * k for f, k in zip(first, chunk)), 8)
    block2 = max(sum((g - 1) * k for g, k in zip(second, chunk)), 8)
    ns, nl = max(ship, 1), max(steps - ship, 1)
    total = sum(size)
    out1 = sum((f - 1) * k for f, k in zip(first, chunk))
    out2 = sum((g - 1) * k for g, k in zip(second, chunk))
    fields = 2 * (steps - ship) * out1 + steps * out2 + 4 * ml + 2
    if ship:
        fields += ship * ml * out1 + 2 * ml * sum(f - 1 for f in first)
    sent_rows = fields * nc * rows + 6 * total * nc + (tiles - 1) * ml
    buf = {
        "es": vmem(ns, ml * block1, *tile),
        "er": vmem(ns, ml * block1, *tile),
        "to": vmem(nl, block1, *tile),
        "r1": vmem(nl, block1, *tile),
        "part": vmem(total, *tile),
        "r2": vmem(steps, block2, *tile),
        "grad": vmem(total, *tile),
        "gr": vmem(nl, block1, *tile),
        "iv": vmem(total, *tile),
        "ip": vmem(rows + 4, total, ny),
        "ov": vmem(rows + 2, total, ny),
        "coef": vmem(3, total, LANES),
        "pp": vmem(links, ml, *field),
        "pr": vmem(links, ml, *field),
        "sr": vmem(links, ml, *field),
        "loc": vmem(ml, *field),
        "scl": vmem(ml, *field),
        "proj": vmem(ml, *field),
        "ch": vmem(2, ml, *field),
        "wh": vmem(2, *field),
        "wb": vmem(rows + 2, 8, ny),
        "ph": vmem(2, ml, *field),
        "gwr": vmem(tiles, ml, LANES),
        "last": vmem(ml, *field),
        "all": vmem(sent_rows + 2 * links * ml * EXTRA * nc * rows, LANES),
        "xs": vmem(links * ml * EXTRA, *tile),
        "xr": vmem(links * ml * EXTRA, *tile),
    }
    sems = {
        "sent": dma((1,)), "ship": dma((ns,)), "scl": dma((1,)), "part": dma((nl + 1,)),
        "swap": dma((steps,)), "grad": dma((nl + 1,)), "extra": dma((2,)), "proj": dma((1,)), "control": dma((1,)),
        "weight": dma((1,)), "innov": dma((1,)), "field": dma((1,)), "halo": dma((steps,)),
        "gw": dma((1,)),
    }
    args = (
        vmem(*control.shape),
        vmem(*obs_weight.shape),
        pltpu.SMEM(weights.shape, f32),
        pltpu.SMEM(member_band.shape, member_band.dtype),
        pltpu.SMEM(spread.shape, f32),
        pltpu.SMEM(advect.shape, f32),
        pltpu.SMEM(damping.shape, f32),
    )
    out, gw = pl.pallas_call(
        functools.partial(kernel, n, tiles, steps, ship, sent_rows),
        out_shape=(pltpu.VMEM((ml, rows, ny), f32), pltpu.VMEM((ml,), f32)),
        in_specs=[hbm] * 9,
        out_specs=(whole, whole),
        scratch_shapes=[args, dma((10,)), pltpu.VMEM((ml, vl) + field, ensemble.dtype), buf, sems],
        compiler_params=pltpu.CompilerParams(
            collective_id=0, has_side_effects=True, vmem_limit_bytes=63 * 1024 * 1024
        ),
    )(ensemble, control, weights, member_band, spread, advect, damping, innovation, obs_weight)
    return pl.pallas_call(
        store,
        out_shape=(
            jax.ShapeDtypeStruct((ml, rows, ny), f32),
            jax.ShapeDtypeStruct((ml,), f32),
        ),
        in_specs=[whole, whole],
        out_specs=(hbm, hbm),
        scratch_shapes=[dma((2,))],
    )(*(pltpu.with_memory_space_constraint(x, pltpu.VMEM) for x in (out, gw)))


def solution(mesh):
    in_specs = (
        P("mem", None, "tile", None),
        P("mem", "tile", None),
        P("mem"),
        P("mem"),
        P(),
        P(),
        P(),
        P(None, "tile", None),
        P("tile", None),
    )
    out_specs = (P("mem", "tile", None), P("mem"))
    return jax.shard_map(
        functools.partial(per_device, mesh.shape["mem"], mesh.shape["tile"]),
        mesh=mesh, in_specs=in_specs, out_specs=out_specs, check_vma=False,
    )
```

```python
import functools
import math

import jax
import jax.numpy as jnp
from jax import lax
from jax.experimental import pallas as pl
from jax.experimental.pallas import tpu as pltpu
from jax.sharding import PartitionSpec as P

SWEEPS = 8
CHUNKS = 4
SHIPPED = 1
AFTER = 9
LAG = 1
EXTRA = 4
LANES = 128
MESH = pl.DeviceIdType.MESH


def factors(n):
    a = max(d for d in range(1, n + 1) if n % d == 0 and d * d <= n)
    return a, n // a


def sweeps(f, rates):
    rows, ny = f.shape
    col = lax.broadcasted_iota(jnp.int32, f.shape, 1)
    inside = jnp.where(col == 0, 1.0, jnp.where(col == ny - 1, 1.0, 2.0))
    c = 1.0 - 4.0 * rates
    one = 2.0 * c * rates
    two = rates * rates
    here = c * c + two * inside

    def along_x(g):
        return pltpu.roll(g, rows - 1, 0) + pltpu.roll(g, 1, 0)

    def along_y(g, k):
        return jnp.where(col < ny - k, pltpu.roll(g, ny - k, 1), 0.0) + jnp.where(
            col >= k, pltpu.roll(g, k, 1), 0.0
        )

    for _ in range(SWEEPS // 2):
        near = along_y(f, 1)
        inner = one * f + two * along_x(f) + (2.0 * two) * near
        f = here * f + one * near + two * along_y(f, 2) + along_x(inner)
    return f


def kernel(
    n, tiles, steps, ship, sent_rows,
    ens, control_h, weights_h, band_h, spread_h, advect_h, damping_h, innov, obs_h,
    out, gw_out,
    args, arg_sem, e_v, buf, sems,
):
    a, b = factors(n)
    control, obs, weights, band, spread, advect, damping = args
    loc, scl, proj = buf["loc"], buf["scl"], buf["proj"]
    ml, rows, ny = control.shape
    vl = ens.shape[1]
    nc = ny // LANES
    me = lax.axis_index("mem")
    t = lax.axis_index("tile")
    nxt = (t + 1) % tiles
    prv = (t + tiles - 1) % tiles
    ia = me // b
    ib = me % b
    first = (b, a)
    second = (a, b)
    fi = (ib, ia)
    gi = (ia, ib)
    size = [vl // (2 * f) for f in first]
    chunk = [k // steps for k in size]
    both_q = sum(chunk)
    lead = (0, chunk[0])
    lead1 = (0, (first[0] - 1) * chunk[0])
    lead2 = (0, (second[0] - 1) * chunk[0])
    some_first = sum(f - 1 for f in first) > 0
    some_second = sum(g - 1 for g in second) > 0
    lone = tuple(range(ship, steps))
    sent = tuple(range(ship)) if some_first else ()
    extra = EXTRA if sent and min(chunk) > EXTRA else 0
    order = lone[:AFTER] + tuple(range(ship)) + lone[AFTER:]
    near = tiles // 2 <= 2 + steps
    greet = sorted({1, tiles - 1}) if near else list(range(1, tiles))
    greet = [d for d in greet if d % tiles]

    def device(q, f, g):
        return g * b + f if q == 0 else f * b + g

    def start_of(q, owner, s):
        return pl.multiple_of(q * (vl // 2) + (owner * steps + s) * chunk[q], chunk[q])

    def ahead(q, d):
        return (fi[q] + d) % first[q]

    def behind(q, d):
        return (fi[q] + first[q] - d) % first[q]

    def to_first(q, d):
        return device(q, ahead(q, d), gi[q])

    def back_first(q, d):
        return device(q, behind(q, d), gi[q])

    def to_second(q, d):
        return device(q, fi[q], (gi[q] + d) % second[q])

    def first_peers():
        return [(q, d) for q in range(2) for d in range(1, first[q])]

    def second_peers():
        return [(q, d) for q in range(2) for d in range(1, second[q])]

    def remote(kind, index, src, dst, axis, dev):
        return pltpu.make_async_remote_copy(
            src_ref=src, dst_ref=dst, send_sem=sems["sent"].at[0], recv_sem=sems[kind].at[index],
            device_id={axis: dev}, device_id_type=MESH,
        )

    def arrived(kind, index, ref):
        remote(kind, index, ref, ref, "tile", nxt).wait_recv()

    def lanes(c):
        return slice(c * LANES, (c + 1) * LANES)

    def load(k, src, dst):
        return pltpu.make_async_copy(src, dst, arg_sem.at[k])

    def ens_load(k, q, owner, start, count):
        where = pl.ds(start_of(q, owner, 0) + start, count)
        return load(k, ens.at[:, where], e_v.at[:, where])

    soon = [ship * k + extra for k in chunk]
    early = [ens_load(0, q, ahead(q, d), 0, soon[q]) for q, d in first_peers() if ship]
    late = [ens_load(1, q, fi[q], 0, size[q]) for q in range(2)]
    late += [ens_load(1, q, ahead(q, d), soon[q], size[q] - soon[q]) for q, d in first_peers()]
    innov_load = [
        load(
            2,
            innov.at[pl.ds(start_of(q, fi[q], s), chunk[q]), :, lanes(c)],
            buf["iv"].at[pl.ds(s * both_q + lead[q], chunk[q]), c],
        )
        for s in range(steps)
        for q in range(2)
        for c in range(nc)
    ]
    arg_load = [
        load(3 + i, src, dst)
        for i, (src, dst) in enumerate((
            (control_h, control), (obs_h, obs), (weights_h, weights), (band_h, band),
            (spread_h, spread), (advect_h, advect), (damping_h, damping),
        ))
    ]
    for c in early:
        c.start()
    barrier = pltpu.get_barrier_semaphore()
    for q, d in first_peers():
        pl.semaphore_signal(
            barrier, inc=1, device_id={"mem": to_first(q, d)}, device_id_type=MESH
        )
    for d in greet:
        pl.semaphore_signal(
            barrier, inc=1, device_id={"tile": (t + d) % tiles}, device_id_type=MESH
        )
    for c in arg_load + innov_load + late:
        c.start()
    early_planes = sum((first[q] - 1) * soon[q] for q in range(2))

    def block1(q, d, per=1):
        return pl.ds((lead1[q] + (d - 1) * chunk[q]) * per, chunk[q] * per)

    def block2(q, d):
        return pl.ds(lead2[q] + (d - 1) * chunk[q], chunk[q])

    def own(q, s):
        return pl.ds(s * both_q + lead[q], chunk[q])

    def slot(q, d):
        return (first[0] - 1) * q + d - 1

    def ship_copy(q, s, d):
        where = block1(q, d, ml)
        return remote(
            "ship", s, buf["es"].at[s, where], buf["er"].at[s, where], "mem", to_first(q, d)
        )

    def scl_copy(q, d):
        return remote("scl", 0, scl, buf["sr"].at[slot(q, d)], "mem", to_first(q, d))

    def part_copy(q, s, d, skip):
        where = pl.ds(lead1[q] + (d - 1) * chunk[q] + skip, chunk[q] - skip)
        return remote(
            "part", part_sem(q, s), buf["to"].at[s - ship, where], buf["r1"].at[s - ship, where],
            "mem", to_first(q, d),
        )

    def takes(coordinate):
        return coordinate != 0

    def extra_copy(q, d):
        where = pl.ds(((first[0] - 1) * q + d - 1) * ml * extra, ml * extra)
        return remote(
            "extra", q, buf["xs"].at[where], buf["xr"].at[where], "mem", to_first(q, d)
        )

    def split(copy, q, s, d, coordinate):
        if s == ship and extra:
            pl.when(takes(coordinate))(lambda: copy(q, s, d, extra).start())
            pl.when(jnp.logical_not(takes(coordinate)))(lambda: copy(q, s, d, 0).start())
        else:
            copy(q, s, d, 0).start()

    def part_sem(q, s):
        return s - ship if s > ship or q == 0 else steps - ship

    def swap_copy(q, s, d):
        return remote(
            "swap", s, buf["part"].at[own(q, s)], buf["r2"].at[s, block2(q, d)],
            "mem", to_second(q, d),
        )

    def grad_copy(q, s, d, skip):
        count = chunk[q] - skip
        return remote(
            "grad", part_sem(q, s),
            buf["grad"].at[pl.ds(s * both_q + lead[q] + skip, count)],
            buf["gr"].at[s - ship, pl.ds(lead1[q] + (d - 1) * chunk[q] + skip, count)],
            "mem", to_first(q, d),
        )

    def arrived_split(kind, ref, some, short, full):
        for q in range(2):
            if first[q] > 1:
                index = part_sem(q, ship)
                if extra:
                    pl.when(some(q))(
                        lambda q=q, index=index: arrived(kind, index, ref.at[pl.ds(0, short(q))])
                    )
                    pl.when(jnp.logical_not(some(q)))(
                        lambda q=q, index=index: arrived(kind, index, ref.at[pl.ds(0, full(q))])
                    )
                else:
                    arrived(kind, index, ref.at[pl.ds(0, (first[q] - 1) * chunk[q])])

    def proj_copy(q, d):
        return remote(
            "proj", 0, buf["pp"].at[slot(q, d)], buf["pr"].at[slot(q, d)],
            "mem", back_first(q, d),
        )

    def to_both(kind, src, dst):
        return (
            remote(kind, 0, src, dst.at[0], "tile", nxt),
            remote(kind, 0, src, dst.at[1], "tile", prv),
        )

    ip, ov = buf["ip"], buf["ov"]

    def halo(s):
        where = pl.ds(s * both_q, both_q)
        return (
            remote("halo", s, ip.at[pl.ds(rows, 2), where], ip.at[pl.ds(0, 2), where], "tile", nxt),
            remote("halo", s, ip.at[pl.ds(2, 2), where], ip.at[pl.ds(rows + 2, 2), where], "tile", prv),
        )

    c_copy = to_both("control", control, buf["ch"])
    w_copy = to_both("weight", obs, buf["wh"])
    last = buf["last"]
    p_copy = to_both("field", last, buf["ph"])
    o_copy = (
        remote("innov", 0, ov.at[rows], ov.at[0], "tile", nxt),
        remote("innov", 0, ov.at[1], ov.at[rows + 1], "tile", prv),
    )

    if sent:
        where = e_v.at[:, pl.ds(0, early_planes)]
        load(0, where, where).wait()
    for s in sent:
        for q, d in first_peers():
            where = pl.ds(start_of(q, ahead(q, d), s), chunk[q])
            for m in range(ml):
                e = e_v[m, where].astype(jnp.float32)
                at = (lead1[q] + (d - 1) * chunk[q]) * ml + m * chunk[q]
                for c in range(nc):
                    buf["es"][s, at : at + chunk[q], c] = e[:, :, lanes(c)]
    if extra:
        for q, d in first_peers():
            where = pl.ds(start_of(q, ahead(q, d), ship), extra)
            for m in range(ml):
                e = e_v[m, where].astype(jnp.float32)
                at = (slot(q, d) * ml + m) * extra
                for c in range(nc):
                    buf["xs"][at : at + extra, c] = e[:, :, lanes(c)]
    pl.semaphore_wait(barrier, len(greet) + a - 1 + b - 1)
    for s in sent:
        for q, d in first_peers():
            ship_copy(q, s, d).start()
    if extra:
        for q, d in first_peers():
            pl.when(takes(ahead(q, d)))(lambda q=q, d=d: extra_copy(q, d).start())
    for c in arg_load[:2]:
        c.wait()
    for c in c_copy + w_copy:
        c.start()

    load(2, buf["iv"], buf["iv"]).wait()
    flat_iv = buf["iv"].reshape(steps * both_q * nc * rows, LANES)

    @pl.loop(0, steps * both_q // 8)
    def _(j):
        for c in range(nc):
            for r in range(rows):
                ov[1 + r, pl.ds(pl.multiple_of(j * 8, 8), 8), lanes(c)] = flat_iv[
                    pl.ds(j * (8 * nc * rows) + c * rows + r, 8, stride=nc * rows), :
                ]

    for c in o_copy:
        c.start()
    for c in arg_load[2:]:
        c.wait()
    coef = buf["coef"]
    sub = lax.broadcasted_iota(jnp.int32, (8, LANES), 0)
    for q in range(2):

        @pl.loop(0, size[q] // 8)
        def _(j):
            s = j // (chunk[q] // 8)
            at = pl.multiple_of(s * both_q + lead[q] + (j % (chunk[q] // 8)) * 8, 8)
            k = start_of(q, fi[q], 0) + j * 8
            for kind, value in enumerate((
                lambda i: advect[0, i], lambda i: advect[1, i], lambda i: damping[i]
            )):
                v = jnp.full((8, LANES), value(k), jnp.float32)
                for i in range(1, 8):
                    v = jnp.where(sub == i, value(k + i), v)
                coef[kind, pl.ds(at, 8)] = v

    rates = jnp.concatenate(
        [jnp.full((3 * rows, ny), spread[band[m]], jnp.float32) for m in range(ml)], axis=0
    )
    arrived("control", 0, buf["ch"])
    field = []
    for m in range(ml):
        field += [buf["ch"][0, m], control[m], buf["ch"][1, m]]
    field = sweeps(jnp.concatenate(field, axis=0), rates)
    for m in range(ml):
        center = field[(3 * m + 1) * rows : (3 * m + 2) * rows]
        loc[m] = center
        scl[m] = weights[m] * center
        proj[m] = jnp.zeros_like(center)
        for q, d in first_peers():
            buf["pp"][slot(q, d), m] = jnp.zeros_like(center)
    if sent:
        for q, d in first_peers():
            scl_copy(q, d).start()
    where = e_v.at[:, pl.ds(0, vl - early_planes)]
    load(1, where, where).wait()

    def own_sum(q, owner, s, c):
        where = pl.ds(start_of(q, owner, s), chunk[q])
        total = None
        for m in range(ml):
            term = e_v[m, where, :, lanes(c)].astype(jnp.float32) * scl[m, :, lanes(c)][None]
            total = term if total is None else total + term
        return total

    for s in lone:
        for q, d in first_peers():
            for c in range(nc):
                buf["to"][s - ship, block1(q, d), c] = own_sum(q, ahead(q, d), s, c)
            split(part_copy, q, s, d, ahead(q, d))
    for s in range(steps):
        for q in range(2):
            for c in range(nc):
                buf["part"][own(q, s), c] = own_sum(q, fi[q], s, c)
    arrived("weight", 0, buf["wh"])
    wb = buf["wb"]
    wb[0] = jnp.broadcast_to(buf["wh"][0, rows - 1 :], (8, ny))
    wb[rows + 1] = jnp.broadcast_to(buf["wh"][1, :1], (8, ny))
    for r in range(rows):
        wb[1 + r] = jnp.broadcast_to(obs[r : r + 1], (8, ny))

    def add_first(s):
        if some_first:
            if s > ship:
                arrived("part", s - ship, buf["r1"].at[s - ship])
            elif s == ship:
                arrived_split(
                    "part", buf["r1"].at[0], lambda q: takes(fi[q]),
                    lambda q: (first[q] - 1) * (chunk[q] - extra),
                    lambda q: (first[q] - 1) * chunk[q],
                )
                for q in range(2):
                    if extra and first[q] > 1:
                        where = pl.ds(0, (first[q] - 1) * ml * extra)
                        pl.when(takes(fi[q]))(
                            lambda q=q, where=where: arrived("extra", q, buf["xr"].at[where])
                        )
            else:
                arrived("ship", s, buf["er"].at[s])
        skip = extra if s == ship else 0
        for q in range(2):
            rest = pl.ds(s * both_q + lead[q] + skip, chunk[q] - skip)
            for c in range(nc):
                total = buf["part"][rest, c]
                for d in range(1, first[q]):
                    if s >= ship:
                        at = lead1[q] + (d - 1) * chunk[q]
                        total = total + buf["r1"][s - ship, at + skip : at + chunk[q], c]
                    else:
                        for m in range(ml):
                            at = (lead1[q] + (d - 1) * chunk[q]) * ml + m * chunk[q]
                            total = total + (
                                buf["er"][s, at : at + chunk[q], c]
                                * buf["sr"][slot(q, d), m, :, lanes(c)][None]
                            )
                buf["part"][rest, c] = total
            if s == ship and extra and first[q] > 1:
                head = pl.ds(s * both_q + lead[q], extra)

                @pl.when(takes(fi[q]))
                def _(q=q, head=head):
                    for c in range(nc):
                        total = buf["part"][head, c]
                        for d in range(1, first[q]):
                            for m in range(ml):
                                at = (slot(q, d) * ml + m) * extra
                                total = total + (
                                    buf["xr"][at : at + extra, c]
                                    * buf["sr"][slot(q, d), m, :, lanes(c)][None]
                                )
                        buf["part"][head, c] = total

                @pl.when(jnp.logical_not(takes(fi[q])))
                def _(q=q, head=head):
                    for c in range(nc):
                        total = buf["part"][head, c]
                        for d in range(1, first[q]):
                            at = lead1[q] + (d - 1) * chunk[q]
                            total = total + buf["r1"][0, at : at + extra, c]
                        buf["part"][head, c] = total

            for d in range(1, second[q]):
                swap_copy(q, s, d).start()

    def add_second(s):
        if some_second:
            arrived("swap", s, buf["r2"].at[s])
        rows_of = lambda planes: planes * nc * rows
        flat = buf["part"].reshape(rows_of(steps * both_q), LANES)
        for q in range(2):
            peers = [
                buf["r2"].at[s, block2(q, d)].reshape(rows_of(chunk[q]), LANES)
                for d in range(1, second[q])
            ]
            base = s * both_q + lead[q]

            @pl.loop(0, chunk[q] // 8)
            def _(j):
                for c in range(nc):
                    for r in range(rows):
                        at = j * rows_of(8) + c * rows + r
                        total = flat[pl.ds(rows_of(base) + at, 8, stride=nc * rows), :]
                        for p in peers:
                            total = total + p[pl.ds(at, 8, stride=nc * rows), :]
                        ip[2 + r, pl.ds(pl.multiple_of(base + j * 8, 8), 8), lanes(c)] = total

        for c in halo(s):
            c.start()

    def adjoint(s):
        arrived("halo", s, ip.at[pl.ds(0, 4), pl.ds(s * both_q, both_q)])
        col = lax.broadcasted_iota(jnp.int32, (8, ny), 1)
        flat = buf["grad"].reshape(steps * both_q * nc * rows, LANES)

        @pl.loop(0, both_q // 8)
        def _(j):
            where = pl.ds(pl.multiple_of(s * both_q + j * 8, 8), 8)
            ax, ay, e = (jnp.concatenate([coef[k, where]] * nc, axis=1) for k in range(3))
            mid = 1.0 - 4.0 * e
            up = e - 0.5 * ax
            down = e + 0.5 * ax
            left_c = e - 0.5 * ay
            right_c = e + 0.5 * ay
            north1 = jnp.where(col == ny - 1, 0.0, left_c)
            south1 = jnp.where(col == 0, 0.0, right_c)
            north2 = jnp.where(col == ny - 1, 0.0, right_c)
            south2 = jnp.where(col == 0, 0.0, left_c)

            def turn(f):
                return pltpu.roll(f, ny - 1, 1), pltpu.roll(f, 1, 1)

            f = [ip[r, where, :] for r in range(rows + 4)]
            w = []
            for r in range(1, rows + 3):
                north, south = turn(f[r])
                d = (
                    mid * f[r] + up * f[r + 1] + down * f[r - 1]
                    + north1 * north + south1 * south
                )
                w.append(wb[r - 1] * (d - ov[r - 1, where, :]))
            for r in range(1, rows + 1):
                north, south = turn(w[r])
                g = (
                    mid * w[r] + down * w[r + 1] + up * w[r - 1]
                    + north2 * north + south2 * south
                )
                for c in range(nc):
                    at = (s * both_q + j * 8) * (nc * rows) + c * rows + r - 1
                    flat[pl.ds(at, 8, stride=nc * rows), :] = g[:, lanes(c)]

        if s >= ship:
            for q, d in first_peers():
                split(grad_copy, q, s, d, fi[q])

    def project_own(s):
        for q in range(2):
            where = pl.ds(start_of(q, fi[q], s), chunk[q])
            for c in range(nc):
                g = buf["grad"][own(q, s), c]
                for m in range(ml):
                    e = e_v[m, where, :, lanes(c)].astype(jnp.float32)
                    proj[m, :, lanes(c)] += jnp.sum(e * g, axis=0)
                if s < ship:
                    for d in range(1, first[q]):
                        for m in range(ml):
                            at = (lead1[q] + (d - 1) * chunk[q]) * ml + m * chunk[q]
                            e = buf["er"][s, at : at + chunk[q], c]
                            buf["pp"][slot(q, d), m, :, lanes(c)] += jnp.sum(e * g, axis=0)

            if s == ship and extra and first[q] > 1:

                @pl.when(takes(fi[q]))
                def _(q=q):
                    for c in range(nc):
                        g = buf["grad"][pl.ds(s * both_q + lead[q], extra), c]
                        for d in range(1, first[q]):
                            for m in range(ml):
                                at = (slot(q, d) * ml + m) * extra
                                e = buf["xr"][at : at + extra, c]
                                buf["pp"][slot(q, d), m, :, lanes(c)] += jnp.sum(e * g, axis=0)

    def project_in(s):
        if s == ship:
            arrived_split(
                "grad", buf["gr"].at[0], lambda q: jnp.logical_not(takes(fi[q])),
                lambda q: (first[q] - 1) * (chunk[q] - extra),
                lambda q: (first[q] - 1) * chunk[q] - (first[q] - 2) * extra,
            )
        else:
            arrived("grad", s - ship, buf["gr"].at[s - ship])

        def add(q, d, start, count):
            where = pl.ds(start_of(q, behind(q, d), s) + start, count)
            at = lead1[q] + (d - 1) * chunk[q] + start
            for c in range(nc):
                g = buf["gr"][s - ship, at : at + count, c]
                for m in range(ml):
                    e = e_v[m, where, :, lanes(c)].astype(jnp.float32)
                    proj[m, :, lanes(c)] += jnp.sum(e * g, axis=0)

        for q, d in first_peers():
            if s == ship and extra:
                add(q, d, extra, chunk[q] - extra)
                pl.when(jnp.logical_not(takes(behind(q, d))))(
                    lambda q=q, d=d: add(q, d, 0, extra)
                )
            else:
                add(q, d, 0, chunk[q])

    scope = jax.named_scope
    if sent:
        arrived("scl", 0, buf["sr"])
    for s in order:
        with scope(f"add_first{s}"):
            add_first(s)
    for tick in range(steps + LAG):
        if tick < steps:
            with scope(f"add_second{order[tick]}"):
                add_second(order[tick])
        if tick == LAG:
            arrived("innov", 0, ov.at[pl.ds(0, 2)])
        if tick >= LAG:
            s = order[tick - LAG]
            with scope(f"adjoint{s}"):
                adjoint(s)
            with scope(f"project_own{s}"):
                project_own(s)
            if sent and s == ship - 1:
                for q, d in first_peers():
                    proj_copy(q, d).start()
    if some_first:
        for s in lone:
            with scope(f"project_in{s}"):
                project_in(s)
    with scope("tail"):
        if sent:
            arrived("proj", 0, buf["pr"])
        for m in range(ml):
            total = proj[m]
            if sent:
                for q, d in first_peers():
                    total = total + buf["pr"][slot(q, d), m]
            proj[m] = total
            last[m] = weights[m] * total
    with scope("halo_out"):
        for c in p_copy:
            c.start()
        gwr = buf["gwr"]
        for m in range(ml):
            v = jnp.sum(loc[m] * proj[m], axis=0, keepdims=True)
            gwr[t, m : m + 1] = sum(v[:, lanes(c)] for c in range(nc))
        for d in range(1, tiles):
            remote("gw", 0, gwr.at[t], gwr.at[t], "tile", (t + d) % tiles).start()
        arrived("field", 0, buf["ph"])
    with scope("sweeps"):
        field = []
        for m in range(ml):
            field += [buf["ph"][0, m], last[m], buf["ph"][1, m]]
        field = sweeps(jnp.concatenate(field, axis=0), rates)
        for m in range(ml):
            out[m] = control[m] + field[(3 * m + 1) * rows : (3 * m + 2) * rows]
    with scope("finish"):
        if tiles > 1:
            arrived("gw", 0, gwr.at[pl.ds(0, tiles - 1)])
        total = gwr[0]
        for d in range(1, tiles):
            total = total + gwr[d]
        total = jnp.broadcast_to(jnp.sum(total, axis=1, keepdims=True), (ml, LANES))
        row = lax.broadcasted_iota(jnp.int32, (ml, LANES), 0)
        lane = lax.broadcasted_iota(jnp.int32, (ml, LANES), 1)
        sums = jnp.sum(jnp.where(row == lane, total, 0.0), axis=0)
        gw_out[...] = sums[:ml] / math.sqrt(tiles * rows * ny * vl)
        def all_left(count):
            ref = buf["all"].at[pl.ds(0, count)]
            remote("gw", 0, ref, ref, "tile", nxt).wait_send()

        if extra:
            for case in range(4):
                is_first = (case % 2 == 0, case // 2 == 0)
                change = 0
                for q in range(2):
                    if first[q] > 1:
                        out = first[q] - 1 if is_first[q] else first[q] - 2
                        change += out * (ml - 1) * extra
                        change -= 0 if is_first[q] else (first[q] - 1) * extra
                here = jnp.logical_and(
                    (fi[0] == 0) == is_first[0], (fi[1] == 0) == is_first[1]
                )
                pl.when(here)(functools.partial(all_left, sent_rows + change * nc * rows))
        else:
            all_left(sent_rows)


def store(field, sums, out, gw, sem):
    copies = [
        pltpu.make_async_copy(src, dst, sem.at[i])
        for i, (src, dst) in enumerate(((field, out), (sums, gw)))
    ]
    for c in copies:
        c.start()
    for c in copies:
        c.wait()


def per_device(
    n, tiles,
    ensemble, control, weights, member_band, spread, advect, damping, innovation, obs_weight
):
    ml, vl, rows, ny = ensemble.shape
    a, b = factors(n)
    first, second = (b, a), (a, b)
    assert rows == SWEEPS and ny % LANES == 0 and ml <= 8 and vl % (16 * b) == 0
    assert tiles > 2
    nc = ny // LANES
    size = [vl // (2 * f) for f in first]
    steps = max(d for d in range(1, CHUNKS + 1) if all(k % (8 * d) == 0 for k in size))
    ship = steps * SHIPPED // CHUNKS
    chunk = [k // steps for k in size]
    f32 = jnp.float32
    dma = pltpu.SemaphoreType.DMA
    hbm = pl.BlockSpec(memory_space=pl.ANY)
    whole = pl.BlockSpec(memory_space=pltpu.VMEM)
    field = (rows, ny)
    tile = (nc, rows, LANES)
    vmem = lambda *shape: pltpu.VMEM(shape, f32)
    links = max(sum(f - 1 for f in first), 1)
    block1 = max(sum((f - 1) * k for f, k in zip(first, chunk)), 8)
    block2 = max(sum((g - 1) * k for g, k in zip(second, chunk)), 8)
    ns, nl = max(ship, 1), max(steps - ship, 1)
    total = sum(size)
    out1 = sum((f - 1) * k for f, k in zip(first, chunk))
    out2 = sum((g - 1) * k for g, k in zip(second, chunk))
    fields = 2 * (steps - ship) * out1 + steps * out2 + 4 * ml + 2
    if ship:
        fields += ship * ml * out1 + 2 * ml * sum(f - 1 for f in first)
    sent_rows = fields * nc * rows + 6 * total * nc + (tiles - 1) * ml
    buf = {
        "es": vmem(ns, ml * block1, *tile),
        "er": vmem(ns, ml * block1, *tile),
        "to": vmem(nl, block1, *tile),
        "r1": vmem(nl, block1, *tile),
        "part": vmem(total, *tile),
        "r2": vmem(steps, block2, *tile),
        "grad": vmem(total, *tile),
        "gr": vmem(nl, block1, *tile),
        "iv": vmem(total, *tile),
        "ip": vmem(rows + 4, total, ny),
        "ov": vmem(rows + 2, total, ny),
        "coef": vmem(3, total, LANES),
        "pp": vmem(links, ml, *field),
        "pr": vmem(links, ml, *field),
        "sr": vmem(links, ml, *field),
        "loc": vmem(ml, *field),
        "scl": vmem(ml, *field),
        "proj": vmem(ml, *field),
        "ch": vmem(2, ml, *field),
        "wh": vmem(2, *field),
        "wb": vmem(rows + 2, 8, ny),
        "ph": vmem(2, ml, *field),
        "gwr": vmem(tiles, ml, LANES),
        "last": vmem(ml, *field),
        "all": vmem(sent_rows + 2 * links * ml * EXTRA * nc * rows, LANES),
        "xs": vmem(links * ml * EXTRA, *tile),
        "xr": vmem(links * ml * EXTRA, *tile),
    }
    sems = {
        "sent": dma((1,)), "ship": dma((ns,)), "scl": dma((1,)), "part": dma((nl + 1,)),
        "swap": dma((steps,)), "grad": dma((nl + 1,)), "extra": dma((2,)), "proj": dma((1,)), "control": dma((1,)),
        "weight": dma((1,)), "innov": dma((1,)), "field": dma((1,)), "halo": dma((steps,)),
        "gw": dma((1,)),
    }
    args = (
        vmem(*control.shape),
        vmem(*obs_weight.shape),
        pltpu.SMEM(weights.shape, f32),
        pltpu.SMEM(member_band.shape, member_band.dtype),
        pltpu.SMEM(spread.shape, f32),
        pltpu.SMEM(advect.shape, f32),
        pltpu.SMEM(damping.shape, f32),
    )
    out, gw = pl.pallas_call(
        functools.partial(kernel, n, tiles, steps, ship, sent_rows),
        out_shape=(pltpu.VMEM((ml, rows, ny), f32), pltpu.VMEM((ml,), f32)),
        in_specs=[hbm] * 9,
        out_specs=(whole, whole),
        scratch_shapes=[args, dma((10,)), pltpu.VMEM((ml, vl) + field, ensemble.dtype), buf, sems],
        compiler_params=pltpu.CompilerParams(
            collective_id=0, has_side_effects=True, vmem_limit_bytes=63 * 1024 * 1024
        ),
    )(ensemble, control, weights, member_band, spread, advect, damping, innovation, obs_weight)
    return pl.pallas_call(
        store,
        out_shape=(
            jax.ShapeDtypeStruct((ml, rows, ny), f32),
            jax.ShapeDtypeStruct((ml,), f32),
        ),
        in_specs=[whole, whole],
        out_specs=(hbm, hbm),
        scratch_shapes=[dma((2,))],
    )(*(pltpu.with_memory_space_constraint(x, pltpu.VMEM) for x in (out, gw)))


def solution(mesh):
    in_specs = (
        P("mem", None, "tile", None),
        P("mem", "tile", None),
        P("mem"),
        P("mem"),
        P(),
        P(),
        P(),
        P(None, "tile", None),
        P("tile", None),
    )
    out_specs = (P("mem", "tile", None), P("mem"))
    return jax.shard_map(
        functools.partial(per_device, mesh.shape["mem"], mesh.shape["tile"]),
        mesh=mesh, in_specs=in_specs, out_specs=out_specs, check_vma=False,
    )
```

```python
import functools
import math

import jax
import jax.numpy as jnp
from jax import lax
from jax.experimental import pallas as pl
from jax.experimental.pallas import tpu as pltpu
from jax.sharding import PartitionSpec as P

SWEEPS = 8
CHUNKS = 4
SHIPPED = 1
AFTER = 9
LAG = 1
EXTRA = 4
LANES = 128
MESH = pl.DeviceIdType.MESH


def factors(n):
    a = max(d for d in range(1, n + 1) if n % d == 0 and d * d <= n)
    return a, n // a


def sweeps(f, rates):
    rows, ny = f.shape
    col = lax.broadcasted_iota(jnp.int32, f.shape, 1)
    inside = jnp.where(col == 0, 1.0, jnp.where(col == ny - 1, 1.0, 2.0))
    c = 1.0 - 4.0 * rates
    one = 2.0 * c * rates
    two = rates * rates
    here = c * c + two * inside

    def along_x(g):
        return pltpu.roll(g, rows - 1, 0) + pltpu.roll(g, 1, 0)

    def along_y(g, k):
        return jnp.where(col < ny - k, pltpu.roll(g, ny - k, 1), 0.0) + jnp.where(
            col >= k, pltpu.roll(g, k, 1), 0.0
        )

    for _ in range(SWEEPS // 2):
        near = along_y(f, 1)
        inner = one * f + two * along_x(f) + (2.0 * two) * near
        f = here * f + one * near + two * along_y(f, 2) + along_x(inner)
    return f


def kernel(
    n, tiles, steps, ship, sent_rows,
    ens, control_h, weights_h, band_h, spread_h, advect_h, damping_h, innov, obs_h,
    out, gw_out,
    args, arg_sem, e_v, buf, sems,
):
    a, b = factors(n)
    control, obs, weights, band, spread, advect, damping = args
    loc, scl, proj = buf["loc"], buf["scl"], buf["proj"]
    ml, rows, ny = control.shape
    vl = ens.shape[1]
    nc = ny // LANES
    me = lax.axis_index("mem")
    t = lax.axis_index("tile")
    nxt = (t + 1) % tiles
    prv = (t + tiles - 1) % tiles
    ia = me // b
    ib = me % b
    first = (b, a)
    second = (a, b)
    fi = (ib, ia)
    gi = (ia, ib)
    size = [vl // (2 * f) for f in first]
    chunk = [k // steps for k in size]
    both_q = sum(chunk)
    lead = (0, chunk[0])
    lead1 = (0, (first[0] - 1) * chunk[0])
    lead2 = (0, (second[0] - 1) * chunk[0])
    some_first = sum(f - 1 for f in first) > 0
    some_second = sum(g - 1 for g in second) > 0
    lone = tuple(range(ship, steps))
    sent = tuple(range(ship)) if some_first else ()
    extra = EXTRA if sent and min(chunk) > EXTRA else 0
    order = lone[:AFTER] + tuple(range(ship)) + lone[AFTER:]
    near = tiles // 2 <= 2 + steps
    greet = sorted({1, tiles - 1}) if near else list(range(1, tiles))
    greet = [d for d in greet if d % tiles]

    def device(q, f, g):
        return g * b + f if q == 0 else f * b + g

    def start_of(q, owner, s):
        return pl.multiple_of(q * (vl // 2) + (owner * steps + s) * chunk[q], chunk[q])

    def ahead(q, d):
        return (fi[q] + d) % first[q]

    def behind(q, d):
        return (fi[q] + first[q] - d) % first[q]

    def to_first(q, d):
        return device(q, ahead(q, d), gi[q])

    def back_first(q, d):
        return device(q, behind(q, d), gi[q])

    def to_second(q, d):
        return device(q, fi[q], (gi[q] + d) % second[q])

    def first_peers():
        return [(q, d) for q in range(2) for d in range(1, first[q])]

    def second_peers():
        return [(q, d) for q in range(2) for d in range(1, second[q])]

    def remote(kind, index, src, dst, axis, dev):
        return pltpu.make_async_remote_copy(
            src_ref=src, dst_ref=dst, send_sem=sems["sent"].at[0], recv_sem=sems[kind].at[index],
            device_id={axis: dev}, device_id_type=MESH,
        )

    def arrived(kind, index, ref):
        remote(kind, index, ref, ref, "tile", nxt).wait_recv()

    def lanes(c):
        return slice(c * LANES, (c + 1) * LANES)

    def load(k, src, dst):
        return pltpu.make_async_copy(src, dst, arg_sem.at[k])

    def ens_load(k, q, owner, start, count):
        where = pl.ds(start_of(q, owner, 0) + start, count)
        return load(k, ens.at[:, where], e_v.at[:, where])

    soon = [ship * k + extra for k in chunk]
    early = [ens_load(0, q, ahead(q, d), 0, soon[q]) for q, d in first_peers() if ship]
    late = [ens_load(1, q, fi[q], 0, size[q]) for q in range(2)]
    late += [ens_load(1, q, ahead(q, d), soon[q], size[q] - soon[q]) for q, d in first_peers()]
    innov_load = [
        load(
            2,
            innov.at[pl.ds(start_of(q, fi[q], s), chunk[q]), :, lanes(c)],
            buf["iv"].at[pl.ds(s * both_q + lead[q], chunk[q]), c],
        )
        for s in range(steps)
        for q in range(2)
        for c in range(nc)
    ]
    arg_load = [
        load(3 + i, src, dst)
        for i, (src, dst) in enumerate((
            (control_h, control), (obs_h, obs), (weights_h, weights), (band_h, band),
            (spread_h, spread), (advect_h, advect), (damping_h, damping),
        ))
    ]
    for c in early:
        c.start()
    barrier = pltpu.get_barrier_semaphore()
    for q, d in first_peers():
        pl.semaphore_signal(
            barrier, inc=1, device_id={"mem": to_first(q, d)}, device_id_type=MESH
        )
    for d in greet:
        pl.semaphore_signal(
            barrier, inc=1, device_id={"tile": (t + d) % tiles}, device_id_type=MESH
        )
    for c in arg_load:
        c.start()
    early_planes = sum((first[q] - 1) * soon[q] for q in range(2))

    def block1(q, d, per=1):
        return pl.ds((lead1[q] + (d - 1) * chunk[q]) * per, chunk[q] * per)

    def block2(q, d):
        return pl.ds(lead2[q] + (d - 1) * chunk[q], chunk[q])

    def own(q, s):
        return pl.ds(s * both_q + lead[q], chunk[q])

    def slot(q, d):
        return (first[0] - 1) * q + d - 1

    def ship_copy(q, s, d):
        where = block1(q, d, ml)
        return remote(
            "ship", s, buf["es"].at[s, where], buf["er"].at[s, where], "mem", to_first(q, d)
        )

    def scl_copy(q, d):
        return remote("scl", 0, scl, buf["sr"].at[slot(q, d)], "mem", to_first(q, d))

    def part_copy(q, s, d, skip):
        where = pl.ds(lead1[q] + (d - 1) * chunk[q] + skip, chunk[q] - skip)
        return remote(
            "part", part_sem(q, s), buf["to"].at[s - ship, where], buf["r1"].at[s - ship, where],
            "mem", to_first(q, d),
        )

    def takes(coordinate):
        return coordinate != 0

    def extra_copy(q, d):
        where = pl.ds(((first[0] - 1) * q + d - 1) * ml * extra, ml * extra)
        return remote(
            "extra", q, buf["xs"].at[where], buf["xr"].at[where], "mem", to_first(q, d)
        )

    def split(copy, q, s, d, coordinate):
        if s == ship and extra:
            pl.when(takes(coordinate))(lambda: copy(q, s, d, extra).start())
            pl.when(jnp.logical_not(takes(coordinate)))(lambda: copy(q, s, d, 0).start())
        else:
            copy(q, s, d, 0).start()

    def part_sem(q, s):
        return s - ship if s > ship or q == 0 else steps - ship

    def swap_copy(q, s, d):
        return remote(
            "swap", s, buf["part"].at[own(q, s)], buf["r2"].at[s, block2(q, d)],
            "mem", to_second(q, d),
        )

    def grad_copy(q, s, d, skip):
        count = chunk[q] - skip
        return remote(
            "grad", part_sem(q, s),
            buf["grad"].at[pl.ds(s * both_q + lead[q] + skip, count)],
            buf["gr"].at[s - ship, pl.ds(lead1[q] + (d - 1) * chunk[q] + skip, count)],
            "mem", to_first(q, d),
        )

    def arrived_split(kind, ref, some, short, full):
        for q in range(2):
            if first[q] > 1:
                index = part_sem(q, ship)
                if extra:
                    pl.when(some(q))(
                        lambda q=q, index=index: arrived(kind, index, ref.at[pl.ds(0, short(q))])
                    )
                    pl.when(jnp.logical_not(some(q)))(
                        lambda q=q, index=index: arrived(kind, index, ref.at[pl.ds(0, full(q))])
                    )
                else:
                    arrived(kind, index, ref.at[pl.ds(0, (first[q] - 1) * chunk[q])])

    def proj_copy(q, d):
        return remote(
            "proj", 0, buf["pp"].at[slot(q, d)], buf["pr"].at[slot(q, d)],
            "mem", back_first(q, d),
        )

    def to_both(kind, src, dst):
        return (
            remote(kind, 0, src, dst.at[0], "tile", nxt),
            remote(kind, 0, src, dst.at[1], "tile", prv),
        )

    ip, ov = buf["ip"], buf["ov"]

    def halo(s):
        where = pl.ds(s * both_q, both_q)
        return (
            remote("halo", s, ip.at[pl.ds(rows, 2), where], ip.at[pl.ds(0, 2), where], "tile", nxt),
            remote("halo", s, ip.at[pl.ds(2, 2), where], ip.at[pl.ds(rows + 2, 2), where], "tile", prv),
        )

    c_copy = to_both("control", control, buf["ch"])
    w_copy = to_both("weight", obs, buf["wh"])
    last = buf["last"]
    p_copy = to_both("field", last, buf["ph"])
    o_copy = (
        remote("innov", 0, ov.at[rows], ov.at[0], "tile", nxt),
        remote("innov", 0, ov.at[1], ov.at[rows + 1], "tile", prv),
    )

    if sent:
        where = e_v.at[:, pl.ds(0, early_planes)]
        load(0, where, where).wait()
    for c in innov_load + late:
        c.start()
    for s in sent:
        for q, d in first_peers():
            where = pl.ds(start_of(q, ahead(q, d), s), chunk[q])
            for m in range(ml):
                e = e_v[m, where].astype(jnp.float32)
                at = (lead1[q] + (d - 1) * chunk[q]) * ml + m * chunk[q]
                for c in range(nc):
                    buf["es"][s, at : at + chunk[q], c] = e[:, :, lanes(c)]
    if extra:
        for q, d in first_peers():
            where = pl.ds(start_of(q, ahead(q, d), ship), extra)
            for m in range(ml):
                e = e_v[m, where].astype(jnp.float32)
                at = (slot(q, d) * ml + m) * extra
                for c in range(nc):
                    buf["xs"][at : at + extra, c] = e[:, :, lanes(c)]
    pl.semaphore_wait(barrier, len(greet) + a - 1 + b - 1)
    for s in sent:
        for q, d in first_peers():
            ship_copy(q, s, d).start()
    if extra:
        for q, d in first_peers():
            pl.when(takes(ahead(q, d)))(lambda q=q, d=d: extra_copy(q, d).start())
    for c in arg_load[:2]:
        c.wait()
    for c in c_copy + w_copy:
        c.start()

    load(2, buf["iv"], buf["iv"]).wait()
    flat_iv = buf["iv"].reshape(steps * both_q * nc * rows, LANES)

    @pl.loop(0, steps * both_q // 8)
    def _(j):
        for c in range(nc):
            for r in range(rows):
                ov[1 + r, pl.ds(pl.multiple_of(j * 8, 8), 8), lanes(c)] = flat_iv[
                    pl.ds(j * (8 * nc * rows) + c * rows + r, 8, stride=nc * rows), :
                ]

    for c in o_copy:
        c.start()
    for c in arg_load[2:]:
        c.wait()
    coef = buf["coef"]
    sub = lax.broadcasted_iota(jnp.int32, (8, LANES), 0)
    for q in range(2):

        @pl.loop(0, size[q] // 8)
        def _(j):
            s = j // (chunk[q] // 8)
            at = pl.multiple_of(s * both_q + lead[q] + (j % (chunk[q] // 8)) * 8, 8)
            k = start_of(q, fi[q], 0) + j * 8
            for kind, value in enumerate((
                lambda i: advect[0, i], lambda i: advect[1, i], lambda i: damping[i]
            )):
                v = jnp.full((8, LANES), value(k), jnp.float32)
                for i in range(1, 8):
                    v = jnp.where(sub == i, value(k + i), v)
                coef[kind, pl.ds(at, 8)] = v

    rates = jnp.concatenate(
        [jnp.full((3 * rows, ny), spread[band[m]], jnp.float32) for m in range(ml)], axis=0
    )
    arrived("control", 0, buf["ch"])
    field = []
    for m in range(ml):
        field += [buf["ch"][0, m], control[m], buf["ch"][1, m]]
    field = sweeps(jnp.concatenate(field, axis=0), rates)
    for m in range(ml):
        center = field[(3 * m + 1) * rows : (3 * m + 2) * rows]
        loc[m] = center
        scl[m] = weights[m] * center
        proj[m] = jnp.zeros_like(center)
        for q, d in first_peers():
            buf["pp"][slot(q, d), m] = jnp.zeros_like(center)
    if sent:
        for q, d in first_peers():
            scl_copy(q, d).start()
    where = e_v.at[:, pl.ds(0, vl - early_planes)]
    load(1, where, where).wait()

    def own_sum(q, owner, s, c):
        where = pl.ds(start_of(q, owner, s), chunk[q])
        total = None
        for m in range(ml):
            term = e_v[m, where, :, lanes(c)].astype(jnp.float32) * scl[m, :, lanes(c)][None]
            total = term if total is None else total + term
        return total

    for s in lone:
        for q, d in first_peers():
            for c in range(nc):
                buf["to"][s - ship, block1(q, d), c] = own_sum(q, ahead(q, d), s, c)
            split(part_copy, q, s, d, ahead(q, d))
    for s in range(steps):
        for q in range(2):
            for c in range(nc):
                buf["part"][own(q, s), c] = own_sum(q, fi[q], s, c)
    arrived("weight", 0, buf["wh"])
    wb = buf["wb"]
    wb[0] = jnp.broadcast_to(buf["wh"][0, rows - 1 :], (8, ny))
    wb[rows + 1] = jnp.broadcast_to(buf["wh"][1, :1], (8, ny))
    for r in range(rows):
        wb[1 + r] = jnp.broadcast_to(obs[r : r + 1], (8, ny))

    def add_first(s):
        if some_first:
            if s > ship:
                arrived("part", s - ship, buf["r1"].at[s - ship])
            elif s == ship:
                arrived_split(
                    "part", buf["r1"].at[0], lambda q: takes(fi[q]),
                    lambda q: (first[q] - 1) * (chunk[q] - extra),
                    lambda q: (first[q] - 1) * chunk[q],
                )
                for q in range(2):
                    if extra and first[q] > 1:
                        where = pl.ds(0, (first[q] - 1) * ml * extra)
                        pl.when(takes(fi[q]))(
                            lambda q=q, where=where: arrived("extra", q, buf["xr"].at[where])
                        )
            else:
                arrived("ship", s, buf["er"].at[s])
        skip = extra if s == ship else 0
        for q in range(2):
            rest = pl.ds(s * both_q + lead[q] + skip, chunk[q] - skip)
            for c in range(nc):
                total = buf["part"][rest, c]
                for d in range(1, first[q]):
                    if s >= ship:
                        at = lead1[q] + (d - 1) * chunk[q]
                        total = total + buf["r1"][s - ship, at + skip : at + chunk[q], c]
                    else:
                        for m in range(ml):
                            at = (lead1[q] + (d - 1) * chunk[q]) * ml + m * chunk[q]
                            total = total + (
                                buf["er"][s, at : at + chunk[q], c]
                                * buf["sr"][slot(q, d), m, :, lanes(c)][None]
                            )
                buf["part"][rest, c] = total
            if s == ship and extra and first[q] > 1:
                head = pl.ds(s * both_q + lead[q], extra)

                @pl.when(takes(fi[q]))
                def _(q=q, head=head):
                    for c in range(nc):
                        total = buf["part"][head, c]
                        for d in range(1, first[q]):
                            for m in range(ml):
                                at = (slot(q, d) * ml + m) * extra
                                total = total + (
                                    buf["xr"][at : at + extra, c]
                                    * buf["sr"][slot(q, d), m, :, lanes(c)][None]
                                )
                        buf["part"][head, c] = total

                @pl.when(jnp.logical_not(takes(fi[q])))
                def _(q=q, head=head):
                    for c in range(nc):
                        total = buf["part"][head, c]
                        for d in range(1, first[q]):
                            at = lead1[q] + (d - 1) * chunk[q]
                            total = total + buf["r1"][0, at : at + extra, c]
                        buf["part"][head, c] = total

            for d in range(1, second[q]):
                swap_copy(q, s, d).start()

    def add_second(s):
        if some_second:
            arrived("swap", s, buf["r2"].at[s])
        rows_of = lambda planes: planes * nc * rows
        flat = buf["part"].reshape(rows_of(steps * both_q), LANES)
        for q in range(2):
            peers = [
                buf["r2"].at[s, block2(q, d)].reshape(rows_of(chunk[q]), LANES)
                for d in range(1, second[q])
            ]
            base = s * both_q + lead[q]

            @pl.loop(0, chunk[q] // 8)
            def _(j):
                for c in range(nc):
                    for r in range(rows):
                        at = j * rows_of(8) + c * rows + r
                        total = flat[pl.ds(rows_of(base) + at, 8, stride=nc * rows), :]
                        for p in peers:
                            total = total + p[pl.ds(at, 8, stride=nc * rows), :]
                        ip[2 + r, pl.ds(pl.multiple_of(base + j * 8, 8), 8), lanes(c)] = total

        for c in halo(s):
            c.start()

    def adjoint(s):
        arrived("halo", s, ip.at[pl.ds(0, 4), pl.ds(s * both_q, both_q)])
        col = lax.broadcasted_iota(jnp.int32, (8, ny), 1)
        flat = buf["grad"].reshape(steps * both_q * nc * rows, LANES)

        @pl.loop(0, both_q // 8)
        def _(j):
            where = pl.ds(pl.multiple_of(s * both_q + j * 8, 8), 8)
            ax, ay, e = (jnp.concatenate([coef[k, where]] * nc, axis=1) for k in range(3))
            mid = 1.0 - 4.0 * e
            up = e - 0.5 * ax
            down = e + 0.5 * ax
            left_c = e - 0.5 * ay
            right_c = e + 0.5 * ay
            north1 = jnp.where(col == ny - 1, 0.0, left_c)
            south1 = jnp.where(col == 0, 0.0, right_c)
            north2 = jnp.where(col == ny - 1, 0.0, right_c)
            south2 = jnp.where(col == 0, 0.0, left_c)

            def turn(f):
                return pltpu.roll(f, ny - 1, 1), pltpu.roll(f, 1, 1)

            f = [ip[r, where, :] for r in range(rows + 4)]
            w = []
            for r in range(1, rows + 3):
                north, south = turn(f[r])
                d = (
                    mid * f[r] + up * f[r + 1] + down * f[r - 1]
                    + north1 * north + south1 * south
                )
                w.append(wb[r - 1] * (d - ov[r - 1, where, :]))
            for r in range(1, rows + 1):
                north, south = turn(w[r])
                g = (
                    mid * w[r] + down * w[r + 1] + up * w[r - 1]
                    + north2 * north + south2 * south
                )
                for c in range(nc):
                    at = (s * both_q + j * 8) * (nc * rows) + c * rows + r - 1
                    flat[pl.ds(at, 8, stride=nc * rows), :] = g[:, lanes(c)]

        if s >= ship:
            for q, d in first_peers():
                split(grad_copy, q, s, d, fi[q])

    def project_peers(s):
        for q, d in first_peers():
            for c in range(nc):
                g = buf["grad"][own(q, s), c]
                for m in range(ml):
                    at = (lead1[q] + (d - 1) * chunk[q]) * ml + m * chunk[q]
                    e = buf["er"][s, at : at + chunk[q], c]
                    buf["pp"][slot(q, d), m, :, lanes(c)] += jnp.sum(e * g, axis=0)
        if s == ship - 1:
            for q, d in first_peers():
                proj_copy(q, d).start()

    def project_own(s):
        for q in range(2):
            where = pl.ds(start_of(q, fi[q], s), chunk[q])
            for c in range(nc):
                g = buf["grad"][own(q, s), c]
                for m in range(ml):
                    e = e_v[m, where, :, lanes(c)].astype(jnp.float32)
                    proj[m, :, lanes(c)] += jnp.sum(e * g, axis=0)

            if s == ship and extra and first[q] > 1:

                @pl.when(takes(fi[q]))
                def _(q=q):
                    for c in range(nc):
                        g = buf["grad"][pl.ds(s * both_q + lead[q], extra), c]
                        for d in range(1, first[q]):
                            for m in range(ml):
                                at = (slot(q, d) * ml + m) * extra
                                e = buf["xr"][at : at + extra, c]
                                buf["pp"][slot(q, d), m, :, lanes(c)] += jnp.sum(e * g, axis=0)

    def project_in(s):
        if s == ship:
            arrived_split(
                "grad", buf["gr"].at[0], lambda q: jnp.logical_not(takes(fi[q])),
                lambda q: (first[q] - 1) * (chunk[q] - extra),
                lambda q: (first[q] - 1) * chunk[q] - (first[q] - 2) * extra,
            )
        else:
            arrived("grad", s - ship, buf["gr"].at[s - ship])

        def add(q, d, start, count):
            where = pl.ds(start_of(q, behind(q, d), s) + start, count)
            at = lead1[q] + (d - 1) * chunk[q] + start
            for c in range(nc):
                g = buf["gr"][s - ship, at : at + count, c]
                for m in range(ml):
                    e = e_v[m, where, :, lanes(c)].astype(jnp.float32)
                    proj[m, :, lanes(c)] += jnp.sum(e * g, axis=0)

        for q, d in first_peers():
            if s == ship and extra:
                add(q, d, extra, chunk[q] - extra)
                pl.when(jnp.logical_not(takes(behind(q, d))))(
                    lambda q=q, d=d: add(q, d, 0, extra)
                )
            else:
                add(q, d, 0, chunk[q])

    scope = jax.named_scope
    if sent:
        arrived("scl", 0, buf["sr"])
    for s in order:
        with scope(f"add_first{s}"):
            add_first(s)
    for tick in range(steps + LAG):
        if tick < steps:
            with scope(f"add_second{order[tick]}"):
                add_second(order[tick])
        if tick == LAG:
            arrived("innov", 0, ov.at[pl.ds(0, 2)])
        if tick >= LAG:
            s = order[tick - LAG]
            with scope(f"adjoint{s}"):
                adjoint(s)
            if s in sent:
                with scope(f"project_peers{s}"):
                    project_peers(s)
            with scope(f"project_own{s}"):
                project_own(s)
    if some_first:
        for s in lone:
            with scope(f"project_in{s}"):
                project_in(s)
    with scope("tail"):
        if sent:
            arrived("proj", 0, buf["pr"])
        for m in range(ml):
            total = proj[m]
            if sent:
                for q, d in first_peers():
                    total = total + buf["pr"][slot(q, d), m]
            proj[m] = total
            last[m] = weights[m] * total
    with scope("halo_out"):
        for c in p_copy:
            c.start()
        gwr = buf["gwr"]
        for m in range(ml):
            v = jnp.sum(loc[m] * proj[m], axis=0, keepdims=True)
            gwr[t, m : m + 1] = sum(v[:, lanes(c)] for c in range(nc))
        for d in range(1, tiles):
            remote("gw", 0, gwr.at[t], gwr.at[t], "tile", (t + d) % tiles).start()
        arrived("field", 0, buf["ph"])
    with scope("sweeps"):
        field = []
        for m in range(ml):
            field += [buf["ph"][0, m], last[m], buf["ph"][1, m]]
        field = sweeps(jnp.concatenate(field, axis=0), rates)
        for m in range(ml):
            out[m] = control[m] + field[(3 * m + 1) * rows : (3 * m + 2) * rows]
    with scope("finish"):
        if tiles > 1:
            arrived("gw", 0, gwr.at[pl.ds(0, tiles - 1)])
        total = gwr[0]
        for d in range(1, tiles):
            total = total + gwr[d]
        total = jnp.broadcast_to(jnp.sum(total, axis=1, keepdims=True), (ml, LANES))
        row = lax.broadcasted_iota(jnp.int32, (ml, LANES), 0)
        lane = lax.broadcasted_iota(jnp.int32, (ml, LANES), 1)
        sums = jnp.sum(jnp.where(row == lane, total, 0.0), axis=0)
        gw_out[...] = sums[:ml] / math.sqrt(tiles * rows * ny * vl)
        def all_left(count):
            ref = buf["all"].at[pl.ds(0, count)]
            remote("gw", 0, ref, ref, "tile", nxt).wait_send()

        if extra:
            for case in range(4):
                is_first = (case % 2 == 0, case // 2 == 0)
                change = 0
                for q in range(2):
                    if first[q] > 1:
                        out = first[q] - 1 if is_first[q] else first[q] - 2
                        change += out * (ml - 1) * extra
                        change -= 0 if is_first[q] else (first[q] - 1) * extra
                here = jnp.logical_and(
                    (fi[0] == 0) == is_first[0], (fi[1] == 0) == is_first[1]
                )
                pl.when(here)(functools.partial(all_left, sent_rows + change * nc * rows))
        else:
            all_left(sent_rows)


def store(field, sums, out, gw, sem):
    copies = [
        pltpu.make_async_copy(src, dst, sem.at[i])
        for i, (src, dst) in enumerate(((field, out), (sums, gw)))
    ]
    for c in copies:
        c.start()
    for c in copies:
        c.wait()


def per_device(
    n, tiles,
    ensemble, control, weights, member_band, spread, advect, damping, innovation, obs_weight
):
    ml, vl, rows, ny = ensemble.shape
    a, b = factors(n)
    first, second = (b, a), (a, b)
    assert rows == SWEEPS and ny % LANES == 0 and ml <= 8 and vl % (16 * b) == 0
    assert tiles > 2
    nc = ny // LANES
    size = [vl // (2 * f) for f in first]
    steps = max(d for d in range(1, CHUNKS + 1) if all(k % (8 * d) == 0 for k in size))
    ship = steps * SHIPPED // CHUNKS
    chunk = [k // steps for k in size]
    f32 = jnp.float32
    dma = pltpu.SemaphoreType.DMA
    hbm = pl.BlockSpec(memory_space=pl.ANY)
    whole = pl.BlockSpec(memory_space=pltpu.VMEM)
    field = (rows, ny)
    tile = (nc, rows, LANES)
    vmem = lambda *shape: pltpu.VMEM(shape, f32)
    links = max(sum(f - 1 for f in first), 1)
    block1 = max(sum((f - 1) * k for f, k in zip(first, chunk)), 8)
    block2 = max(sum((g - 1) * k for g, k in zip(second, chunk)), 8)
    ns, nl = max(ship, 1), max(steps - ship, 1)
    total = sum(size)
    out1 = sum((f - 1) * k for f, k in zip(first, chunk))
    out2 = sum((g - 1) * k for g, k in zip(second, chunk))
    fields = 2 * (steps - ship) * out1 + steps * out2 + 4 * ml + 2
    if ship:
        fields += ship * ml * out1 + 2 * ml * sum(f - 1 for f in first)
    sent_rows = fields * nc * rows + 6 * total * nc + (tiles - 1) * ml
    buf = {
        "es": vmem(ns, ml * block1, *tile),
        "er": vmem(ns, ml * block1, *tile),
        "to": vmem(nl, block1, *tile),
        "r1": vmem(nl, block1, *tile),
        "part": vmem(total, *tile),
        "r2": vmem(steps, block2, *tile),
        "grad": vmem(total, *tile),
        "gr": vmem(nl, block1, *tile),
        "iv": vmem(total, *tile),
        "ip": vmem(rows + 4, total, ny),
        "ov": vmem(rows + 2, total, ny),
        "coef": vmem(3, total, LANES),
        "pp": vmem(links, ml, *field),
        "pr": vmem(links, ml, *field),
        "sr": vmem(links, ml, *field),
        "loc": vmem(ml, *field),
        "scl": vmem(ml, *field),
        "proj": vmem(ml, *field),
        "ch": vmem(2, ml, *field),
        "wh": vmem(2, *field),
        "wb": vmem(rows + 2, 8, ny),
        "ph": vmem(2, ml, *field),
        "gwr": vmem(tiles, ml, LANES),
        "last": vmem(ml, *field),
        "all": vmem(sent_rows + 2 * links * ml * EXTRA * nc * rows, LANES),
        "xs": vmem(links * ml * EXTRA, *tile),
        "xr": vmem(links * ml * EXTRA, *tile),
    }
    sems = {
        "sent": dma((1,)), "ship": dma((ns,)), "scl": dma((1,)), "part": dma((nl + 1,)),
        "swap": dma((steps,)), "grad": dma((nl + 1,)), "extra": dma((2,)), "proj": dma((1,)), "control": dma((1,)),
        "weight": dma((1,)), "innov": dma((1,)), "field": dma((1,)), "halo": dma((steps,)),
        "gw": dma((1,)),
    }
    args = (
        vmem(*control.shape),
        vmem(*obs_weight.shape),
        pltpu.SMEM(weights.shape, f32),
        pltpu.SMEM(member_band.shape, member_band.dtype),
        pltpu.SMEM(spread.shape, f32),
        pltpu.SMEM(advect.shape, f32),
        pltpu.SMEM(damping.shape, f32),
    )
    out, gw = pl.pallas_call(
        functools.partial(kernel, n, tiles, steps, ship, sent_rows),
        out_shape=(pltpu.VMEM((ml, rows, ny), f32), pltpu.VMEM((ml,), f32)),
        in_specs=[hbm] * 9,
        out_specs=(whole, whole),
        scratch_shapes=[args, dma((10,)), pltpu.VMEM((ml, vl) + field, ensemble.dtype), buf, sems],
        compiler_params=pltpu.CompilerParams(
            collective_id=0, has_side_effects=True, vmem_limit_bytes=63 * 1024 * 1024
        ),
    )(ensemble, control, weights, member_band, spread, advect, damping, innovation, obs_weight)
    return pl.pallas_call(
        store,
        out_shape=(
            jax.ShapeDtypeStruct((ml, rows, ny), f32),
            jax.ShapeDtypeStruct((ml,), f32),
        ),
        in_specs=[whole, whole],
        out_specs=(hbm, hbm),
        scratch_shapes=[dma((2,))],
    )(*(pltpu.with_memory_space_constraint(x, pltpu.VMEM) for x in (out, gw)))


def solution(mesh):
    in_specs = (
        P("mem", None, "tile", None),
        P("mem", "tile", None),
        P("mem"),
        P("mem"),
        P(),
        P(),
        P(),
        P(None, "tile", None),
        P("tile", None),
    )
    out_specs = (P("mem", "tile", None), P("mem"))
    return jax.shard_map(
        functools.partial(per_device, mesh.shape["mem"], mesh.shape["tile"]),
        mesh=mesh, in_specs=in_specs, out_specs=out_specs, check_vma=False,
    )
```

```python
import functools
import math

import jax
import jax.numpy as jnp
from jax import lax
from jax.experimental import pallas as pl
from jax.experimental.pallas import tpu as pltpu
from jax.sharding import PartitionSpec as P

SWEEPS = 8
CHUNKS = 4
SHIPPED = 1
AFTER = 9
LAG = 1
EXTRA = 4
LANES = 128
MESH = pl.DeviceIdType.MESH


def factors(n):
    a = max(d for d in range(1, n + 1) if n % d == 0 and d * d <= n)
    return a, n // a


def sweeps(f, rates):
    rows, ny = f.shape
    col = lax.broadcasted_iota(jnp.int32, f.shape, 1)
    inside = jnp.where(col == 0, 1.0, jnp.where(col == ny - 1, 1.0, 2.0))
    c = 1.0 - 4.0 * rates
    one = 2.0 * c * rates
    two = rates * rates
    here = c * c + two * inside

    def along_x(g):
        return pltpu.roll(g, rows - 1, 0) + pltpu.roll(g, 1, 0)

    def along_y(g, k):
        return jnp.where(col < ny - k, pltpu.roll(g, ny - k, 1), 0.0) + jnp.where(
            col >= k, pltpu.roll(g, k, 1), 0.0
        )

    for _ in range(SWEEPS // 2):
        near = along_y(f, 1)
        inner = one * f + two * along_x(f) + (2.0 * two) * near
        f = here * f + one * near + two * along_y(f, 2) + along_x(inner)
    return f


def kernel(
    n, tiles, steps, ship, sent_rows,
    ens, control_h, weights_h, band_h, spread_h, advect_h, damping_h, innov, obs_h,
    out, gw_out,
    args, arg_sem, e_v, buf, sems,
):
    a, b = factors(n)
    both_in, weights, band, spread, advect, damping = args
    ml = both_in.shape[0] - 1
    control, obs = both_in.at[pl.ds(0, ml)], both_in.at[ml]
    loc, scl, proj = buf["loc"], buf["scl"], buf["proj"]
    _, rows, ny = both_in.shape
    vl = ens.shape[1]
    nc = ny // LANES
    me = lax.axis_index("mem")
    t = lax.axis_index("tile")
    nxt = (t + 1) % tiles
    prv = (t + tiles - 1) % tiles
    ia = me // b
    ib = me % b
    first = (b, a)
    second = (a, b)
    fi = (ib, ia)
    gi = (ia, ib)
    size = [vl // (2 * f) for f in first]
    chunk = [k // steps for k in size]
    both_q = sum(chunk)
    lead = (0, chunk[0])
    lead1 = (0, (first[0] - 1) * chunk[0])
    lead2 = (0, (second[0] - 1) * chunk[0])
    some_first = sum(f - 1 for f in first) > 0
    some_second = sum(g - 1 for g in second) > 0
    lone = tuple(range(ship, steps))
    sent = tuple(range(ship)) if some_first else ()
    extra = EXTRA if sent and min(chunk) > EXTRA else 0
    order = lone[:AFTER] + tuple(range(ship)) + lone[AFTER:]
    near = tiles // 2 <= 2 + steps
    greet = sorted({1, tiles - 1}) if near else list(range(1, tiles))
    greet = [d for d in greet if d % tiles]

    def device(q, f, g):
        return g * b + f if q == 0 else f * b + g

    def start_of(q, owner, s):
        return pl.multiple_of(q * (vl // 2) + (owner * steps + s) * chunk[q], chunk[q])

    def ahead(q, d):
        return (fi[q] + d) % first[q]

    def behind(q, d):
        return (fi[q] + first[q] - d) % first[q]

    def to_first(q, d):
        return device(q, ahead(q, d), gi[q])

    def back_first(q, d):
        return device(q, behind(q, d), gi[q])

    def to_second(q, d):
        return device(q, fi[q], (gi[q] + d) % second[q])

    def first_peers():
        return [(q, d) for q in range(2) for d in range(1, first[q])]

    def second_peers():
        return [(q, d) for q in range(2) for d in range(1, second[q])]

    def remote(kind, index, src, dst, axis, dev):
        return pltpu.make_async_remote_copy(
            src_ref=src, dst_ref=dst, send_sem=sems["sent"].at[0], recv_sem=sems[kind].at[index],
            device_id={axis: dev}, device_id_type=MESH,
        )

    def arrived(kind, index, ref):
        remote(kind, index, ref, ref, "tile", nxt).wait_recv()

    def lanes(c):
        return slice(c * LANES, (c + 1) * LANES)

    def load(k, src, dst):
        return pltpu.make_async_copy(src, dst, arg_sem.at[k])

    def ens_load(k, q, owner, start, count):
        where = pl.ds(start_of(q, owner, 0) + start, count)
        return load(k, ens.at[:, where], e_v.at[:, where])

    soon = [ship * k + extra for k in chunk]
    early = [ens_load(0, q, ahead(q, d), 0, soon[q]) for q, d in first_peers() if ship]
    late = [ens_load(1, q, fi[q], 0, size[q]) for q in range(2)]
    late += [ens_load(1, q, ahead(q, d), soon[q], size[q] - soon[q]) for q, d in first_peers()]
    innov_load = [
        load(
            2,
            innov.at[pl.ds(start_of(q, fi[q], s), chunk[q]), :, lanes(c)],
            buf["iv"].at[pl.ds(s * both_q + lead[q], chunk[q]), c],
        )
        for s in range(steps)
        for q in range(2)
        for c in range(nc)
    ]
    arg_load = [
        load(3 + i, src, dst)
        for i, (src, dst) in enumerate((
            (control_h, control), (obs_h, obs), (weights_h, weights), (band_h, band),
            (spread_h, spread), (advect_h, advect), (damping_h, damping),
        ))
    ]
    for c in early:
        c.start()
    barrier = pltpu.get_barrier_semaphore()
    for q, d in first_peers():
        pl.semaphore_signal(
            barrier, inc=1, device_id={"mem": to_first(q, d)}, device_id_type=MESH
        )
    for d in greet:
        pl.semaphore_signal(
            barrier, inc=1, device_id={"tile": (t + d) % tiles}, device_id_type=MESH
        )
    for c in arg_load + innov_load + late:
        c.start()
    early_planes = sum((first[q] - 1) * soon[q] for q in range(2))

    def block1(q, d, per=1):
        return pl.ds((lead1[q] + (d - 1) * chunk[q]) * per, chunk[q] * per)

    def block2(q, d):
        return pl.ds(lead2[q] + (d - 1) * chunk[q], chunk[q])

    def own(q, s):
        return pl.ds(s * both_q + lead[q], chunk[q])

    def slot(q, d):
        return (first[0] - 1) * q + d - 1

    def ship_copy(q, s, d):
        where = block1(q, d, ml)
        return remote(
            "ship", s, buf["es"].at[s, where], buf["er"].at[s, where], "mem", to_first(q, d)
        )

    def scl_copy(q, d):
        return remote("scl", 0, scl, buf["sr"].at[slot(q, d)], "mem", to_first(q, d))

    def part_copy(q, s, d, skip):
        where = pl.ds(lead1[q] + (d - 1) * chunk[q] + skip, chunk[q] - skip)
        return remote(
            "part", part_sem(q, s), buf["to"].at[s - ship, where], buf["r1"].at[s - ship, where],
            "mem", to_first(q, d),
        )

    def takes(coordinate):
        return coordinate != 0

    def extra_copy(q, d):
        where = pl.ds(((first[0] - 1) * q + d - 1) * ml * extra, ml * extra)
        return remote(
            "extra", q, buf["xs"].at[where], buf["xr"].at[where], "mem", to_first(q, d)
        )

    def split(copy, q, s, d, coordinate):
        if s == ship and extra:
            pl.when(takes(coordinate))(lambda: copy(q, s, d, extra).start())
            pl.when(jnp.logical_not(takes(coordinate)))(lambda: copy(q, s, d, 0).start())
        else:
            copy(q, s, d, 0).start()

    def part_sem(q, s):
        return s - ship if s > ship or q == 0 else steps - ship

    def swap_copy(q, s, d):
        return remote(
            "swap", s, buf["part"].at[own(q, s)], buf["r2"].at[s, block2(q, d)],
            "mem", to_second(q, d),
        )

    def grad_copy(q, s, d, skip):
        count = chunk[q] - skip
        return remote(
            "grad", part_sem(q, s),
            buf["grad"].at[pl.ds(s * both_q + lead[q] + skip, count)],
            buf["gr"].at[s - ship, pl.ds(lead1[q] + (d - 1) * chunk[q] + skip, count)],
            "mem", to_first(q, d),
        )

    def arrived_split(kind, ref, some, short, full):
        for q in range(2):
            if first[q] > 1:
                index = part_sem(q, ship)
                if extra:
                    pl.when(some(q))(
                        lambda q=q, index=index: arrived(kind, index, ref.at[pl.ds(0, short(q))])
                    )
                    pl.when(jnp.logical_not(some(q)))(
                        lambda q=q, index=index: arrived(kind, index, ref.at[pl.ds(0, full(q))])
                    )
                else:
                    arrived(kind, index, ref.at[pl.ds(0, (first[q] - 1) * chunk[q])])

    def proj_copy(q, d):
        return remote(
            "proj", 0, buf["pp"].at[slot(q, d)], buf["pr"].at[slot(q, d)],
            "mem", back_first(q, d),
        )

    def to_both(kind, src, dst):
        return (
            remote(kind, 0, src, dst.at[0], "tile", nxt),
            remote(kind, 0, src, dst.at[1], "tile", prv),
        )

    ip, ov = buf["ip"], buf["ov"]

    def halo(s):
        where = pl.ds(s * both_q, both_q)
        return (
            remote("halo", s, ip.at[pl.ds(rows, 2), where], ip.at[pl.ds(0, 2), where], "tile", nxt),
            remote("halo", s, ip.at[pl.ds(2, 2), where], ip.at[pl.ds(rows + 2, 2), where], "tile", prv),
        )

    c_copy = to_both("control", both_in, buf["ch"])
    last = buf["last"]
    p_copy = to_both("field", last, buf["ph"])
    o_copy = (
        remote("innov", 0, ov.at[rows], ov.at[0], "tile", nxt),
        remote("innov", 0, ov.at[1], ov.at[rows + 1], "tile", prv),
    )

    if sent:
        where = e_v.at[:, pl.ds(0, early_planes)]
        load(0, where, where).wait()
    for s in sent:
        for q, d in first_peers():
            where = pl.ds(start_of(q, ahead(q, d), s), chunk[q])
            for m in range(ml):
                e = e_v[m, where].astype(jnp.float32)
                at = (lead1[q] + (d - 1) * chunk[q]) * ml + m * chunk[q]
                for c in range(nc):
                    buf["es"][s, at : at + chunk[q], c] = e[:, :, lanes(c)]
    if extra:
        for q, d in first_peers():
            where = pl.ds(start_of(q, ahead(q, d), ship), extra)
            for m in range(ml):
                e = e_v[m, where].astype(jnp.float32)
                at = (slot(q, d) * ml + m) * extra
                for c in range(nc):
                    buf["xs"][at : at + extra, c] = e[:, :, lanes(c)]
    pl.semaphore_wait(barrier, len(greet) + a - 1 + b - 1)
    for s in sent:
        for q, d in first_peers():
            ship_copy(q, s, d).start()
    if extra:
        for q, d in first_peers():
            pl.when(takes(ahead(q, d)))(lambda q=q, d=d: extra_copy(q, d).start())
    for c in arg_load[:2]:
        c.wait()
    for c in c_copy:
        c.start()

    load(2, buf["iv"], buf["iv"]).wait()
    flat_iv = buf["iv"].reshape(steps * both_q * nc * rows, LANES)

    @pl.loop(0, steps * both_q // 8)
    def _(j):
        for c in range(nc):
            for r in range(rows):
                ov[1 + r, pl.ds(pl.multiple_of(j * 8, 8), 8), lanes(c)] = flat_iv[
                    pl.ds(j * (8 * nc * rows) + c * rows + r, 8, stride=nc * rows), :
                ]

    for c in o_copy:
        c.start()
    for c in arg_load[2:]:
        c.wait()
    coef = buf["coef"]
    sub = lax.broadcasted_iota(jnp.int32, (8, LANES), 0)
    for q in range(2):

        @pl.loop(0, size[q] // 8)
        def _(j):
            s = j // (chunk[q] // 8)
            at = pl.multiple_of(s * both_q + lead[q] + (j % (chunk[q] // 8)) * 8, 8)
            k = start_of(q, fi[q], 0) + j * 8
            for kind, value in enumerate((
                lambda i: advect[0, i], lambda i: advect[1, i], lambda i: damping[i]
            )):
                v = jnp.full((8, LANES), value(k), jnp.float32)
                for i in range(1, 8):
                    v = jnp.where(sub == i, value(k + i), v)
                coef[kind, pl.ds(at, 8)] = v

    rates = jnp.concatenate(
        [jnp.full((3 * rows, ny), spread[band[m]], jnp.float32) for m in range(ml)], axis=0
    )
    arrived("control", 0, buf["ch"])
    field = []
    for m in range(ml):
        field += [buf["ch"][0, m], control[m], buf["ch"][1, m]]
    field = sweeps(jnp.concatenate(field, axis=0), rates)
    for m in range(ml):
        center = field[(3 * m + 1) * rows : (3 * m + 2) * rows]
        loc[m] = center
        scl[m] = weights[m] * center
        proj[m] = jnp.zeros_like(center)
        for q, d in first_peers():
            buf["pp"][slot(q, d), m] = jnp.zeros_like(center)
    if sent:
        for q, d in first_peers():
            scl_copy(q, d).start()
    where = e_v.at[:, pl.ds(0, vl - early_planes)]
    load(1, where, where).wait()

    def own_sum(q, owner, s, c):
        where = pl.ds(start_of(q, owner, s), chunk[q])
        total = None
        for m in range(ml):
            term = e_v[m, where, :, lanes(c)].astype(jnp.float32) * scl[m, :, lanes(c)][None]
            total = term if total is None else total + term
        return total

    for s in lone:
        for q, d in first_peers():
            for c in range(nc):
                buf["to"][s - ship, block1(q, d), c] = own_sum(q, ahead(q, d), s, c)
            split(part_copy, q, s, d, ahead(q, d))
    for s in range(steps):
        for q in range(2):
            for c in range(nc):
                buf["part"][own(q, s), c] = own_sum(q, fi[q], s, c)
    wb = buf["wb"]
    wb[0] = jnp.broadcast_to(buf["ch"][0, ml, rows - 1 :], (8, ny))
    wb[rows + 1] = jnp.broadcast_to(buf["ch"][1, ml, :1], (8, ny))
    for r in range(rows):
        wb[1 + r] = jnp.broadcast_to(obs[r : r + 1], (8, ny))

    def add_first(s):
        if some_first:
            if s > ship:
                arrived("part", s - ship, buf["r1"].at[s - ship])
            elif s == ship:
                arrived_split(
                    "part", buf["r1"].at[0], lambda q: takes(fi[q]),
                    lambda q: (first[q] - 1) * (chunk[q] - extra),
                    lambda q: (first[q] - 1) * chunk[q],
                )
                for q in range(2):
                    if extra and first[q] > 1:
                        where = pl.ds(0, (first[q] - 1) * ml * extra)
                        pl.when(takes(fi[q]))(
                            lambda q=q, where=where: arrived("extra", q, buf["xr"].at[where])
                        )
            else:
                arrived("ship", s, buf["er"].at[s])
        skip = extra if s == ship else 0
        for q in range(2):
            rest = pl.ds(s * both_q + lead[q] + skip, chunk[q] - skip)
            for c in range(nc):
                total = buf["part"][rest, c]
                for d in range(1, first[q]):
                    if s >= ship:
                        at = lead1[q] + (d - 1) * chunk[q]
                        total = total + buf["r1"][s - ship, at + skip : at + chunk[q], c]
                    else:
                        for m in range(ml):
                            at = (lead1[q] + (d - 1) * chunk[q]) * ml + m * chunk[q]
                            total = total + (
                                buf["er"][s, at : at + chunk[q], c]
                                * buf["sr"][slot(q, d), m, :, lanes(c)][None]
                            )
                buf["part"][rest, c] = total
            if s == ship and extra and first[q] > 1:
                head = pl.ds(s * both_q + lead[q], extra)

                @pl.when(takes(fi[q]))
                def _(q=q, head=head):
                    for c in range(nc):
                        total = buf["part"][head, c]
                        for d in range(1, first[q]):
                            for m in range(ml):
                                at = (slot(q, d) * ml + m) * extra
                                total = total + (
                                    buf["xr"][at : at + extra, c]
                                    * buf["sr"][slot(q, d), m, :, lanes(c)][None]
                                )
                        buf["part"][head, c] = total

                @pl.when(jnp.logical_not(takes(fi[q])))
                def _(q=q, head=head):
                    for c in range(nc):
                        total = buf["part"][head, c]
                        for d in range(1, first[q]):
                            at = lead1[q] + (d - 1) * chunk[q]
                            total = total + buf["r1"][0, at : at + extra, c]
                        buf["part"][head, c] = total

            for d in range(1, second[q]):
                swap_copy(q, s, d).start()

    def add_second(s):
        if some_second:
            arrived("swap", s, buf["r2"].at[s])
        rows_of = lambda planes: planes * nc * rows
        flat = buf["part"].reshape(rows_of(steps * both_q), LANES)
        for q in range(2):
            peers = [
                buf["r2"].at[s, block2(q, d)].reshape(rows_of(chunk[q]), LANES)
                for d in range(1, second[q])
            ]
            base = s * both_q + lead[q]

            @pl.loop(0, chunk[q] // 8)
            def _(j):
                for c in range(nc):
                    for r in range(rows):
                        at = j * rows_of(8) + c * rows + r
                        total = flat[pl.ds(rows_of(base) + at, 8, stride=nc * rows), :]
                        for p in peers:
                            total = total + p[pl.ds(at, 8, stride=nc * rows), :]
                        ip[2 + r, pl.ds(pl.multiple_of(base + j * 8, 8), 8), lanes(c)] = total

        for c in halo(s):
            c.start()

    def adjoint(s):
        arrived("halo", s, ip.at[pl.ds(0, 4), pl.ds(s * both_q, both_q)])
        col = lax.broadcasted_iota(jnp.int32, (8, ny), 1)
        flat = buf["grad"].reshape(steps * both_q * nc * rows, LANES)

        @pl.loop(0, both_q // 8)
        def _(j):
            where = pl.ds(pl.multiple_of(s * both_q + j * 8, 8), 8)
            ax, ay, e = (jnp.concatenate([coef[k, where]] * nc, axis=1) for k in range(3))
            mid = 1.0 - 4.0 * e
            up = e - 0.5 * ax
            down = e + 0.5 * ax
            left_c = e - 0.5 * ay
            right_c = e + 0.5 * ay
            north1 = jnp.where(col == ny - 1, 0.0, left_c)
            south1 = jnp.where(col == 0, 0.0, right_c)
            north2 = jnp.where(col == ny - 1, 0.0, right_c)
            south2 = jnp.where(col == 0, 0.0, left_c)

            def turn(f):
                return pltpu.roll(f, ny - 1, 1), pltpu.roll(f, 1, 1)

            f = [ip[r, where, :] for r in range(rows + 4)]
            w = []
            for r in range(1, rows + 3):
                north, south = turn(f[r])
                d = (
                    mid * f[r] + up * f[r + 1] + down * f[r - 1]
                    + north1 * north + south1 * south
                )
                w.append(wb[r - 1] * (d - ov[r - 1, where, :]))
            for r in range(1, rows + 1):
                north, south = turn(w[r])
                g = (
                    mid * w[r] + down * w[r + 1] + up * w[r - 1]
                    + north2 * north + south2 * south
                )
                for c in range(nc):
                    at = (s * both_q + j * 8) * (nc * rows) + c * rows + r - 1
                    flat[pl.ds(at, 8, stride=nc * rows), :] = g[:, lanes(c)]

        if s >= ship:
            for q, d in first_peers():
                split(grad_copy, q, s, d, fi[q])

    def project_own(s):
        for q in range(2):
            where = pl.ds(start_of(q, fi[q], s), chunk[q])
            for c in range(nc):
                g = buf["grad"][own(q, s), c]
                for m in range(ml):
                    e = e_v[m, where, :, lanes(c)].astype(jnp.float32)
                    proj[m, :, lanes(c)] += jnp.sum(e * g, axis=0)
                if s < ship:
                    for d in range(1, first[q]):
                        for m in range(ml):
                            at = (lead1[q] + (d - 1) * chunk[q]) * ml + m * chunk[q]
                            e = buf["er"][s, at : at + chunk[q], c]
                            buf["pp"][slot(q, d), m, :, lanes(c)] += jnp.sum(e * g, axis=0)

            if s == ship and extra and first[q] > 1:

                @pl.when(takes(fi[q]))
                def _(q=q):
                    for c in range(nc):
                        g = buf["grad"][pl.ds(s * both_q + lead[q], extra), c]
                        for d in range(1, first[q]):
                            for m in range(ml):
                                at = (slot(q, d) * ml + m) * extra
                                e = buf["xr"][at : at + extra, c]
                                buf["pp"][slot(q, d), m, :, lanes(c)] += jnp.sum(e * g, axis=0)

    def project_in(s):
        if s == ship:
            arrived_split(
                "grad", buf["gr"].at[0], lambda q: jnp.logical_not(takes(fi[q])),
                lambda q: (first[q] - 1) * (chunk[q] - extra),
                lambda q: (first[q] - 1) * chunk[q] - (first[q] - 2) * extra,
            )
        else:
            arrived("grad", s - ship, buf["gr"].at[s - ship])

        def add(q, d, start, count):
            where = pl.ds(start_of(q, behind(q, d), s) + start, count)
            at = lead1[q] + (d - 1) * chunk[q] + start
            for c in range(nc):
                g = buf["gr"][s - ship, at : at + count, c]
                for m in range(ml):
                    e = e_v[m, where, :, lanes(c)].astype(jnp.float32)
                    proj[m, :, lanes(c)] += jnp.sum(e * g, axis=0)

        for q, d in first_peers():
            if s == ship and extra:
                add(q, d, extra, chunk[q] - extra)
                pl.when(jnp.logical_not(takes(behind(q, d))))(
                    lambda q=q, d=d: add(q, d, 0, extra)
                )
            else:
                add(q, d, 0, chunk[q])

    scope = jax.named_scope
    if sent:
        arrived("scl", 0, buf["sr"])
    for s in order:
        with scope(f"add_first{s}"):
            add_first(s)
    for tick in range(steps + LAG):
        if tick < steps:
            with scope(f"add_second{order[tick]}"):
                add_second(order[tick])
        if tick == LAG:
            arrived("innov", 0, ov.at[pl.ds(0, 2)])
        if tick >= LAG:
            s = order[tick - LAG]
            with scope(f"adjoint{s}"):
                adjoint(s)
            with scope(f"project_own{s}"):
                project_own(s)
            if sent and s == ship - 1:
                for q, d in first_peers():
                    proj_copy(q, d).start()
    if some_first:
        for s in lone:
            with scope(f"project_in{s}"):
                project_in(s)
    with scope("tail"):
        if sent:
            arrived("proj", 0, buf["pr"])
        for m in range(ml):
            total = proj[m]
            if sent:
                for q, d in first_peers():
                    total = total + buf["pr"][slot(q, d), m]
            proj[m] = total
            last[m] = weights[m] * total
    with scope("halo_out"):
        for c in p_copy:
            c.start()
        gwr = buf["gwr"]
        for m in range(ml):
            v = jnp.sum(loc[m] * proj[m], axis=0, keepdims=True)
            gwr[t, m : m + 1] = sum(v[:, lanes(c)] for c in range(nc))
        for d in range(1, tiles):
            remote("gw", 0, gwr.at[t], gwr.at[t], "tile", (t + d) % tiles).start()
        arrived("field", 0, buf["ph"])
    with scope("sweeps"):
        field = []
        for m in range(ml):
            field += [buf["ph"][0, m], last[m], buf["ph"][1, m]]
        field = sweeps(jnp.concatenate(field, axis=0), rates)
        for m in range(ml):
            out[m] = control[m] + field[(3 * m + 1) * rows : (3 * m + 2) * rows]
    with scope("finish"):
        if tiles > 1:
            arrived("gw", 0, gwr.at[pl.ds(0, tiles - 1)])
        total = gwr[0]
        for d in range(1, tiles):
            total = total + gwr[d]
        total = jnp.broadcast_to(jnp.sum(total, axis=1, keepdims=True), (ml, LANES))
        row = lax.broadcasted_iota(jnp.int32, (ml, LANES), 0)
        lane = lax.broadcasted_iota(jnp.int32, (ml, LANES), 1)
        sums = jnp.sum(jnp.where(row == lane, total, 0.0), axis=0)
        gw_out[...] = sums[:ml] / math.sqrt(tiles * rows * ny * vl)
        def all_left(count):
            ref = buf["all"].at[pl.ds(0, count)]
            remote("gw", 0, ref, ref, "tile", nxt).wait_send()

        if extra:
            for case in range(4):
                is_first = (case % 2 == 0, case // 2 == 0)
                change = 0
                for q in range(2):
                    if first[q] > 1:
                        out = first[q] - 1 if is_first[q] else first[q] - 2
                        change += out * (ml - 1) * extra
                        change -= 0 if is_first[q] else (first[q] - 1) * extra
                here = jnp.logical_and(
                    (fi[0] == 0) == is_first[0], (fi[1] == 0) == is_first[1]
                )
                pl.when(here)(functools.partial(all_left, sent_rows + change * nc * rows))
        else:
            all_left(sent_rows)


def store(field, sums, out, gw, sem):
    copies = [
        pltpu.make_async_copy(src, dst, sem.at[i])
        for i, (src, dst) in enumerate(((field, out), (sums, gw)))
    ]
    for c in copies:
        c.start()
    for c in copies:
        c.wait()


def per_device(
    n, tiles,
    ensemble, control, weights, member_band, spread, advect, damping, innovation, obs_weight
):
    ml, vl, rows, ny = ensemble.shape
    a, b = factors(n)
    first, second = (b, a), (a, b)
    assert rows == SWEEPS and ny % LANES == 0 and ml <= 8 and vl % (16 * b) == 0
    assert tiles > 2
    nc = ny // LANES
    size = [vl // (2 * f) for f in first]
    steps = max(d for d in range(1, CHUNKS + 1) if all(k % (8 * d) == 0 for k in size))
    ship = steps * SHIPPED // CHUNKS
    chunk = [k // steps for k in size]
    f32 = jnp.float32
    dma = pltpu.SemaphoreType.DMA
    hbm = pl.BlockSpec(memory_space=pl.ANY)
    whole = pl.BlockSpec(memory_space=pltpu.VMEM)
    field = (rows, ny)
    tile = (nc, rows, LANES)
    vmem = lambda *shape: pltpu.VMEM(shape, f32)
    links = max(sum(f - 1 for f in first), 1)
    block1 = max(sum((f - 1) * k for f, k in zip(first, chunk)), 8)
    block2 = max(sum((g - 1) * k for g, k in zip(second, chunk)), 8)
    ns, nl = max(ship, 1), max(steps - ship, 1)
    total = sum(size)
    out1 = sum((f - 1) * k for f, k in zip(first, chunk))
    out2 = sum((g - 1) * k for g, k in zip(second, chunk))
    fields = 2 * (steps - ship) * out1 + steps * out2 + 4 * ml + 2
    if ship:
        fields += ship * ml * out1 + 2 * ml * sum(f - 1 for f in first)
    sent_rows = fields * nc * rows + 6 * total * nc + (tiles - 1) * ml
    buf = {
        "es": vmem(ns, ml * block1, *tile),
        "er": vmem(ns, ml * block1, *tile),
        "to": vmem(nl, block1, *tile),
        "r1": vmem(nl, block1, *tile),
        "part": vmem(total, *tile),
        "r2": vmem(steps, block2, *tile),
        "grad": vmem(total, *tile),
        "gr": vmem(nl, block1, *tile),
        "iv": vmem(total, *tile),
        "ip": vmem(rows + 4, total, ny),
        "ov": vmem(rows + 2, total, ny),
        "coef": vmem(3, total, LANES),
        "pp": vmem(links, ml, *field),
        "pr": vmem(links, ml, *field),
        "sr": vmem(links, ml, *field),
        "loc": vmem(ml, *field),
        "scl": vmem(ml, *field),
        "proj": vmem(ml, *field),
        "ch": vmem(2, ml + 1, *field),
        "wb": vmem(rows + 2, 8, ny),
        "ph": vmem(2, ml, *field),
        "gwr": vmem(tiles, ml, LANES),
        "last": vmem(ml, *field),
        "all": vmem(sent_rows + 2 * links * ml * EXTRA * nc * rows, LANES),
        "xs": vmem(links * ml * EXTRA, *tile),
        "xr": vmem(links * ml * EXTRA, *tile),
    }
    sems = {
        "sent": dma((1,)), "ship": dma((ns,)), "scl": dma((1,)), "part": dma((nl + 1,)),
        "swap": dma((steps,)), "grad": dma((nl + 1,)), "extra": dma((2,)), "proj": dma((1,)), "control": dma((1,)),
        "innov": dma((1,)), "field": dma((1,)), "halo": dma((steps,)),
        "gw": dma((1,)),
    }
    args = (
        vmem(ml + 1, *field),
        pltpu.SMEM(weights.shape, f32),
        pltpu.SMEM(member_band.shape, member_band.dtype),
        pltpu.SMEM(spread.shape, f32),
        pltpu.SMEM(advect.shape, f32),
        pltpu.SMEM(damping.shape, f32),
    )
    out, gw = pl.pallas_call(
        functools.partial(kernel, n, tiles, steps, ship, sent_rows),
        out_shape=(pltpu.VMEM((ml, rows, ny), f32), pltpu.VMEM((ml,), f32)),
        in_specs=[hbm] * 9,
        out_specs=(whole, whole),
        scratch_shapes=[args, dma((10,)), pltpu.VMEM((ml, vl) + field, ensemble.dtype), buf, sems],
        compiler_params=pltpu.CompilerParams(
            collective_id=0, has_side_effects=True, vmem_limit_bytes=63 * 1024 * 1024
        ),
    )(ensemble, control, weights, member_band, spread, advect, damping, innovation, obs_weight)
    return pl.pallas_call(
        store,
        out_shape=(
            jax.ShapeDtypeStruct((ml, rows, ny), f32),
            jax.ShapeDtypeStruct((ml,), f32),
        ),
        in_specs=[whole, whole],
        out_specs=(hbm, hbm),
        scratch_shapes=[dma((2,))],
    )(*(pltpu.with_memory_space_constraint(x, pltpu.VMEM) for x in (out, gw)))


def solution(mesh):
    in_specs = (
        P("mem", None, "tile", None),
        P("mem", "tile", None),
        P("mem"),
        P("mem"),
        P(),
        P(),
        P(),
        P(None, "tile", None),
        P("tile", None),
    )
    out_specs = (P("mem", "tile", None), P("mem"))
    return jax.shard_map(
        functools.partial(per_device, mesh.shape["mem"], mesh.shape["tile"]),
        mesh=mesh, in_specs=in_specs, out_specs=out_specs, check_vma=False,
    )
```
